32 devices in a mesh: gx: 4 (over y, x), gy: 4 (over z), gz: 2 (over core).
Axes of the slice: x: 2, y: 2, z: 4, core: 2. Of those that a mesh axis runs over, the one named last changes fastest.
Arguments:
- membrane: float32 [64, 64, 512], P('gx', 'gy', 'gz'), may hold values from 0 to 0.95
- recovery: float32 [64, 64, 512], P('gx', 'gy', 'gz'), may hold values from 0 to 2
- extracellular: float32 [64, 64, 512], P('gx', 'gy', 'gz'), may hold values from -6 to 6
- fiber_scale: float32 [64, 64, 512], P('gx', 'gy', 'gz'), may hold values from 0.5 to 2
- labels: int32 [8, 8, 64], P('gx', 'gy', 'gz'), may hold values from 0 to 2
Outputs:
- membrane_next: float32 [64, 64, 512], P('gx', 'gy', 'gz')
- recovery_next: float32 [64, 64, 512], P('gx', 'gy', 'gz')
- extracellular_next: float32 [64, 64, 512], P('gx', 'gy', 'gz')
The draws below stay inside these ranges and needn't reach their ends.
All inputs are finite; a program needn't handle non-finite values.
Results may differ from the reference program's by a relative error of at most 0.0003.
Values sent between devices are 32-bit elements; how exact they have to be, the bound alone decides.
A program may use at most 128 MiB of HBM per device.

```python
import math
import jax
import jax.numpy as jnp
from jax import lax

LEVELS = 4
SMOOTH_SWEEPS = 1
COARSE_SWEEPS = 8
NX = 64
NY = 64
NZ = 512


def draw_membrane(key, part):
    shape = (NX, NY, NZ)
    along_x = lax.broadcasted_iota(jnp.int32, shape, 0)
    along_y = lax.broadcasted_iota(jnp.int32, shape, 1)
    raised = (along_x < NX // 2) != (along_y < NY // 4)
    levels = jnp.where(raised, 0.85, 0.1).astype(jnp.float32)
    spread = 0.1
    noise = jax.random.uniform(key, shape, jnp.float32, -spread, spread)
    return (levels + noise).astype(jnp.float32)


def touch_ends(values, key, least, top_value):
    extent = values.shape
    place = [jax.random.randint(jax.random.fold_in(key, axis), (), 0, extent[axis]) for axis in range(len(extent))]
    values = values.at[tuple(place)].set(least)
    longest = extent.index(max(extent))
    place[longest] = (place[longest] + 1) % extent[longest]
    return values.at[tuple(place)].set(top_value)


def level_of(key, extent, split, least, largest):
    gain = 1.0
    for axis_at, shards_of in split:
        heights = jax.random.uniform(jax.random.fold_in(jax.random.fold_in(key, 6), axis_at), (shards_of,), jnp.float32, least / len(split), largest / len(split))
        gain = gain * jnp.repeat(jnp.exp(heights), extent[axis_at] // shards_of).reshape((-1,) + (1,) * (len(extent) - 1 - axis_at))
    return gain


def gaussian(own_key, extent, scale, bound, shards=(), kind=jnp.bfloat16):
    values = scale * jax.random.normal(own_key, extent, jnp.float32)
    if shards:
        values = values * level_of(own_key, extent, shards, -0.22, 0.18)
    return jnp.clip(values, -bound, bound).astype(kind)


def setup_inputs(seed: int = 0) -> dict:
    arg_keys = jax.random.split(jax.random.key(seed), 6)
    return {
        "membrane": draw_membrane(jax.random.fold_in(arg_keys[5], 71), 0),
        "recovery": jnp.clip(2.0 * jax.random.uniform(arg_keys[1], (NX, NY, NZ), jnp.float32) ** level_of(arg_keys[1], (NX, NY, NZ), ((0, 4), (1, 4), (2, 2)), -0.2, 0.2), 0.0, 2.0),
        "extracellular": gaussian(arg_keys[2], (NX, NY, NZ), 1.0, 6.0, ((0, 4), (1, 4), (2, 2)), jnp.float32),
        "fiber_scale": jnp.clip(jnp.exp(math.log(2.0) - 1.3862944 * jax.random.uniform(arg_keys[3], (NX, NY, NZ), jnp.float32) ** level_of(arg_keys[3], (NX, NY, NZ), ((0, 4), (1, 4), (2, 2)), -0.2, 0.2)), 0.5, 2.0),
        "labels": touch_ends(jax.random.randint(arg_keys[4], (NX // 8, NY // 8, NZ // 8), 0, 3), jax.random.fold_in(arg_keys[4], 1), 0, 2).astype(jnp.int32),
    }


TIME_STEP = 0.05
ionic_gain = 8.0
ionic_onset = 0.15
recovery_rate = 0.01
DIRECTIONS = ((0, -1), (0, 1), (1, -1), (1, 1), (2, -1), (2, 1))


def lookup(labels):
    inner = jnp.where(labels == 1, 1.0, jnp.where(labels == 2, 0.3, 0.0)).astype(jnp.float32)
    outer = jnp.where(labels == 0, 3.0, 1.0).astype(jnp.float32)
    return inner, outer


def expand(blocks, factor):
    sa, sb, sc = blocks.shape
    big = jnp.broadcast_to(blocks[:, None, :, None, :, None], (sa, factor, sb, factor, sc, factor))
    return big.reshape(sa * factor, sb * factor, sc * factor)


def restrict(values):
    shape = values.shape
    lead = shape[:-3]
    folded = values.reshape(lead + (shape[-3] // 2, 2, shape[-2] // 2, 2, shape[-1] // 2, 2))
    return jnp.mean(folded, axis=(-5, -3, -1))


def neighbour(padded, axis_index, side):
    pieces = [slice(1, padded.shape[0] - 1), slice(1, padded.shape[1] - 1), slice(1, padded.shape[2] - 1)]
    pieces[axis_index] = slice(1 + side, padded.shape[axis_index] - 1 + side)
    return padded[tuple(pieces)]


def widen(field):
    return jnp.pad(field, 1)


def widen_stack(coef):
    return jnp.pad(coef, ((0, 0), (1, 1), (1, 1), (1, 1)))


def couplings(pcoef):
    centre_in = neighbour(pcoef[0], 0, 0)
    centre_out = neighbour(pcoef[1], 0, 0)
    result = []
    for axis_index, side in DIRECTIONS:
        result.append(jnp.minimum(centre_in, neighbour(pcoef[0], axis_index, side))
                      + 0.5 * (centre_out + neighbour(pcoef[1], axis_index, side)))
    return result


def offdiag(padded_field, coupling):
    total = jnp.zeros(coupling[0].shape, jnp.float32)
    for index, (axis_index, side) in enumerate(DIRECTIONS):
        total = total + coupling[index] * neighbour(padded_field, axis_index, side)
    return total


def intra(padded_field, pcoef):
    centre_in = neighbour(pcoef[0], 0, 0)
    centre_val = neighbour(padded_field, 0, 0)
    total = jnp.zeros(centre_val.shape, jnp.float32)
    for axis_index, side in DIRECTIONS:
        weight = jnp.minimum(centre_in, neighbour(pcoef[0], axis_index, side))
        total = total + weight * (neighbour(padded_field, axis_index, side) - centre_val)
    return total


def parity_of(shape):
    total = lax.broadcasted_iota(jnp.int32, shape, 0) + lax.broadcasted_iota(jnp.int32, shape, 1)
    total = total + lax.broadcasted_iota(jnp.int32, shape, 2)
    return total % 2


def sweeps(field, rhs, coupling, diagonal, parity, count):
    for sweep_index in range(count):
        for colour in (0, 1):
            updated = (rhs + offdiag(widen(field), coupling)) / diagonal
            field = jnp.where(parity == colour, updated, field)
    return field


def cycle(level_index, field, rhs, padded_coefs):
    coupling = couplings(padded_coefs[level_index])
    diagonal = sum(coupling)
    parity = parity_of(rhs.shape)
    if level_index == LEVELS - 1:
        return sweeps(jnp.zeros_like(rhs), rhs, coupling, diagonal, parity, COARSE_SWEEPS)
    field = sweeps(field, rhs, coupling, diagonal, parity, SMOOTH_SWEEPS)
    remainder = rhs - (diagonal * field - offdiag(widen(field), coupling))
    coarse_rhs = 4.0 * restrict(remainder)
    correction = cycle(level_index + 1, jnp.zeros_like(coarse_rhs), coarse_rhs, padded_coefs)
    field = field + expand(correction, 2)
    return sweeps(field, rhs, coupling, diagonal, parity, SMOOTH_SWEEPS)


def reference(membrane, recovery, extracellular, fiber_scale, labels):
    lab_in, lab_out = lookup(labels)
    tissue = (expand(labels, 8) != 0).astype(jnp.float32)
    inner = expand(lab_in, 8) * fiber_scale
    outer = expand(lab_out, 8)
    coef = jnp.stack([inner, outer])
    padded_coefs = []
    for level_index in range(LEVELS):
        padded_coefs.append(widen_stack(coef))
        if level_index + 1 < LEVELS:
            coef = restrict(coef)
    drive = intra(widen(membrane + extracellular), padded_coefs[0])
    ionic = ionic_gain * membrane * (membrane - ionic_onset) * (membrane - 1.0) + membrane * recovery
    membrane_next = membrane + TIME_STEP * (drive - tissue * ionic)
    recovery_next = recovery + TIME_STEP * recovery_rate * (-recovery - ionic_gain * membrane * (membrane - ionic_onset - 1.0))
    rhs = intra(widen(membrane_next), padded_coefs[0])
    extracellular_next = cycle(0, extracellular, rhs, padded_coefs)
    return membrane_next, recovery_next, extracellular_next
```

```python
import functools

import jax
import jax.numpy as jnp
from jax import lax
from jax.experimental import pallas as pl
from jax.experimental.pallas import tpu as pltpu
from jax.sharding import PartitionSpec as P

COARSE_SWEEPS = 8
TIME_STEP = 0.05
ionic_gain = 8.0
ionic_onset = 0.15
recovery_rate = 0.01
MESH = pl.DeviceIdType.MESH
LANES = 128
F32 = jnp.float32

INNER, U, OUTER, V, NEXT, RED, BLACK, FIXED, LAST = range(9)
INNER1, OUTER1, RED1, BLACK1, FIXED1, LASTRED1, LASTBLACK1 = range(7)
EXCHANGES = (
    (0, INNER, 2),
    (0, OUTER, 2),
    (1, INNER1, 2),
    (0, NEXT, 1),
    (0, RED, 1),
    (0, BLACK, 1),
    (1, RED1, 1),
    (1, BLACK1, 1),
    (1, LASTRED1, 1),
    (1, LASTBLACK1, 1),
    (0, LAST, 1),
)
SIDES = 5


def dot(a, b):
    return jnp.dot(a, b, precision=lax.Precision.HIGHEST, preferred_element_type=F32)


def pair_matrix(rows, cols, offset):
    j = lax.broadcasted_iota(jnp.int32, (rows, cols), 0)
    k = lax.broadcasted_iota(jnp.int32, (rows, cols), 1)
    return jnp.where(lax.shift_right_logical(j, 1) + offset == k, 1.0, 0.0).astype(F32)


def copy_matrix(rows, cols, shift):
    k = lax.broadcasted_iota(jnp.int32, (rows, cols), 0)
    j = lax.broadcasted_iota(jnp.int32, (rows, cols), 1)
    return jnp.where(lax.shift_right_logical(j, shift) == k, 1.0, 0.0).astype(F32)


class Grid:
    def __init__(self, planes, rows, lanes):
        self.planes, self.rows, self.lanes = planes, rows, lanes
        self.row = lax.broadcasted_iota(jnp.int32, (rows, lanes), 0)
        self.lane = lax.broadcasted_iota(jnp.int32, (rows, lanes), 1)
        self.even = jnp.bitwise_and(self.row + self.lane, 1) == 0
        self.odd = jnp.bitwise_and(self.row + self.lane, 1) == 1

    def colour(self, x, colour):
        return self.even if (x + colour) % 2 == 0 else self.odd


class Halo:
    def __init__(self, grid, refs, iz):
        self.grid, self.iz = grid, iz
        self.xs, self.ys, self.zs, self.xh, self.yh, self.zh = refs
        self.flane = lax.broadcasted_iota(jnp.int32, (grid.rows, LANES), 1)

    def faces(self, slot, planes):
        g = self.grid
        acc = jnp.zeros((g.rows, LANES), F32)
        for x, val in planes:
            self.ys[0, slot, x : x + 1, :] = val[0:1]
            self.ys[1, slot, x : x + 1, :] = val[g.rows - 1 :]
            if g.lanes > LANES:
                end = jnp.where(self.iz == 0, val[:, g.lanes - LANES :], val[:, :LANES])
            else:
                end = val
            acc = jnp.where(self.flane == x, pltpu.roll(end, x + 1 - self.iz, 1), acc)
            yield
        self.zs[slot] = acc

    def put_ends(self, slot, ref):
        self.xs[0, slot] = ref[0]
        self.xs[1, slot] = ref[self.grid.planes - 1]

    def put_rest(self, slot, ref):
        for _ in self.faces(slot, [(x, ref[x]) for x in range(self.grid.planes)]):
            pass

    def put(self, slot, ref):
        self.put_ends(slot, ref)
        self.put_rest(slot, ref)

    def neighbours(self, slot, planes, x, edge=False):
        g = self.grid
        val = planes(x)
        xm = planes(x - 1) if x > 0 else self.xh[0, slot]
        xp = planes(x + 1) if x < g.planes - 1 else self.xh[1, slot]
        shape = (g.rows, g.lanes)
        low = jnp.broadcast_to(self.yh[0, slot, x : x + 1, :], shape)
        high = jnp.broadcast_to(self.yh[1, slot, x : x + 1, :], shape)
        ym = jnp.where(g.row == 0, low, pltpu.roll(val, 1, 0))
        yp = jnp.where(g.row == g.rows - 1, high, pltpu.roll(val, g.rows - 1, 0))
        side = jnp.broadcast_to(self.zh[slot, :, x : x + 1], shape)
        side_m, side_p = side, side
        if edge:
            side_m = jnp.where(self.iz == 0, 0.0, side)
            side_p = jnp.where(self.iz == 0, side, 0.0)
        zm = jnp.where(g.lane == 0, side_m, pltpu.roll(val, 1, 1))
        zp = jnp.where(g.lane == g.lanes - 1, side_p, pltpu.roll(val, g.lanes - 1, 1))
        return val, (xm, xp, ym, yp, zm, zp)


def halve_rows(tmp, slot, val):
    rows, lanes = val.shape
    parts = []
    for k in range(lanes // LANES):
        at = 2 * slot + k
        tmp[at, 0:rows, :] = val[:, k * LANES : (k + 1) * LANES]
        parts.append(tmp[at, pl.ds(0, rows // 2, 2), :] + tmp[at, pl.ds(1, rows // 2, 2), :])
    return parts[0] if len(parts) == 1 else jnp.concatenate(parts, axis=1)


def double_rows(tmp, slot, val):
    rows, lanes = val.shape
    parts = []
    for k in range(lanes // LANES):
        at = 2 * slot + k
        piece = val[:, k * LANES : (k + 1) * LANES]
        tmp[at, pl.ds(0, rows, 2), :] = piece
        tmp[at, pl.ds(1, rows, 2), :] = piece
        parts.append(tmp[at, 0 : 2 * rows, :])
    return parts[0] if len(parts) == 1 else jnp.concatenate(parts, axis=1)


def kernel(counts, *refs):
    sources, (mem_out, rec_out, ext_out) = refs[:5], refs[5:8]
    refs = refs[8:]
    mem, rec, ext, fib, lab, in_sem = refs[:6]
    refs = (None,) + refs
    (xs0, ys0, zs0, xh0, yh0, zh0, xs1, ys1, zs1, xh1, yh1, zh1) = refs[7:19]
    (in0, out0, uu, w0, c0, d0, b0, va, vb, tmp, tall) = refs[19:30]
    (in1, out1, c1, d1, b1, v1a, v1b) = refs[30:37]
    (gc_own, gc, gr_own, gr, in2, out2, c2, d2, b2, v2a, v2b) = refs[37:48]
    (c3, b3, v3, k3, h3, send_sem, recv_sem, gs_sem, gr_sem) = refs[48:]
    nx, ny, nz = counts
    ix, iy, iz = lax.axis_index("gx"), lax.axis_index("gy"), lax.axis_index("gz")
    me = (ix * ny + iy) * nz + iz
    total = nx * ny * nz

    loads = [
        pltpu.make_async_copy(src, dst, in_sem.at[i])
        for i, (src, dst) in enumerate(zip(sources, (mem, rec, ext, fib, lab)))
    ]
    for i in (4, 3, 0, 2, 1):
        loads[i].start()

    barrier = pltpu.get_barrier_semaphore()

    def others(body):
        def step(i, carry):
            dev = lax.rem(me + i, total)
            body(dev, (dev // (ny * nz), lax.rem(dev // nz, ny), lax.rem(dev, nz)))
            return carry

        lax.fori_loop(1, total, step, 0)

    others(lambda dev, where: pl.semaphore_signal(barrier, inc=1, device_id=where, device_id_type=MESH))

    def clear(missing, ref, side):
        def fill():
            ref[side] = jnp.zeros(ref.shape[1:], F32)

        pl.when(missing)(fill)

    for xh, yh in ((xh0, yh0), (xh1, yh1)):
        clear(ix == 0, xh, 0)
        clear(ix == nx - 1, xh, 1)
        clear(iy == 0, yh, 0)
        clear(iy == ny - 1, yh, 1)
    for load in loads:
        load.wait()

    g0 = Grid(*mem.shape)
    g1 = Grid(*in1.shape)
    halo0 = Halo(g0, (xs0, ys0, zs0, xh0, yh0, zh0), iz)
    halo1 = Halo(g1, (xs1, ys1, zs1, xh1, yh1, zh1), iz)

    def copies(number):
        level, first, slots = EXCHANGES[number]
        h = (halo0, halo1)[level]
        part = pl.ds(first, slots)
        plan = (
            (h.xs.at[0, part], h.xh.at[1, part], (ix - 1, iy, iz), ix > 0, ix < nx - 1),
            (h.xs.at[1, part], h.xh.at[0, part], (ix + 1, iy, iz), ix < nx - 1, ix > 0),
            (h.ys.at[0, part], h.yh.at[1, part], (ix, iy - 1, iz), iy > 0, iy < ny - 1),
            (h.ys.at[1, part], h.yh.at[0, part], (ix, iy + 1, iz), iy < ny - 1, iy > 0),
            (h.zs.at[part], h.zh.at[part], (ix, iy, 1 - iz), None, None),
        )
        for side, (src, dst, dev, goes, comes) in enumerate(plan):
            copy = pltpu.make_async_remote_copy(
                src_ref=src,
                dst_ref=dst,
                send_sem=send_sem.at[number * SIDES + side],
                recv_sem=recv_sem.at[number * SIDES + side],
                device_id=dev,
                device_id_type=MESH,
            )
            yield copy, goes, comes

    ends, rest = slice(0, 2), slice(2, SIDES)

    def send(number, sides=slice(0, SIDES)):
        for copy, goes, _ in list(copies(number))[sides]:
            if goes is None:
                copy.start()
            else:
                pl.when(goes)(copy.start)

    def arrive(number, sides=slice(0, SIDES)):
        for copy, _, comes in list(copies(number))[sides]:
            if comes is None:
                copy.wait_recv()
            else:
                pl.when(comes)(copy.wait_recv)

    def inner_first(number, count):
        arrive(number, rest)
        yield from range(1, count - 1)
        arrive(number, ends)
        yield 0
        yield count - 1

    def publish(number, halo, slot, ref):
        halo.put_ends(slot, ref)
        send(number, ends)
        halo.put_rest(slot, ref)
        send(number, rest)

    def sent(number):
        for copy, goes, _ in copies(number):
            if goes is None:
                copy.wait_send()
            else:
                pl.when(goes)(copy.wait_send)

    def gather_send(own, whole, which):
        def go(dev, where):
            pltpu.make_async_remote_copy(
                src_ref=own,
                dst_ref=whole.at[me],
                send_sem=gs_sem.at[which],
                recv_sem=gr_sem.at[which],
                device_id=where,
                device_id_type=MESH,
            ).start()

        others(go)
        whole[pl.ds(me, 1)] = own[...][None]

    def gather_wait(whole, which, recv):
        rest = whole.at[pl.ds(0, total - 1)]
        copy = pltpu.make_async_remote_copy(
            src_ref=rest,
            dst_ref=rest,
            send_sem=gs_sem.at[which],
            recv_sem=gr_sem.at[which],
            device_id=(ix, iy, 1 - iz),
            device_id_type=MESH,
        )
        if recv:
            copy.wait_recv()
        else:
            copy.wait_send()

    X0, R0, Z0 = mem.shape
    X1, R1, Z1 = in1.shape
    X2 = X1 // 2
    R2 = R1 // 2
    half = Z1 // 2

    widen8 = copy_matrix(lab.shape[2], Z0, 3)
    lab_planes = []
    for bx in range(lab.shape[0]):
        wide = jnp.dot(lab[bx].astype(F32), widen8, preferred_element_type=F32)
        lab_planes.append(
            jnp.concatenate(
                [jnp.broadcast_to(wide[by : by + 1], (8, Z0)) for by in range(lab.shape[1])], axis=0
            )
        )

    def label_of(x):
        return lab_planes[x // 8]

    for x in range(X0):
        label = label_of(x)
        in0[x] = jnp.where(label == 1.0, 1.0, jnp.where(label == 2.0, 0.3, 0.0)) * fib[x]
        out0[x] = jnp.where(label == 0.0, 3.0, 1.0)
        uu[x] = mem[x] + ext[x]
    halo0.put(INNER, in0)
    halo0.put(U, uu)
    pl.semaphore_wait(barrier, total - 1)
    send(0)
    halo0.put(OUTER, out0)
    halo0.put(V, ext)
    send(1)

    narrow = pair_matrix(Z0, Z1, 0)
    narrow_low = pair_matrix(Z1, Z1, 0)
    narrow_high = pair_matrix(Z1, Z1, half)
    double01 = copy_matrix(Z1, Z0, 1)
    double12 = copy_matrix(Z1, Z1, 1)

    def restrict0(plane, factor, base, order=None):
        for x in order or range(X1):
            tall[base + x * R1 : base + (x + 1) * R1, :] = halve_rows(tmp, x, plane(2 * x) + plane(2 * x + 1))
        whole = dot(tall[base : base + X1 * R1, :], narrow) * factor
        return [whole[x * R1 : (x + 1) * R1] for x in range(X1)]

    def restrict1(plane, factor, order=None):
        rows = [None] * X2
        for x in order or range(X2):
            rows[x] = halve_rows(tmp, x, plane(2 * x) + plane(2 * x + 1))
        low = jnp.concatenate(rows[: X2 // 2], axis=0)
        high = jnp.concatenate(rows[X2 // 2 :], axis=0)
        return (dot(low, narrow_low) + dot(high, narrow_high)) * factor

    for x, val in enumerate(restrict0(lambda x: in0[x], 0.125, 0)):
        in1[x] = val
    for x, val in enumerate(restrict0(lambda x: out0[x], 0.125, 0)):
        out1[x] = val
    halo1.put(INNER1, in1)
    halo1.put(OUTER1, out1)
    send(2)
    gc_own[0] = restrict1(lambda x: in1[x], 0.125)
    gc_own[1] = restrict1(lambda x: out1[x], 0.125)
    gather_send(gc_own, gc, 0)

    for x in inner_first(0, X0):
        centre, near = halo0.neighbours(INNER, lambda x: in0[x], x, edge=True)
        u, near_u = halo0.neighbours(U, lambda x: uu[x], x)
        drive = jnp.zeros_like(u)
        for d in range(6):
            weight = jnp.minimum(centre, near[d])
            w0[d, x] = weight
            drive = drive + weight * (near_u[d] - u)
        m, r = mem[x], rec[x]
        tissue = jnp.where(label_of(x) != 0.0, 1.0, 0.0)
        ionic = ionic_gain * m * (m - ionic_onset) * (m - 1.0) + m * r
        mem_out[x] = m + TIME_STEP * (drive - tissue * ionic)
    publish(3, halo0, NEXT, mem_out)
    for x in range(X0):
        m, r = mem[x], rec[x]
        rec_out[x] = r + TIME_STEP * recovery_rate * (-r - ionic_gain * m * (m - ionic_onset - 1.0))

    def scaled(grid, weights, centre, near, iz_edges):
        full = [weights[d] + 0.5 * (centre + near[d]) for d in range(6)]
        diag = ((full[0] + full[1]) + (full[2] + full[3])) + (full[4] + full[5])
        inv = 1.0 / diag
        full = [f * inv for f in full]
        low, high = iz_edges
        full[4] = jnp.where(low, 0.0, full[4])
        full[5] = jnp.where(high, 0.0, full[5])
        return full, diag, inv

    first0 = (g0.lane == 0) & (iz == 0)
    last0 = (g0.lane == Z0 - 1) & (iz == nz - 1)
    arrive(1)
    inv0 = vb
    for x in range(X0):
        centre, near = halo0.neighbours(OUTER, lambda x: out0[x], x, edge=True)
        full, diag, inv = scaled(g0, [w0[d, x] for d in range(6)], centre, near, (first0, last0))
        for d in range(6):
            c0[d, x] = full[d]
        d0[x] = diag
        b0[x] = inv

    def update(halo, slot, planes, c, b, x):
        val, near = halo.neighbours(slot, planes, x)
        a = b[x] + c[0, x] * near[0]
        e = c[1, x] * near[1] + c[2, x] * near[2]
        f = c[3, x] * near[3] + c[4, x] * near[4]
        return val, (a + c[5, x] * near[5]) + (e + f)

    def half_sweep(number, halo, slot, src, dst, c, b, colour):
        planes = halo.grid.planes
        for x in range(planes) if number is None else inner_first(number, planes):
            val, new = update(halo, slot, lambda x: src[x], c, b, x)
            dst[x] = jnp.where(halo.grid.colour(x, colour), new, val)

    for x in inner_first(3, X0):
        m, near = halo0.neighbours(NEXT, lambda x: mem_out[x], x)
        rhs = jnp.zeros_like(m)
        for d in range(6):
            rhs = rhs + w0[d, x] * (near[d] - m)
        b0[x] = rhs * b0[x]
        val, new = update(halo0, V, lambda x: ext[x], c0, b0, x)
        va[x] = jnp.where(g0.colour(x, 0), new, val)
    publish(4, halo0, RED, va)

    first1 = (g1.lane == 0) & (iz == 0)
    last1 = (g1.lane == Z1 - 1) & (iz == nz - 1)
    arrive(2)
    for x in range(X1):
        ci, ni = halo1.neighbours(INNER1, lambda x: in1[x], x, edge=True)
        co, no = halo1.neighbours(OUTER1, lambda x: out1[x], x, edge=True)
        full, diag, inv = scaled(g1, [jnp.minimum(ci, n) for n in ni], co, no, (first1, last1))
        for d in range(6):
            c1[d, x] = full[d]
        d1[x] = diag
        b1[x] = inv

    half_sweep(4, halo0, RED, va, vb, c0, b0, 1)
    publish(5, halo0, BLACK, vb)

    XG, RG, ZG = in2.shape
    XH, RH = XG // 2, RG // 2
    g2 = Grid(XG, RG, ZG)
    g3 = Grid(XH, RH, ZG)
    tile_row = lax.broadcasted_iota(jnp.int32, (8, LANES), 0)
    tile_lane = lax.broadcasted_iota(jnp.int32, (8, LANES), 1)

    def unpack(tile, dst):
        for px in range(nx):
            for py in range(ny // 2):
                lows, highs = [], []
                for part in range(2):
                    base = (px * ny + 2 * py + part) * nz
                    s0, s1 = tile(base), tile(base + 1)
                    lows.append(jnp.where(tile_lane < half, s0, pltpu.roll(s1, half, 1)))
                    highs.append(jnp.where(tile_lane < half, pltpu.roll(s0, half, 1), s1))
                for xhi, pair in enumerate((lows, highs)):
                    p = px * X2 + xhi * 2
                    dst[p, py * 8 : py * 8 + 8, :] = jnp.where(tile_row < R2, pair[0], pltpu.roll(pair[1], R2, 0))
                    dst[p + 1, py * 8 : py * 8 + 8, :] = jnp.where(
                        tile_row < R2, pltpu.roll(pair[0], R2, 0), pair[1]
                    )

    def whole_neighbours(grid, planes, x, last, mask):
        val = planes(x)
        zero = jnp.zeros_like(val)
        xm = planes(x - 1) if x > 0 else zero
        xp = planes(x + 1) if x < grid.planes - 1 else zero
        near = [
            xm,
            xp,
            pltpu.roll(val, 1, 0),
            pltpu.roll(val, grid.rows - 1, 0),
            pltpu.roll(val, 1, 1),
            pltpu.roll(val, grid.lanes - 1, 1),
        ]
        if mask:
            near[2] = jnp.where(grid.row == 0, 0.0, near[2])
            near[3] = jnp.where(grid.row == grid.rows - 1, 0.0, near[3])
            near[4] = jnp.where(grid.lane == 0, 0.0, near[4])
            near[5] = jnp.where(grid.lane >= last, 0.0, near[5])
        return val, near

    def whole_couplings(grid, inner, outer, last, c, d, b):
        for x in range(grid.planes):
            ci, ni = whole_neighbours(grid, lambda x: inner[x], x, last, True)
            co, no = whole_neighbours(grid, lambda x: outer[x], x, last, True)
            full = [jnp.minimum(ci, ni[k]) + 0.5 * (co + no[k]) for k in range(6)]
            diag = ((full[0] + full[1]) + (full[2] + full[3])) + (full[4] + full[5])
            if last < grid.lanes - 1:
                diag = jnp.where(grid.lane <= last, diag, 1.0)
            inv = 1.0 / diag
            edges = (
                None,
                None,
                grid.row == 0,
                grid.row == grid.rows - 1,
                grid.lane == 0,
                grid.lane >= last,
            )
            for k in range(6):
                f = full[k] * inv
                if edges[k] is not None:
                    f = jnp.where(edges[k], 0.0, f)
                if last < grid.lanes - 1:
                    f = jnp.where(grid.lane <= last, f, 0.0)
                c[k, x] = f
            if d is not None:
                d[x] = diag
            b[x] = inv

    def whole_update(grid, planes, c, b, x):
        val, near = whole_neighbours(grid, planes, x, None, False)
        a = b[x] + c[2, x] * near[2]
        e = c[3, x] * near[3] + c[4, x] * near[4]
        a = a + c[5, x] * near[5]
        if x > 0:
            a = a + c[0, x] * near[0]
        if x < grid.planes - 1:
            e = e + c[1, x] * near[1]
        return val, a + e

    def restrict2(plane, factor):
        pieces = [halve_rows(tmp, x, plane(2 * x) + plane(2 * x + 1)) for x in range(XH)]
        for x in range(XH):
            tall[x * RH : (x + 1) * RH, 0:ZG] = pieces[x]
        whole = dot(tall[0 : XH * RH, 0:ZG], narrow_low) * factor
        return [whole[x * RH : (x + 1) * RH] for x in range(XH)]

    gather_wait(gc, 0, True)
    unpack(lambda t: gc[t, 0], in2)
    unpack(lambda t: gc[t, 1], out2)
    whole_couplings(g2, in2, out2, ZG - 1, c2, d2, b2)
    for x, val in enumerate(restrict2(lambda x: in2[x], 0.125)):
        v3[x] = val
    for x, val in enumerate(restrict2(lambda x: out2[x], 0.125)):
        v2a[x, 0:RH] = val
    whole_couplings(g3, v3, v2a.at[:, 0:RH], ZG // 2 - 1, c3, None, b3)

    XP = XH // 2
    own = (g3.even, g3.odd)

    def pack(colour, near, far):
        return jnp.where(own[colour], near, far)

    for colour in range(2):
        for p in range(XP):
            a, z = 2 * p, 2 * p + 1
            k3[colour * 6, p] = pack(colour, c3[1, a], c3[0, z])
            k3[colour * 6 + 1, p] = pack(colour, c3[0, a], c3[1, z])
            for k in range(2, 6):
                k3[colour * 6 + k, p] = pack(colour, c3[k, a], c3[k, z])

    def residual0(x):
        val, new = update(halo0, BLACK, lambda x: vb[x], c0, b0, x)
        return d0[x] * (new - val)

    for x, val in enumerate(restrict0(residual0, 0.5, 0, inner_first(5, X1))):
        b1[x] = val * b1[x]
        v1a[x] = jnp.where(g1.colour(x, 0), b1[x], 0.0)
    publish(6, halo1, RED1, v1a)
    half_sweep(6, halo1, RED1, v1a, v1b, c1, b1, 1)
    publish(7, halo1, BLACK1, v1b)

    def residual1(x):
        val, new = update(halo1, BLACK1, lambda x: v1b[x], c1, b1, x)
        return d1[x] * (new - val)

    gr_own[...] = restrict1(residual1, 0.5, inner_first(7, X2))
    gather_send(gr_own, gr, 1)
    gather_wait(gr, 1, True)
    unpack(lambda t: gr[t], v2b)
    for x in range(XG):
        b2[x] = v2b[x] * b2[x]
        v2a[x] = jnp.where(g2.colour(x, 0), b2[x], 0.0)
    for x in range(XG):
        val, new = whole_update(g2, lambda x: v2a[x], c2, b2, x)
        v2b[x] = jnp.where(g2.colour(x, 1), new, val)

    def residual2(x):
        val, new = whole_update(g2, lambda x: v2b[x], c2, b2, x)
        return d2[x] * (new - val)

    for x, val in enumerate(restrict2(residual2, 0.5)):
        b3[x] = val * b3[x]

    for colour in range(2):
        for p in range(XP):
            h3[colour, p] = pack(colour, b3[2 * p], b3[2 * p + 1])
    none = jnp.zeros((RH, ZG), F32)

    def relaxed(colour, other):
        fresh = []
        for p in range(XP):
            val, at = other[p], colour * 6
            before = other[p - 1] if p > 0 else none
            after = other[p + 1] if p < XP - 1 else none
            i = h3[colour, p] + k3[at, p] * val
            j = k3[at + 1, p] * pack(colour, before, after) + k3[at + 2, p] * pltpu.roll(val, 1, 0)
            l = k3[at + 3, p] * pltpu.roll(val, RH - 1, 0) + k3[at + 4, p] * pltpu.roll(val, 1, 1)
            fresh.append((i + k3[at + 5, p] * pltpu.roll(val, ZG - 1, 1)) + (j + l))
        return fresh

    def coarse(step, state):
        red = relaxed(0, state[XP:])
        black = relaxed(1, red)
        return tuple(red + black)

    state = lax.fori_loop(0, COARSE_SWEEPS, coarse, (none,) * (2 * XP))
    solved = []
    for p in range(XP):
        solved.append(pack(0, state[p], state[XP + p]))
        solved.append(pack(1, state[p], state[XP + p]))
    for x in range(XH):
        tall[x * RH : (x + 1) * RH, 0:ZG] = solved[x]
    wide = dot(tall[0 : XH * RH, 0:ZG], double12)
    for x in range(XH):
        corr = double_rows(tmp, x, wide[x * RH : (x + 1) * RH])
        v2a[2 * x] = v2b[2 * x] + corr
        v2a[2 * x + 1] = v2b[2 * x + 1] + corr
    for colour, src, dst in ((0, v2a, v2b), (1, v2b, v2a)):
        for x in range(XG):
            val, new = whole_update(g2, lambda x: src[x], c2, b2, x)
            dst[x] = jnp.where(g2.colour(x, colour), new, val)

    row_shift = lax.rem(RG - iy * R2, RG)
    lane_shift = lax.rem(ZG - iz * half, ZG)
    lane8 = lax.broadcasted_iota(jnp.int32, (8, LANES), 1)
    side = jnp.zeros((8, LANES), F32)
    below, above = X2 * 8, X2 * 8 + 8
    low, high, across = above + 8, above + 16, above + 24
    tall[low : across, 0:ZG] = jnp.zeros((across - low, ZG), F32)
    for k in range(-1, X2 + 1):
        part = v2a[jnp.clip(ix * X2 + k, 0, XG - 1)]
        part = pltpu.roll(pltpu.roll(part, row_shift, 0), lane_shift, 1)
        if k < 0:
            tall[below : below + 8, 0:ZG] = jnp.where(ix > 0, part[0:8], 0.0)
        elif k == X2:
            tall[above : above + 8, 0:ZG] = jnp.where(ix < nx - 1, part[0:8], 0.0)
        else:
            tall[k * 8 : (k + 1) * 8, 0:ZG] = part[0:8]
            tall[low + k : low + k + 1, 0:ZG] = jnp.where(iy > 0, part[RG - 1 : RG], 0.0)
            tall[high + k : high + k + 1, 0:ZG] = jnp.where(iy < ny - 1, part[R2 : R2 + 1], 0.0)
            turned = pltpu.roll(part[0:8], k + 1 + (half - 1) * (1 - iz), 1)
            side = jnp.where(lane8 == k, turned, side)
    tall[across : across + 8, 0:ZG] = side
    wide = dot(tall[0 : across + 8, 0:ZG], double12)

    def grown(slot, row):
        return double_rows(tmp, slot, wide[row : row + R2])

    for x in range(X2):
        corr = grown(x, x * 8)
        v1a[2 * x] = v1b[2 * x] + corr
        v1a[2 * x + 1] = v1b[2 * x + 1] + corr
    xh1[0, FIXED1] = xh1[0, BLACK1] + grown(0, below)
    xh1[1, FIXED1] = xh1[1, BLACK1] + grown(1, above)
    yh1[0, FIXED1] = yh1[0, BLACK1] + grown(2, low)
    yh1[1, FIXED1] = yh1[1, BLACK1] + grown(3, high)
    zh1[FIXED1] = zh1[BLACK1] + grown(0, across)
    half_sweep(None, halo1, FIXED1, v1a, v1b, c1, b1, 0)
    publish(8, halo1, LASTRED1, v1b)
    half_sweep(8, halo1, LASTRED1, v1b, v1a, c1, b1, 1)
    publish(9, halo1, LASTBLACK1, v1a)

    def enlarge(count, read, write):
        for x in range(count):
            tall[x * R1 : (x + 1) * R1, 0:Z1] = read(x)
        wide = dot(tall[0 : count * R1, 0:Z1], double01)
        for x in range(count):
            write(x, double_rows(tmp, x, wide[x * R1 : (x + 1) * R1]))

    def inside(x, corr):
        va[2 * x] = vb[2 * x] + corr
        va[2 * x + 1] = vb[2 * x + 1] + corr

    enlarge(X1, lambda x: v1a[x], inside)
    arrive(9)

    def rim(k):
        if k < 2:
            return xh1[k, LASTBLACK1]
        if k < 4:
            return yh1[k - 2, LASTBLACK1]
        return zh1[LASTBLACK1]

    def outside(k, corr):
        if k < 2:
            xh0[k, FIXED] = xh0[k, BLACK] + corr
        elif k < 4:
            yh0[k - 2, FIXED] = yh0[k - 2, BLACK] + corr
        else:
            zh0[FIXED] = zh0[BLACK] + corr[:, 0:LANES]

    enlarge(5, rim, outside)
    half_sweep(None, halo0, FIXED, va, vb, c0, b0, 0)
    publish(10, halo0, LAST, vb)
    half_sweep(10, halo0, LAST, vb, ext_out, c0, b0, 1)

    for number in range(len(EXCHANGES)):
        sent(number)
    gather_wait(gc, 0, False)
    gather_wait(gr, 1, False)


def finish(*refs):
    count = (len(refs) - 1) // 2
    sem = refs[-1]
    copies = [pltpu.make_async_copy(refs[i], refs[count + i], sem.at[i]) for i in range(count)]
    for copy in copies:
        copy.start()
    for copy in copies:
        copy.wait()


def solution(mesh):
    nx, ny, nz = (mesh.shape[a] for a in ("gx", "gy", "gz"))
    spec = P("gx", "gy", "gz")

    def on_device(membrane, recovery, extracellular, fiber_scale, labels):
        X, R, Z = membrane.shape
        X1, R1, Z1 = X // 2, R // 2, Z // 2
        XG, RG, ZG = nx * X // 4, ny * R // 4, nz * Z // 4
        assert nz == 2 and ny % 2 == 0 and ZG == LANES and Z1 == LANES
        assert R1 == 8 and X1 == 8 and X % 8 == 0
        total = nx * ny * nz
        f0, f1 = 9, 7
        field = (X, R, Z)
        lvl1 = (X1, R1, Z1)
        whole = (XG, RG, ZG)
        third = (XG // 2, RG // 2, ZG)

        def v(*shape):
            return pltpu.VMEM(shape, F32)

        def faces(f, x, r, z):
            return [v(2, f, r, z), v(2, f, x, z), v(f, r, LANES)] * 2

        anywhere = pl.BlockSpec(memory_space=pl.ANY)
        scratch = [v(*field)] * 4 + [pltpu.VMEM(labels.shape, jnp.int32), pltpu.SemaphoreType.DMA((5,))]
        scratch += faces(f0, *field) + faces(f1, *lvl1)
        scratch += [v(*field), v(*field), v(*field), v(6, *field), v(6, *field), v(*field), v(*field)]
        scratch += [v(*field), v(*field)]
        scratch += [
            v(2 * max(X1, XG // 2), max(R, RG), LANES),
            v(max(X1 * R1, (XG // 2) * (RG // 2), 2 * X1 * R1), Z),
        ]
        scratch += [v(*lvl1), v(*lvl1), v(6, *lvl1), v(*lvl1), v(*lvl1), v(*lvl1), v(*lvl1)]
        scratch += [v(2, 8, LANES), v(total, 2, 8, LANES), v(8, LANES), v(total, 8, LANES)]
        scratch += [v(*whole), v(*whole), v(6, *whole), v(*whole), v(*whole), v(*whole), v(*whole)]
        scratch += [v(6, *third), v(*third), v(*third)]
        packed = (XG // 4, RG // 2, ZG)
        scratch += [v(12, *packed), v(2, *packed)]
        sems = SIDES * len(EXCHANGES)
        scratch += [pltpu.SemaphoreType.DMA((sems,))] * 2 + [pltpu.SemaphoreType.DMA((2,))] * 2
        vmem = pl.BlockSpec(memory_space=pltpu.VMEM)
        room = 54400 << 10
        shape = jax.ShapeDtypeStruct(field, F32)
        results = pl.pallas_call(
            functools.partial(kernel, (nx, ny, nz)),
            out_shape=[shape] * 3,
            in_specs=[anywhere] * 5,
            out_specs=[vmem] * 3,
            scratch_shapes=scratch,
            compiler_params=pltpu.CompilerParams(
                collective_id=0, has_side_effects=True, vmem_limit_bytes=room
            ),
        )(membrane, recovery, extracellular, fiber_scale, labels)
        return tuple(
            pl.pallas_call(
                finish,
                out_shape=[shape] * 3,
                in_specs=[vmem] * 3,
                out_specs=[anywhere] * 3,
                scratch_shapes=[pltpu.SemaphoreType.DMA((3,))],
                compiler_params=pltpu.CompilerParams(vmem_limit_bytes=4 << 20),
            )(*results)
        )

    return jax.shard_map(
        on_device,
        mesh=mesh,
        in_specs=(spec,) * 5,
        out_specs=(spec,) * 3,
        check_vma=False,
    )
```

```python
import functools

import jax
import jax.numpy as jnp
from jax import lax
from jax.experimental import pallas as pl
from jax.experimental.pallas import tpu as pltpu
from jax.sharding import PartitionSpec as P

COARSE_SWEEPS = 8
TIME_STEP = 0.05
ionic_gain = 8.0
ionic_onset = 0.15
recovery_rate = 0.01
MESH = pl.DeviceIdType.MESH
LANES = 128
F32 = jnp.float32

INNER, U, OUTER, V, NEXT, RED, BLACK, FIXED, LAST = range(9)
INNER1, OUTER1, RHS1 = range(3)
GHOST = 4
EXCHANGES = (
    (INNER, 2),
    (OUTER, 2),
    (NEXT, 1),
    (RED, 1),
    (BLACK, 1),
    (LAST, 1),
)
SIDES = 5
WIDE = ((INNER1, 2), (RHS1, 1))
STEPS = (-1, 0, 1)
WIDE_SIDES = 17


def dot(a, b):
    return jnp.dot(a, b, precision=lax.Precision.HIGHEST, preferred_element_type=F32)


def pair_matrix(rows, cols, offset):
    j = lax.broadcasted_iota(jnp.int32, (rows, cols), 0)
    k = lax.broadcasted_iota(jnp.int32, (rows, cols), 1)
    return jnp.where(lax.shift_right_logical(j, 1) + offset == k, 1.0, 0.0).astype(F32)


def copy_matrix(rows, cols, shift):
    k = lax.broadcasted_iota(jnp.int32, (rows, cols), 0)
    j = lax.broadcasted_iota(jnp.int32, (rows, cols), 1)
    return jnp.where(lax.shift_right_logical(j, shift) == k, 1.0, 0.0).astype(F32)


class Grid:
    def __init__(self, planes, rows, lanes):
        self.planes, self.rows, self.lanes = planes, rows, lanes
        self.row = lax.broadcasted_iota(jnp.int32, (rows, lanes), 0)
        self.lane = lax.broadcasted_iota(jnp.int32, (rows, lanes), 1)
        self.even = jnp.bitwise_and(self.row + self.lane, 1) == 0
        self.odd = jnp.bitwise_and(self.row + self.lane, 1) == 1

    def colour(self, x, colour):
        return self.even if (x + colour) % 2 == 0 else self.odd


class Halo:
    def __init__(self, grid, refs, iz):
        self.grid, self.iz = grid, iz
        self.xs, self.ys, self.zs, self.xh, self.yh, self.zh = refs
        self.flane = lax.broadcasted_iota(jnp.int32, (grid.rows, LANES), 1)

    def faces(self, slot, planes):
        g = self.grid
        acc = jnp.zeros((g.rows, LANES), F32)
        for x, val in planes:
            self.ys[0, slot, x : x + 1, :] = val[0:1]
            self.ys[1, slot, x : x + 1, :] = val[g.rows - 1 :]
            if g.lanes > LANES:
                end = jnp.where(self.iz == 0, val[:, g.lanes - LANES :], val[:, :LANES])
            else:
                end = val
            acc = jnp.where(self.flane == x, pltpu.roll(end, x + 1 - self.iz, 1), acc)
            yield
        self.zs[slot] = acc

    def put_ends(self, slot, ref):
        self.xs[0, slot] = ref[0]
        self.xs[1, slot] = ref[self.grid.planes - 1]

    def put_rest(self, slot, ref):
        for _ in self.faces(slot, [(x, ref[x]) for x in range(self.grid.planes)]):
            pass

    def put(self, slot, ref):
        self.put_ends(slot, ref)
        self.put_rest(slot, ref)

    def neighbours(self, slot, planes, x, edge=False):
        g = self.grid
        val = planes(x)
        xm = planes(x - 1) if x > 0 else self.xh[0, slot]
        xp = planes(x + 1) if x < g.planes - 1 else self.xh[1, slot]
        shape = (g.rows, g.lanes)
        low = jnp.broadcast_to(self.yh[0, slot, x : x + 1, :], shape)
        high = jnp.broadcast_to(self.yh[1, slot, x : x + 1, :], shape)
        ym = jnp.where(g.row == 0, low, pltpu.roll(val, 1, 0))
        yp = jnp.where(g.row == g.rows - 1, high, pltpu.roll(val, g.rows - 1, 0))
        side = jnp.broadcast_to(self.zh[slot, :, x : x + 1], shape)
        side_m, side_p = side, side
        if edge:
            side_m = jnp.where(self.iz == 0, 0.0, side)
            side_p = jnp.where(self.iz == 0, side, 0.0)
        zm = jnp.where(g.lane == 0, side_m, pltpu.roll(val, 1, 1))
        zp = jnp.where(g.lane == g.lanes - 1, side_p, pltpu.roll(val, g.lanes - 1, 1))
        return val, (xm, xp, ym, yp, zm, zp)


def halve_rows(tmp, slot, val):
    rows, lanes = val.shape
    parts = []
    for k in range(lanes // LANES):
        at = 2 * slot + k
        tmp[at, 0:rows, :] = val[:, k * LANES : (k + 1) * LANES]
        parts.append(tmp[at, pl.ds(0, rows // 2, 2), :] + tmp[at, pl.ds(1, rows // 2, 2), :])
    return parts[0] if len(parts) == 1 else jnp.concatenate(parts, axis=1)


def double_rows(tmp, slot, val):
    rows, lanes = val.shape
    parts = []
    for k in range(lanes // LANES):
        at = 2 * slot + k
        piece = val[:, k * LANES : (k + 1) * LANES]
        tmp[at, pl.ds(0, rows, 2), :] = piece
        tmp[at, pl.ds(1, rows, 2), :] = piece
        parts.append(tmp[at, 0 : 2 * rows, :])
    return parts[0] if len(parts) == 1 else jnp.concatenate(parts, axis=1)


def kernel(counts, *refs):
    sources, (mem_out, rec_out, ext_out) = refs[:5], refs[5:8]
    refs = refs[8:]
    mem, rec, ext, fib, lab, in_sem = refs[:6]
    refs = (None,) + refs
    (xs0, ys0, zs0, xh0, yh0, zh0) = refs[7:13]
    (in0, out0, uu, w0, c0, d0, b0, va, vb, tmp, tall) = refs[13:24]
    (ee, ys1, yr1, zs1, zr1, zp1, c1, cz1, d1, b1, v1a, v1b, z1a, z1b, yrim) = refs[24:39]
    (gc_own, gc, gr_own, gr, in2, out2, c2, d2, b2, v2a, v2b) = refs[39:50]
    (c3, b3, v3, k3, h3, send_sem, recv_sem, wide_send, wide_recv, gs_sem, gr_sem) = refs[50:]
    nx, ny, nz = counts
    ix, iy, iz = lax.axis_index("gx"), lax.axis_index("gy"), lax.axis_index("gz")
    me = (ix * ny + iy) * nz + iz
    total = nx * ny * nz

    loads = [
        pltpu.make_async_copy(src, dst, in_sem.at[i])
        for i, (src, dst) in enumerate(zip(sources, (mem, rec, ext, fib, lab)))
    ]
    for i in (4, 3, 0, 2, 1):
        loads[i].start()

    barrier = pltpu.get_barrier_semaphore()

    def others(body):
        def step(i, carry):
            dev = lax.rem(me + i, total)
            body(dev, (dev // (ny * nz), lax.rem(dev // nz, ny), lax.rem(dev, nz)))
            return carry

        lax.fori_loop(1, total, step, 0)

    others(lambda dev, where: pl.semaphore_signal(barrier, inc=1, device_id=where, device_id_type=MESH))

    def clear(missing, ref, side):
        def fill():
            ref[side] = jnp.zeros(ref.at[side].shape, F32)

        pl.when(missing)(fill)

    X1, R1, Z1 = mem.shape[0] // 2, mem.shape[1] // 2, mem.shape[2] // 2
    XE, RE = X1 + 2 * GHOST, R1 + 2 * GHOST
    clear(ix == 0, xh0, 0)
    clear(ix == nx - 1, xh0, 1)
    clear(iy == 0, yh0, 0)
    clear(iy == ny - 1, yh0, 1)
    for slot in range(3):
        for p in range(GHOST):
            clear(ix == 0, ee, (slot, p))
            clear(ix == nx - 1, ee, (slot, XE - 1 - p))
    for load in loads:
        load.wait()

    g0 = Grid(*mem.shape)
    g1 = Grid(XE, RE, Z1)
    halo0 = Halo(g0, (xs0, ys0, zs0, xh0, yh0, zh0), iz)

    def copies(number):
        first, slots = EXCHANGES[number]
        h = halo0
        part = pl.ds(first, slots)
        plan = (
            (h.xs.at[0, part], h.xh.at[1, part], (ix - 1, iy, iz), ix > 0, ix < nx - 1),
            (h.xs.at[1, part], h.xh.at[0, part], (ix + 1, iy, iz), ix < nx - 1, ix > 0),
            (h.ys.at[0, part], h.yh.at[1, part], (ix, iy - 1, iz), iy > 0, iy < ny - 1),
            (h.ys.at[1, part], h.yh.at[0, part], (ix, iy + 1, iz), iy < ny - 1, iy > 0),
            (h.zs.at[part], h.zh.at[part], (ix, iy, 1 - iz), None, None),
        )
        for side, (src, dst, dev, goes, comes) in enumerate(plan):
            copy = pltpu.make_async_remote_copy(
                src_ref=src,
                dst_ref=dst,
                send_sem=send_sem.at[number * SIDES + side],
                recv_sem=recv_sem.at[number * SIDES + side],
                device_id=dev,
                device_id_type=MESH,
            )
            yield copy, goes, comes

    ends, rest = slice(0, 2), slice(2, SIDES)

    def send(number, sides=slice(0, SIDES)):
        for copy, goes, _ in list(copies(number))[sides]:
            if goes is None:
                copy.start()
            else:
                pl.when(goes)(copy.start)

    def arrive(number, sides=slice(0, SIDES)):
        for copy, _, comes in list(copies(number))[sides]:
            if comes is None:
                copy.wait_recv()
            else:
                pl.when(comes)(copy.wait_recv)

    def inner_first(number, count):
        arrive(number, rest)
        yield from range(1, count - 1)
        arrive(number, ends)
        yield 0
        yield count - 1

    def publish(number, halo, slot, ref):
        halo.put_ends(slot, ref)
        send(number, ends)
        halo.put_rest(slot, ref)
        send(number, rest)

    def sent(number):
        for copy, goes, _ in copies(number):
            if goes is None:
                copy.wait_send()
            else:
                pl.when(goes)(copy.wait_send)

    here = {-1: ix > 0, 0: None, 1: ix < nx - 1}
    along = {-1: iy > 0, 0: None, 1: iy < ny - 1}

    def both(a, b):
        if a is None or b is None:
            return b if a is None else a
        return jnp.logical_and(a, b)

    def wide_copies(number):
        first, count = WIDE[number]
        part = pl.ds(first, count)
        pairs, edge = X1 // 2, GHOST // 2
        plan = []
        for sx in (-1, 1):
            src = ee.at[part, pl.ds(GHOST if sx < 0 else X1, GHOST), pl.ds(0, R1)]
            dst = ee.at[part, pl.ds(X1 + GHOST if sx < 0 else 0, GHOST), pl.ds(0, R1)]
            plan.append((src, dst, sx, 0, iz))
        for sx in STEPS:
            for sy in (-1, 1):
                mine, theirs = (0, 1) if sy < 0 else (1, 0)
                at = {-1: (0, edge, pairs + edge), 0: (0, pairs, edge), 1: (pairs - edge, edge, 0)}[sx]
                src = ys1.at[mine, part, pl.ds(at[0], at[1])]
                dst = yr1.at[theirs, part, pl.ds(at[2], at[1])]
                plan.append((src, dst, sx, sy, iz))
        for sx in STEPS:
            for sy in STEPS:
                plan.append((zs1.at[part], zr1.at[(1 - sx) * 3 + 1 - sy, part], sx, sy, 1 - iz))
        for side, (src, dst, sx, sy, z) in enumerate(plan):
            copy = pltpu.make_async_remote_copy(
                src_ref=src,
                dst_ref=dst,
                send_sem=wide_send.at[number * WIDE_SIDES + side],
                recv_sem=wide_recv.at[number * WIDE_SIDES + side],
                device_id=(ix + sx, iy + sy, z),
                device_id_type=MESH,
            )
            yield copy, both(here[sx], along[sy]), both(here[-sx], along[-sy])

    def maybe(condition, action):
        if condition is None:
            action()
        else:
            pl.when(condition)(action)

    tile_row = lax.broadcasted_iota(jnp.int32, (8, LANES), 0)
    tile_lane = lax.broadcasted_iota(jnp.int32, (8, LANES), 1)

    def wide_publish(number):
        first, count = WIDE[number]
        for slot in range(first, first + count):
            acc = jnp.zeros((R1, LANES), F32)
            for x in range(X1):
                val = ee[slot, GHOST + x, 0:R1, :]
                for depth in range(GHOST):
                    at = depth * XE + GHOST + x
                    shift = jnp.where(iz == 0, at + 1 + depth, at - depth)
                    acc = jnp.where(tile_lane == at, pltpu.roll(val, shift, 1), acc)
            zs1[slot] = acc
            for k in range(X1 // 2):
                even, odd = ee[slot, GHOST + 2 * k, 0:R1, :], ee[slot, GHOST + 2 * k + 1, 0:R1, :]
                ys1[0, slot, k] = jnp.where(tile_row < GHOST, even, pltpu.roll(odd, GHOST, 0))
                ys1[1, slot, k] = jnp.where(tile_row < GHOST, pltpu.roll(odd, GHOST, 0), even)
        for copy, goes, _ in wide_copies(number):
            maybe(goes, copy.start)

    def keep(condition, val):
        return val if condition is None else jnp.where(condition, val, 0.0)

    def plane_side(p):
        return here[-1 if p < GHOST else (1 if p >= X1 + GHOST else 0)]

    def wide_arrive(number):
        first, count = WIDE[number]
        for copy, _, comes in wide_copies(number):
            maybe(comes, copy.wait_recv)
        low = tile_row >= GHOST
        pe = jnp.bitwise_and(tile_lane, XE - 1)
        for slot in range(first, first + count):
            for p in range(XE):
                after, before = yr1[1, slot, p // 2], yr1[0, slot, p // 2]
                if p % 2:
                    after, before = pltpu.roll(after, GHOST, 0), pltpu.roll(before, GHOST, 0)
                side = plane_side(p)
                after = keep(both(side, along[1]), after)
                before = keep(both(side, along[-1]), before)
                ee[slot, p, R1:RE, :] = jnp.where(low, before, after)
            rows = []
            for sy in STEPS:
                mid = zr1[3 + sy + 1, slot]
                left = keep(here[-1], pltpu.roll(zr1[sy + 1, slot], LANES - X1, 1))
                right = keep(here[1], pltpu.roll(zr1[6 + sy + 1, slot], X1, 1))
                val = jnp.where(pe < GHOST, left, jnp.where(pe >= X1 + GHOST, right, mid))
                rows.append(keep(along[sy], jnp.where(tile_lane < GHOST * XE, val, 0.0)))
            zp1[slot, 0:R1, :] = rows[1]
            zp1[slot, R1:RE, :] = jnp.where(low, rows[0], rows[2])

    def wide_sent(number):
        for copy, goes, _ in wide_copies(number):
            maybe(goes, copy.wait_send)

    def gather_send(own, whole, which):
        def go(dev, where):
            pltpu.make_async_remote_copy(
                src_ref=own,
                dst_ref=whole.at[me],
                send_sem=gs_sem.at[which],
                recv_sem=gr_sem.at[which],
                device_id=where,
                device_id_type=MESH,
            ).start()

        others(go)
        whole[pl.ds(me, 1)] = own[...][None]

    def gather_wait(whole, which, recv):
        rest = whole.at[pl.ds(0, total - 1)]
        copy = pltpu.make_async_remote_copy(
            src_ref=rest,
            dst_ref=rest,
            send_sem=gs_sem.at[which],
            recv_sem=gr_sem.at[which],
            device_id=(ix, iy, 1 - iz),
            device_id_type=MESH,
        )
        if recv:
            copy.wait_recv()
        else:
            copy.wait_send()

    X0, R0, Z0 = mem.shape
    X2 = X1 // 2
    R2 = R1 // 2
    half = Z1 // 2

    widen8 = copy_matrix(lab.shape[2], Z0, 3)
    lab_planes = []
    for bx in range(lab.shape[0]):
        wide = jnp.dot(lab[bx].astype(F32), widen8, preferred_element_type=F32)
        lab_planes.append(
            jnp.concatenate(
                [jnp.broadcast_to(wide[by : by + 1], (8, Z0)) for by in range(lab.shape[1])], axis=0
            )
        )

    def label_of(x):
        return lab_planes[x // 8]

    for x in range(X0):
        label = label_of(x)
        in0[x] = jnp.where(label == 1.0, 1.0, jnp.where(label == 2.0, 0.3, 0.0)) * fib[x]
        out0[x] = jnp.where(label == 0.0, 3.0, 1.0)
        uu[x] = mem[x] + ext[x]
    halo0.put(INNER, in0)
    halo0.put(U, uu)
    pl.semaphore_wait(barrier, total - 1)
    send(0)
    halo0.put(OUTER, out0)
    halo0.put(V, ext)
    send(1)

    narrow = pair_matrix(Z0, Z1, 0)
    narrow_low = pair_matrix(Z1, Z1, 0)
    narrow_high = pair_matrix(Z1, Z1, half)
    double01 = copy_matrix(Z1, Z0, 1)
    double12 = copy_matrix(Z1, Z1, 1)

    def restrict0(plane, factor, base, order=None):
        for x in order or range(X1):
            tall[base + x * R1 : base + (x + 1) * R1, :] = halve_rows(tmp, x, plane(2 * x) + plane(2 * x + 1))
        whole = dot(tall[base : base + X1 * R1, :], narrow) * factor
        return [whole[x * R1 : (x + 1) * R1] for x in range(X1)]

    def restrict1(plane, factor, order=None):
        rows = [None] * X2
        for x in order or range(X2):
            rows[x] = halve_rows(tmp, x, plane(2 * x) + plane(2 * x + 1))
        low = jnp.concatenate(rows[: X2 // 2], axis=0)
        high = jnp.concatenate(rows[X2 // 2 :], axis=0)
        return (dot(low, narrow_low) + dot(high, narrow_high)) * factor

    for x, val in enumerate(restrict0(lambda x: in0[x], 0.125, 0)):
        ee[INNER1, GHOST + x, 0:R1, :] = val
    for x, val in enumerate(restrict0(lambda x: out0[x], 0.125, 0)):
        ee[OUTER1, GHOST + x, 0:R1, :] = val
    wide_publish(0)
    gc_own[0] = restrict1(lambda x: ee[INNER1, GHOST + x, 0:R1, :], 0.125)
    gc_own[1] = restrict1(lambda x: ee[OUTER1, GHOST + x, 0:R1, :], 0.125)
    gather_send(gc_own, gc, 0)

    for x in inner_first(0, X0):
        centre, near = halo0.neighbours(INNER, lambda x: in0[x], x, edge=True)
        u, near_u = halo0.neighbours(U, lambda x: uu[x], x)
        drive = jnp.zeros_like(u)
        for d in range(6):
            weight = jnp.minimum(centre, near[d])
            w0[d, x] = weight
            drive = drive + weight * (near_u[d] - u)
        m, r = mem[x], rec[x]
        tissue = jnp.where(label_of(x) != 0.0, 1.0, 0.0)
        ionic = ionic_gain * m * (m - ionic_onset) * (m - 1.0) + m * r
        mem_out[x] = m + TIME_STEP * (drive - tissue * ionic)
    publish(2, halo0, NEXT, mem_out)
    for x in range(X0):
        m, r = mem[x], rec[x]
        rec_out[x] = r + TIME_STEP * recovery_rate * (-r - ionic_gain * m * (m - ionic_onset - 1.0))

    def scaled(grid, weights, centre, near, iz_edges):
        full = [weights[d] + 0.5 * (centre + near[d]) for d in range(6)]
        diag = ((full[0] + full[1]) + (full[2] + full[3])) + (full[4] + full[5])
        inv = 1.0 / diag
        full = [f * inv for f in full]
        low, high = iz_edges
        full[4] = jnp.where(low, 0.0, full[4])
        full[5] = jnp.where(high, 0.0, full[5])
        return full, diag, inv

    first0 = (g0.lane == 0) & (iz == 0)
    last0 = (g0.lane == Z0 - 1) & (iz == nz - 1)
    arrive(1)
    inv0 = vb
    for x in range(X0):
        centre, near = halo0.neighbours(OUTER, lambda x: out0[x], x, edge=True)
        full, diag, inv = scaled(g0, [w0[d, x] for d in range(6)], centre, near, (first0, last0))
        for d in range(6):
            c0[d, x] = full[d]
        d0[x] = diag
        b0[x] = inv

    def update(halo, slot, planes, c, b, x):
        val, near = halo.neighbours(slot, planes, x)
        a = b[x] + c[0, x] * near[0]
        e = c[1, x] * near[1] + c[2, x] * near[2]
        f = c[3, x] * near[3] + c[4, x] * near[4]
        return val, (a + c[5, x] * near[5]) + (e + f)

    def half_sweep(number, halo, slot, src, dst, c, b, colour):
        planes = halo.grid.planes
        for x in range(planes) if number is None else inner_first(number, planes):
            val, new = update(halo, slot, lambda x: src[x], c, b, x)
            dst[x] = jnp.where(halo.grid.colour(x, colour), new, val)

    for x in inner_first(2, X0):
        m, near = halo0.neighbours(NEXT, lambda x: mem_out[x], x)
        rhs = jnp.zeros_like(m)
        for d in range(6):
            rhs = rhs + w0[d, x] * (near[d] - m)
        b0[x] = rhs * b0[x]
        val, new = update(halo0, V, lambda x: ext[x], c0, b0, x)
        va[x] = jnp.where(g0.colour(x, 0), new, val)
    publish(3, halo0, RED, va)

    first1 = (g1.lane == 0) & (iz == 0)
    last1 = (g1.lane == Z1 - 1) & (iz == nz - 1)
    pack_row = lax.broadcasted_iota(jnp.int32, (RE, LANES), 0)
    pack_lane = lax.broadcasted_iota(jnp.int32, (RE, LANES), 1)
    pack_x = jnp.bitwise_and(pack_lane, XE - 1)
    depth_parity = lax.div(pack_lane, XE) + iz + pack_x + pack_row
    pack_own = [jnp.bitwise_and(depth_parity + colour, 1) == 0 for colour in range(2)]

    def row_inside(row):
        return (
            (row < R1)
            | ((row < R1 + GHOST) & (iy < ny - 1))
            | ((row >= R1 + GHOST) & (iy > 0))
        )

    inside_row = row_inside(g1.row)
    pack_inside = (
        row_inside(pack_row)
        & (pack_lane < GHOST * XE)
        & ((pack_x >= GHOST) | (ix > 0))
        & ((pack_x < X1 + GHOST) | (ix < nx - 1))
    )

    def inside1(p):
        side = plane_side(p)
        return inside_row if side is None else inside_row & side

    def near1(planes, pack, p, edge=False):
        val = planes(p)
        side = jnp.broadcast_to(pack(p), (RE, Z1))
        side_m, side_p = side, side
        if edge:
            side_m = jnp.where(iz == 0, 0.0, side)
            side_p = jnp.where(iz == 0, side, 0.0)
        return val, (
            planes(p - 1),
            planes(p + 1),
            pltpu.roll(val, 1, 0),
            pltpu.roll(val, RE - 1, 0),
            jnp.where(g1.lane == 0, side_m, pltpu.roll(val, 1, 1)),
            jnp.where(g1.lane == Z1 - 1, side_p, pltpu.roll(val, Z1 - 1, 1)),
        )

    def near_pack(planes, val, first, last):
        own = jnp.zeros((RE, LANES), F32)
        for p in range(first, last):
            own = jnp.where(pack_lane == p, pltpu.roll(planes(p), p + 1 - iz, 1), own)
        return (
            pltpu.roll(val, 1, 1),
            pltpu.roll(val, LANES - 1, 1),
            pltpu.roll(val, 1, 0),
            pltpu.roll(val, RE - 1, 0),
            jnp.where(pack_lane < XE, own, pltpu.roll(val, XE, 1)),
            pltpu.roll(val, LANES - XE, 1),
        )

    def scaled_wide(ci, ni, co, no, inside):
        full = [jnp.minimum(ci, ni[k]) + 0.5 * (co + no[k]) for k in range(6)]
        diag = ((full[0] + full[1]) + (full[2] + full[3])) + (full[4] + full[5])
        inv = jnp.where(inside, 1.0 / diag, 0.0)
        return [jnp.where(inside, f * inv, 0.0) for f in full], diag, inv

    wide_arrive(0)
    for p in range(1, XE - 1):
        ci, ni = near1(lambda p: ee[INNER1, p], lambda p: zp1[INNER1, :, p : p + 1], p, edge=True)
        co, no = near1(lambda p: ee[OUTER1, p], lambda p: zp1[OUTER1, :, p : p + 1], p, edge=True)
        full, diag, inv = scaled_wide(ci, ni, co, no, inside1(p))
        full[4] = jnp.where(first1, 0.0, full[4])
        full[5] = jnp.where(last1, 0.0, full[5])
        for d in range(6):
            c1[d, p] = full[d]
        if GHOST <= p < X1 + GHOST:
            d1[p - GHOST] = diag[0:R1]
            b1[p - GHOST] = inv[0:R1]
    ci, co = zp1[INNER1], zp1[OUTER1]
    full, _, _ = scaled_wide(
        ci,
        near_pack(lambda p: ee[INNER1, p], ci, 0, XE),
        co,
        near_pack(lambda p: ee[OUTER1, p], co, 0, XE),
        pack_inside,
    )
    for d in range(6):
        cz1[d] = full[d]

    def stencil(b, c, near):
        a = b + c(0) * near[0]
        e = c(1) * near[1] + c(2) * near[2]
        f = c(3) * near[3] + c(4) * near[4]
        return (a + c(5) * near[5]) + (e + f)

    def update1(src, pack, p):
        val, near = near1(lambda p: src[p], lambda p: pack[:, p : p + 1], p)
        return val, stencil(ee[RHS1, p], lambda d: c1[d, p], near)

    def half1(src, pack, dst, colour, planes):
        for p in planes:
            val, new = update1(src, pack, p)
            dst[p] = jnp.where(g1.colour(p, colour), new, val)

    def half_pack(src, pack, dst, colour, first, last):
        val = pack[...]
        near = near_pack(lambda p: src[p], val, first, last)
        new = stencil(zp1[RHS1], lambda d: cz1[d], near)
        dst[...] = jnp.where(pack_own[colour], new, val)

    half_sweep(3, halo0, RED, va, vb, c0, b0, 1)
    publish(4, halo0, BLACK, vb)

    XG, RG, ZG = in2.shape
    XH, RH = XG // 2, RG // 2
    g2 = Grid(XG, RG, ZG)
    g3 = Grid(XH, RH, ZG)
    def unpack(tile, dst):
        for px in range(nx):
            for py in range(ny // 2):
                lows, highs = [], []
                for part in range(2):
                    base = (px * ny + 2 * py + part) * nz
                    s0, s1 = tile(base), tile(base + 1)
                    lows.append(jnp.where(tile_lane < half, s0, pltpu.roll(s1, half, 1)))
                    highs.append(jnp.where(tile_lane < half, pltpu.roll(s0, half, 1), s1))
                for xhi, pair in enumerate((lows, highs)):
                    p = px * X2 + xhi * 2
                    dst[p, py * 8 : py * 8 + 8, :] = jnp.where(tile_row < R2, pair[0], pltpu.roll(pair[1], R2, 0))
                    dst[p + 1, py * 8 : py * 8 + 8, :] = jnp.where(
                        tile_row < R2, pltpu.roll(pair[0], R2, 0), pair[1]
                    )

    def whole_neighbours(grid, planes, x, last, mask):
        val = planes(x)
        zero = jnp.zeros_like(val)
        xm = planes(x - 1) if x > 0 else zero
        xp = planes(x + 1) if x < grid.planes - 1 else zero
        near = [
            xm,
            xp,
            pltpu.roll(val, 1, 0),
            pltpu.roll(val, grid.rows - 1, 0),
            pltpu.roll(val, 1, 1),
            pltpu.roll(val, grid.lanes - 1, 1),
        ]
        if mask:
            near[2] = jnp.where(grid.row == 0, 0.0, near[2])
            near[3] = jnp.where(grid.row == grid.rows - 1, 0.0, near[3])
            near[4] = jnp.where(grid.lane == 0, 0.0, near[4])
            near[5] = jnp.where(grid.lane >= last, 0.0, near[5])
        return val, near

    def whole_couplings(grid, inner, outer, last, c, d, b):
        for x in range(grid.planes):
            ci, ni = whole_neighbours(grid, lambda x: inner[x], x, last, True)
            co, no = whole_neighbours(grid, lambda x: outer[x], x, last, True)
            full = [jnp.minimum(ci, ni[k]) + 0.5 * (co + no[k]) for k in range(6)]
            diag = ((full[0] + full[1]) + (full[2] + full[3])) + (full[4] + full[5])
            if last < grid.lanes - 1:
                diag = jnp.where(grid.lane <= last, diag, 1.0)
            inv = 1.0 / diag
            edges = (
                None,
                None,
                grid.row == 0,
                grid.row == grid.rows - 1,
                grid.lane == 0,
                grid.lane >= last,
            )
            for k in range(6):
                f = full[k] * inv
                if edges[k] is not None:
                    f = jnp.where(edges[k], 0.0, f)
                if last < grid.lanes - 1:
                    f = jnp.where(grid.lane <= last, f, 0.0)
                c[k, x] = f
            if d is not None:
                d[x] = diag
            b[x] = inv

    def whole_update(grid, planes, c, b, x):
        val, near = whole_neighbours(grid, planes, x, None, False)
        a = b[x] + c[2, x] * near[2]
        e = c[3, x] * near[3] + c[4, x] * near[4]
        a = a + c[5, x] * near[5]
        if x > 0:
            a = a + c[0, x] * near[0]
        if x < grid.planes - 1:
            e = e + c[1, x] * near[1]
        return val, a + e

    def restrict2(plane, factor):
        pieces = [halve_rows(tmp, x, plane(2 * x) + plane(2 * x + 1)) for x in range(XH)]
        for x in range(XH):
            tall[x * RH : (x + 1) * RH, 0:ZG] = pieces[x]
        whole = dot(tall[0 : XH * RH, 0:ZG], narrow_low) * factor
        return [whole[x * RH : (x + 1) * RH] for x in range(XH)]

    gather_wait(gc, 0, True)
    unpack(lambda t: gc[t, 0], in2)
    unpack(lambda t: gc[t, 1], out2)
    whole_couplings(g2, in2, out2, ZG - 1, c2, d2, b2)
    for x, val in enumerate(restrict2(lambda x: in2[x], 0.125)):
        v3[x] = val
    for x, val in enumerate(restrict2(lambda x: out2[x], 0.125)):
        v2a[x, 0:RH] = val
    whole_couplings(g3, v3, v2a.at[:, 0:RH], ZG // 2 - 1, c3, None, b3)

    XP = XH // 2
    own = (g3.even, g3.odd)

    def pack(colour, near, far):
        return jnp.where(own[colour], near, far)

    for colour in range(2):
        for p in range(XP):
            a, z = 2 * p, 2 * p + 1
            k3[colour * 6, p] = pack(colour, c3[1, a], c3[0, z])
            k3[colour * 6 + 1, p] = pack(colour, c3[0, a], c3[1, z])
            for k in range(2, 6):
                k3[colour * 6 + k, p] = pack(colour, c3[k, a], c3[k, z])

    def residual0(x):
        val, new = update(halo0, BLACK, lambda x: vb[x], c0, b0, x)
        return d0[x] * (new - val)

    for x, val in enumerate(restrict0(residual0, 0.5, 0, inner_first(4, X1))):
        ee[RHS1, GHOST + x, 0:R1, :] = val * b1[x]
    wide_publish(1)
    wide_arrive(1)
    ring = GHOST - 1
    for p in range(ring - 1, XE - ring + 1):
        v1a[p] = jnp.where(g1.colour(p, 0), ee[RHS1, p], 0.0)
    z1a[...] = jnp.where(pack_own[0], zp1[RHS1], 0.0)
    half_pack(v1a, z1a, z1b, 1, ring, XE - ring)
    half1(v1a, z1a, v1b, 1, range(ring, XE - ring))

    def residual1(x):
        val, new = update1(v1b, z1b, GHOST + x)
        return d1[x] * (new - val)[0:R1]

    gr_own[...] = restrict1(residual1, 0.5)
    gather_send(gr_own, gr, 1)
    for p in (0, 1, XE - 2, XE - 1):
        v1a[p] = jnp.where(g1.colour(p, 0), ee[RHS1, p], 0.0)
    half_pack(v1a, z1a, z1b, 1, 0, XE)
    half1(v1a, z1a, v1b, 1, (1, 2, XE - 3, XE - 2))
    gather_wait(gr, 1, True)
    unpack(lambda t: gr[t], v2b)
    for x in range(XG):
        b2[x] = v2b[x] * b2[x]
        v2a[x] = jnp.where(g2.colour(x, 0), b2[x], 0.0)
    for x in range(XG):
        val, new = whole_update(g2, lambda x: v2a[x], c2, b2, x)
        v2b[x] = jnp.where(g2.colour(x, 1), new, val)

    def residual2(x):
        val, new = whole_update(g2, lambda x: v2b[x], c2, b2, x)
        return d2[x] * (new - val)

    for x, val in enumerate(restrict2(residual2, 0.5)):
        b3[x] = val * b3[x]

    for colour in range(2):
        for p in range(XP):
            h3[colour, p] = pack(colour, b3[2 * p], b3[2 * p + 1])
    none = jnp.zeros((RH, ZG), F32)

    def relaxed(colour, other):
        fresh = []
        for p in range(XP):
            val, at = other[p], colour * 6
            before = other[p - 1] if p > 0 else none
            after = other[p + 1] if p < XP - 1 else none
            i = h3[colour, p] + k3[at, p] * val
            j = k3[at + 1, p] * pack(colour, before, after) + k3[at + 2, p] * pltpu.roll(val, 1, 0)
            l = k3[at + 3, p] * pltpu.roll(val, RH - 1, 0) + k3[at + 4, p] * pltpu.roll(val, 1, 1)
            fresh.append((i + k3[at + 5, p] * pltpu.roll(val, ZG - 1, 1)) + (j + l))
        return fresh

    def coarse(step, state):
        red = relaxed(0, state[XP:])
        black = relaxed(1, red)
        return tuple(red + black)

    state = lax.fori_loop(0, COARSE_SWEEPS, coarse, (none,) * (2 * XP))
    solved = []
    for p in range(XP):
        solved.append(pack(0, state[p], state[XP + p]))
        solved.append(pack(1, state[p], state[XP + p]))
    for x in range(XH):
        tall[x * RH : (x + 1) * RH, 0:ZG] = solved[x]
    wide = dot(tall[0 : XH * RH, 0:ZG], double12)
    for x in range(XH):
        corr = double_rows(tmp, x, wide[x * RH : (x + 1) * RH])
        v2a[2 * x] = v2b[2 * x] + corr
        v2a[2 * x + 1] = v2b[2 * x + 1] + corr
    for colour, src, dst in ((0, v2a, v2b), (1, v2b, v2a)):
        for x in range(XG):
            val, new = whole_update(g2, lambda x: src[x], c2, b2, x)
            dst[x] = jnp.where(g2.colour(x, colour), new, val)

    row_shift = lax.rem(RG - iy * R2, RG)
    lane_shift = lax.rem(ZG - iz * half, ZG)
    edge2 = GHOST // 2
    rows2 = R2 + 2 * edge2
    planes2 = X2 + 2 * edge2
    for k in range(planes2):
        part = v2a[jnp.clip(ix * X2 + k - edge2, 0, XG - 1)]
        part = pltpu.roll(pltpu.roll(part, row_shift, 0), lane_shift, 1)
        tall[k * rows2 : (k + 1) * rows2, 0:ZG] = jnp.where(
            tile_row < R2 + edge2, part[0:rows2], part[RG - rows2 : RG]
        )
    source = lax.broadcasted_iota(jnp.int32, (ZG, LANES), 0)
    target = lax.broadcasted_iota(jnp.int32, (ZG, LANES), 1)
    target = lax.div(target, 2 * XE)
    pick = jnp.where(source == jnp.where(iz == 0, half + target, ZG - 1 - target), 1.0, 0.0).astype(F32)
    coarse_rows = tall[0 : planes2 * rows2, 0:ZG]
    wide = dot(coarse_rows, double12)
    sides = dot(coarse_rows, pick)
    acc = jnp.zeros((rows2, LANES), F32)
    tile_plane = lax.div(jnp.bitwise_and(tile_lane, XE - 1), 2)
    for k in range(planes2):
        acc = jnp.where(tile_plane == k, sides[k * rows2 : (k + 1) * rows2], acc)
    z1a[...] = z1b[...] + jnp.where(pack_inside, double_rows(tmp, 0, acc), 0.0)
    for k in range(planes2):
        corr = double_rows(tmp, k, wide[k * rows2 : (k + 1) * rows2])
        for p in (2 * k, 2 * k + 1):
            if 0 < p < XE - 1:
                v1a[p] = v1b[p] + jnp.where(inside1(p), corr, 0.0)
    half_pack(v1a, z1a, z1b, 0, 1, XE - 1)
    half1(v1a, z1a, v1b, 0, range(2, XE - 2))
    half_pack(v1b, z1b, z1a, 1, 2, XE - 2)
    half1(v1b, z1b, v1a, 1, range(3, XE - 3))

    def enlarge(count, read, write):
        for x in range(count):
            tall[x * R1 : (x + 1) * R1, 0:Z1] = read(x)
        wide = dot(tall[0 : count * R1, 0:Z1], double01)
        for x in range(count):
            write(x, double_rows(tmp, x, wide[x * R1 : (x + 1) * R1]))

    def inside(x, corr):
        va[2 * x] = vb[2 * x] + corr
        va[2 * x + 1] = vb[2 * x + 1] + corr

    enlarge(X1, lambda x: v1a[GHOST + x, 0:R1, :], inside)
    for x in range(X1):
        yrim[0, x : x + 1, :] = v1a[GHOST + x, RE - 1 : RE, :]
        yrim[1, x : x + 1, :] = v1a[GHOST + x, R1 : R1 + 1, :]

    def rim(k):
        if k < 2:
            return v1a[GHOST - 1 if k == 0 else X1 + GHOST, 0:R1, :]
        if k < 4:
            return yrim[k - 2]
        return pltpu.roll(z1a[0:R1, :], LANES - GHOST, 1)

    def outside(k, corr):
        if k < 2:
            xh0[k, FIXED] = xh0[k, BLACK] + corr
        elif k < 4:
            yh0[k - 2, FIXED] = yh0[k - 2, BLACK] + corr
        else:
            zh0[FIXED] = zh0[BLACK] + corr[:, 0:LANES]

    enlarge(5, rim, outside)
    half_sweep(None, halo0, FIXED, va, vb, c0, b0, 0)
    publish(5, halo0, LAST, vb)
    half_sweep(5, halo0, LAST, vb, ext_out, c0, b0, 1)

    for number in range(len(EXCHANGES)):
        sent(number)
    for number in range(len(WIDE)):
        wide_sent(number)
    gather_wait(gc, 0, False)
    gather_wait(gr, 1, False)


def finish(*refs):
    count = (len(refs) - 1) // 2
    sem = refs[-1]
    copies = [pltpu.make_async_copy(refs[i], refs[count + i], sem.at[i]) for i in range(count)]
    for copy in copies:
        copy.start()
    for copy in copies:
        copy.wait()


def solution(mesh):
    nx, ny, nz = (mesh.shape[a] for a in ("gx", "gy", "gz"))
    spec = P("gx", "gy", "gz")

    def on_device(membrane, recovery, extracellular, fiber_scale, labels):
        X, R, Z = membrane.shape
        X1, R1, Z1 = X // 2, R // 2, Z // 2
        XG, RG, ZG = nx * X // 4, ny * R // 4, nz * Z // 4
        assert nz == 2 and ny % 2 == 0 and ZG == LANES and Z1 == LANES
        assert R1 == 8 and X1 == 8 and X % 8 == 0
        total = nx * ny * nz
        f0 = 9
        field = (X, R, Z)
        lvl1 = (X1, R1, Z1)
        whole = (XG, RG, ZG)
        third = (XG // 2, RG // 2, ZG)

        def v(*shape):
            return pltpu.VMEM(shape, F32)

        def faces(f, x, r, z):
            return [v(2, f, r, z), v(2, f, x, z), v(f, r, LANES)] * 2

        anywhere = pl.BlockSpec(memory_space=pl.ANY)
        scratch = [v(*field)] * 4 + [pltpu.VMEM(labels.shape, jnp.int32), pltpu.SemaphoreType.DMA((5,))]
        scratch += faces(f0, *field)
        scratch += [v(*field), v(*field), v(*field), v(6, *field), v(6, *field), v(*field), v(*field)]
        scratch += [v(*field), v(*field)]
        scratch += [
            v(2 * max(X1, XG // 2), max(R, RG), LANES),
            v(max(X1 * R1, (XG // 2) * (RG // 2), 2 * X1 * R1), Z),
        ]
        XE, RE = X1 + 2 * GHOST, R1 + 2 * GHOST
        assert GHOST * XE <= LANES and 2 * GHOST == R1 and GHOST <= X1
        wide, pack = (XE, RE, Z1), (RE, LANES)
        scratch += [v(3, *wide), v(2, 3, X1 // 2, R1, Z1), v(2, 3, XE // 2, R1, Z1), v(3, R1, LANES)]
        scratch += [v(9, 3, R1, LANES), v(3, *pack), v(6, *wide), v(6, *pack), v(*lvl1), v(*lvl1)]
        scratch += [v(*wide), v(*wide), v(*pack), v(*pack), v(2, X1, Z1)]
        scratch += [v(2, 8, LANES), v(total, 2, 8, LANES), v(8, LANES), v(total, 8, LANES)]
        scratch += [v(*whole), v(*whole), v(6, *whole), v(*whole), v(*whole), v(*whole), v(*whole)]
        scratch += [v(6, *third), v(*third), v(*third)]
        packed = (XG // 4, RG // 2, ZG)
        scratch += [v(12, *packed), v(2, *packed)]
        sems = SIDES * len(EXCHANGES)
        scratch += [pltpu.SemaphoreType.DMA((sems,))] * 2
        scratch += [pltpu.SemaphoreType.DMA((WIDE_SIDES * len(WIDE),))] * 2
        scratch += [pltpu.SemaphoreType.DMA((2,))] * 2
        vmem = pl.BlockSpec(memory_space=pltpu.VMEM)
        room = 54400 << 10
        shape = jax.ShapeDtypeStruct(field, F32)
        results = pl.pallas_call(
            functools.partial(kernel, (nx, ny, nz)),
            out_shape=[shape] * 3,
            in_specs=[anywhere] * 5,
            out_specs=[vmem] * 3,
            scratch_shapes=scratch,
            compiler_params=pltpu.CompilerParams(
                collective_id=0, has_side_effects=True, vmem_limit_bytes=room
            ),
        )(membrane, recovery, extracellular, fiber_scale, labels)
        return tuple(
            pl.pallas_call(
                finish,
                out_shape=[shape] * 3,
                in_specs=[vmem] * 3,
                out_specs=[anywhere] * 3,
                scratch_shapes=[pltpu.SemaphoreType.DMA((3,))],
                compiler_params=pltpu.CompilerParams(vmem_limit_bytes=4 << 20),
            )(*results)
        )

    return jax.shard_map(
        on_device,
        mesh=mesh,
        in_specs=(spec,) * 5,
        out_specs=(spec,) * 3,
        check_vma=False,
    )
```

```python
import functools

import jax
import jax.numpy as jnp
from jax import lax
from jax.experimental import pallas as pl
from jax.experimental.pallas import tpu as pltpu
from jax.sharding import PartitionSpec as P

COARSE_SWEEPS = 8
TIME_STEP = 0.05
ionic_gain = 8.0
ionic_onset = 0.15
recovery_rate = 0.01
MESH = pl.DeviceIdType.MESH
LOGICAL = pl.DeviceIdType.LOGICAL
LANES = 128
F32 = jnp.float32

INNER, U, OUTER, V, NEXT, RED, BLACK, FIXED, LAST = range(9)
INNER1, OUTER1, RHS1 = range(3)
GHOST = 4
EXCHANGES = (
    (INNER, 2),
    (OUTER, 2),
    (NEXT, 1),
    (RED, 1),
    (BLACK, 1),
    (LAST, 1),
)
SIDES = 5
WIDE = ((INNER1, 1), (RHS1, 1))
STEPS = (-1, 0, 1)
WIDE_SIDES = 17


def dot(a, b):
    return jnp.dot(a, b, precision=lax.Precision.HIGHEST, preferred_element_type=F32)


def pair_matrix(rows, cols, offset):
    j = lax.broadcasted_iota(jnp.int32, (rows, cols), 0)
    k = lax.broadcasted_iota(jnp.int32, (rows, cols), 1)
    return jnp.where(lax.shift_right_logical(j, 1) + offset == k, 1.0, 0.0).astype(F32)


def copy_matrix(rows, cols, shift):
    k = lax.broadcasted_iota(jnp.int32, (rows, cols), 0)
    j = lax.broadcasted_iota(jnp.int32, (rows, cols), 1)
    return jnp.where(lax.shift_right_logical(j, shift) == k, 1.0, 0.0).astype(F32)


class Grid:
    def __init__(self, planes, rows, lanes):
        self.planes, self.rows, self.lanes = planes, rows, lanes
        self.row = lax.broadcasted_iota(jnp.int32, (rows, lanes), 0)
        self.lane = lax.broadcasted_iota(jnp.int32, (rows, lanes), 1)
        self.even = jnp.bitwise_and(self.row + self.lane, 1) == 0
        self.odd = jnp.bitwise_and(self.row + self.lane, 1) == 1

    def colour(self, x, colour):
        return self.even if (x + colour) % 2 == 0 else self.odd


class Halo:
    def __init__(self, grid, refs, iz):
        self.grid, self.iz = grid, iz
        self.xs, self.ys, self.zs, self.xh, self.yh, self.zh = refs
        self.flane = lax.broadcasted_iota(jnp.int32, (grid.rows, LANES), 1)

    def faces(self, slot, planes):
        g = self.grid
        acc = jnp.zeros((g.rows, LANES), F32)
        for x, val in planes:
            self.ys[0, slot, x : x + 1, :] = val[0:1]
            self.ys[1, slot, x : x + 1, :] = val[g.rows - 1 :]
            if g.lanes > LANES:
                end = jnp.where(self.iz == 0, val[:, g.lanes - LANES :], val[:, :LANES])
            else:
                end = val
            acc = jnp.where(self.flane == x, pltpu.roll(end, x + 1 - self.iz, 1), acc)
            yield
        self.zs[slot] = acc

    def put_ends(self, slot, ref):
        self.xs[0, slot] = ref[0]
        self.xs[1, slot] = ref[self.grid.planes - 1]

    def put_rest(self, slot, ref):
        for _ in self.faces(slot, [(x, ref[x]) for x in range(self.grid.planes)]):
            pass

    def put(self, slot, ref):
        self.put_ends(slot, ref)
        self.put_rest(slot, ref)

    def neighbours(self, slot, planes, x, edge=False):
        g = self.grid
        val = planes(x)
        xm = planes(x - 1) if x > 0 else self.xh[0, slot]
        xp = planes(x + 1) if x < g.planes - 1 else self.xh[1, slot]
        shape = (g.rows, g.lanes)
        low = jnp.broadcast_to(self.yh[0, slot, x : x + 1, :], shape)
        high = jnp.broadcast_to(self.yh[1, slot, x : x + 1, :], shape)
        ym = jnp.where(g.row == 0, low, pltpu.roll(val, 1, 0))
        yp = jnp.where(g.row == g.rows - 1, high, pltpu.roll(val, g.rows - 1, 0))
        side = jnp.broadcast_to(self.zh[slot, :, x : x + 1], shape)
        side_m, side_p = side, side
        if edge:
            side_m = jnp.where(self.iz == 0, 0.0, side)
            side_p = jnp.where(self.iz == 0, side, 0.0)
        zm = jnp.where(g.lane == 0, side_m, pltpu.roll(val, 1, 1))
        zp = jnp.where(g.lane == g.lanes - 1, side_p, pltpu.roll(val, g.lanes - 1, 1))
        return val, (xm, xp, ym, yp, zm, zp)


def halve_rows(tmp, slot, val):
    rows, lanes = val.shape
    parts = []
    for k in range(lanes // LANES):
        at = 2 * slot + k
        tmp[at, 0:rows, :] = val[:, k * LANES : (k + 1) * LANES]
        parts.append(tmp[at, pl.ds(0, rows // 2, 2), :] + tmp[at, pl.ds(1, rows // 2, 2), :])
    return parts[0] if len(parts) == 1 else jnp.concatenate(parts, axis=1)


def double_rows(tmp, slot, val):
    rows, lanes = val.shape
    parts = []
    for k in range(lanes // LANES):
        at = 2 * slot + k
        piece = val[:, k * LANES : (k + 1) * LANES]
        tmp[at, pl.ds(0, rows, 2), :] = piece
        tmp[at, pl.ds(1, rows, 2), :] = piece
        parts.append(tmp[at, 0 : 2 * rows, :])
    return parts[0] if len(parts) == 1 else jnp.concatenate(parts, axis=1)


def kernel(counts, *refs):
    sources, (mem_out, rec_out, ext_out) = refs[:5], refs[5:8]
    refs = refs[8:]
    mem, rec, ext, fib, lab, in_sem = refs[:6]
    refs = (None,) + refs
    (xs0, ys0, zs0, xh0, yh0, zh0) = refs[7:13]
    (in0, out0, uu, w0, c0, d0, b0, va, vb, tmp, tall) = refs[13:24]
    (ee, ys1, yr1, zs1, zr1, zp1, c1, cz1, d1, b1, v1a, v1b, z1a, z1b, yrim) = refs[24:39]
    (lab_own, lab_all, gc_own, gc, gr_own, gr, in2, out2, c2, d2, b2, v2a, v2b) = refs[39:52]
    (c3, b3, v3, k3, h3, send_sem, recv_sem, wide_send, wide_recv, gs_sem, gr_sem) = refs[52:]
    nx, ny, nz = counts
    ix, iy, iz = lax.axis_index("gx"), lax.axis_index("gy"), lax.axis_index("gz")
    me = (ix * ny + iy) * nz + iz
    total = nx * ny * nz

    loads = [
        pltpu.make_async_copy(src, dst, in_sem.at[i])
        for i, (src, dst) in enumerate(zip(sources, (mem, rec, ext, fib, lab)))
    ]
    for i in (4, 3, 0, 2, 1):
        loads[i].start()

    barrier = pltpu.get_barrier_semaphore()

    def others(body):
        for i in range(1, total):
            dev = me + i
            body(jnp.where(dev >= total, dev - total, dev))

    others(lambda dev: pl.semaphore_signal(barrier, inc=1, device_id=dev, device_id_type=LOGICAL))

    def clear(missing, ref, side):
        def fill():
            ref[side] = jnp.zeros(ref.at[side].shape, F32)

        pl.when(missing)(fill)

    X1, R1, Z1 = mem.shape[0] // 2, mem.shape[1] // 2, mem.shape[2] // 2
    XE, RE = X1 + 2 * GHOST, R1 + 2 * GHOST
    clear(ix == 0, xh0, 0)
    clear(ix == nx - 1, xh0, 1)
    clear(iy == 0, yh0, 0)
    clear(iy == ny - 1, yh0, 1)
    for slot in range(3):
        for p in range(GHOST):
            clear(ix == 0, ee, (slot, p))
            clear(ix == nx - 1, ee, (slot, XE - 1 - p))
    for load in loads:
        load.wait()

    g0 = Grid(*mem.shape)
    g1 = Grid(XE, RE, Z1)
    halo0 = Halo(g0, (xs0, ys0, zs0, xh0, yh0, zh0), iz)

    def copies(number):
        first, slots = EXCHANGES[number]
        h = halo0
        part = pl.ds(first, slots)
        plan = (
            (h.xs.at[0, part], h.xh.at[1, part], (ix - 1, iy, iz), ix > 0, ix < nx - 1),
            (h.xs.at[1, part], h.xh.at[0, part], (ix + 1, iy, iz), ix < nx - 1, ix > 0),
            (h.ys.at[0, part], h.yh.at[1, part], (ix, iy - 1, iz), iy > 0, iy < ny - 1),
            (h.ys.at[1, part], h.yh.at[0, part], (ix, iy + 1, iz), iy < ny - 1, iy > 0),
            (h.zs.at[part], h.zh.at[part], (ix, iy, 1 - iz), None, None),
        )
        for side, (src, dst, dev, goes, comes) in enumerate(plan):
            copy = pltpu.make_async_remote_copy(
                src_ref=src,
                dst_ref=dst,
                send_sem=send_sem.at[number * SIDES + side],
                recv_sem=recv_sem.at[number * SIDES + side],
                device_id=dev,
                device_id_type=MESH,
            )
            yield copy, goes, comes

    ends, rest = slice(0, 2), slice(2, SIDES)

    def send(number, sides=slice(0, SIDES)):
        for copy, goes, _ in list(copies(number))[sides]:
            if goes is None:
                copy.start()
            else:
                pl.when(goes)(copy.start)

    def arrive(number, sides=slice(0, SIDES)):
        for copy, _, comes in list(copies(number))[sides]:
            if comes is None:
                copy.wait_recv()
            else:
                pl.when(comes)(copy.wait_recv)

    def inner_first(number, count):
        arrive(number, rest)
        yield from range(1, count - 1)
        arrive(number, ends)
        yield 0
        yield count - 1

    def publish(number, halo, slot, ref):
        halo.put_ends(slot, ref)
        send(number, ends)
        halo.put_rest(slot, ref)
        send(number, rest)

    def sent(number):
        for copy, goes, _ in copies(number):
            if goes is None:
                copy.wait_send()
            else:
                pl.when(goes)(copy.wait_send)

    here = {-1: ix > 0, 0: None, 1: ix < nx - 1}
    along = {-1: iy > 0, 0: None, 1: iy < ny - 1}

    def both(a, b):
        if a is None or b is None:
            return b if a is None else a
        return jnp.logical_and(a, b)

    def wide_copies(number):
        first, count = WIDE[number]
        part = pl.ds(first, count)
        pairs, edge = X1 // 2, GHOST // 2
        plan = []
        for sx in (-1, 1):
            src = ee.at[part, pl.ds(GHOST if sx < 0 else X1, GHOST), pl.ds(0, R1)]
            dst = ee.at[part, pl.ds(X1 + GHOST if sx < 0 else 0, GHOST), pl.ds(0, R1)]
            plan.append((src, dst, sx, 0, iz))
        for sx in STEPS:
            for sy in (-1, 1):
                mine, theirs = (0, 1) if sy < 0 else (1, 0)
                at = {-1: (0, edge, pairs + edge), 0: (0, pairs, edge), 1: (pairs - edge, edge, 0)}[sx]
                src = ys1.at[mine, part, pl.ds(at[0], at[1])]
                dst = yr1.at[theirs, part, pl.ds(at[2], at[1])]
                plan.append((src, dst, sx, sy, iz))
        for sx in STEPS:
            for sy in STEPS:
                plan.append((zs1.at[part], zr1.at[(1 - sx) * 3 + 1 - sy, part], sx, sy, 1 - iz))
        for side, (src, dst, sx, sy, z) in enumerate(plan):
            copy = pltpu.make_async_remote_copy(
                src_ref=src,
                dst_ref=dst,
                send_sem=wide_send.at[number * WIDE_SIDES + side],
                recv_sem=wide_recv.at[number * WIDE_SIDES + side],
                device_id=(ix + sx, iy + sy, z),
                device_id_type=MESH,
            )
            yield copy, both(here[sx], along[sy]), both(here[-sx], along[-sy])

    def maybe(condition, action):
        if condition is None:
            action()
        else:
            pl.when(condition)(action)

    tile_row = lax.broadcasted_iota(jnp.int32, (8, LANES), 0)
    tile_lane = lax.broadcasted_iota(jnp.int32, (8, LANES), 1)

    def wide_publish(number):
        first, count = WIDE[number]
        for slot in range(first, first + count):
            acc = jnp.zeros((R1, LANES), F32)
            for x in range(X1):
                val = ee[slot, GHOST + x, 0:R1, :]
                for depth in range(GHOST):
                    at = depth * XE + GHOST + x
                    shift = jnp.where(iz == 0, at + 1 + depth, at - depth)
                    acc = jnp.where(tile_lane == at, pltpu.roll(val, shift, 1), acc)
            zs1[slot] = acc
            for k in range(X1 // 2):
                even, odd = ee[slot, GHOST + 2 * k, 0:R1, :], ee[slot, GHOST + 2 * k + 1, 0:R1, :]
                ys1[0, slot, k] = jnp.where(tile_row < GHOST, even, pltpu.roll(odd, GHOST, 0))
                ys1[1, slot, k] = jnp.where(tile_row < GHOST, pltpu.roll(odd, GHOST, 0), even)
        for copy, goes, _ in wide_copies(number):
            maybe(goes, copy.start)

    def keep(condition, val):
        return val if condition is None else jnp.where(condition, val, 0.0)

    def plane_side(p):
        return here[-1 if p < GHOST else (1 if p >= X1 + GHOST else 0)]

    def wide_arrive(number):
        first, count = WIDE[number]
        for copy, _, comes in wide_copies(number):
            maybe(comes, copy.wait_recv)
        low = tile_row >= GHOST
        pe = jnp.bitwise_and(tile_lane, XE - 1)
        for slot in range(first, first + count):
            for p in range(XE):
                after, before = yr1[1, slot, p // 2], yr1[0, slot, p // 2]
                if p % 2:
                    after, before = pltpu.roll(after, GHOST, 0), pltpu.roll(before, GHOST, 0)
                side = plane_side(p)
                after = keep(both(side, along[1]), after)
                before = keep(both(side, along[-1]), before)
                ee[slot, p, R1:RE, :] = jnp.where(low, before, after)
            rows = []
            for sy in STEPS:
                mid = zr1[3 + sy + 1, slot]
                left = keep(here[-1], pltpu.roll(zr1[sy + 1, slot], LANES - X1, 1))
                right = keep(here[1], pltpu.roll(zr1[6 + sy + 1, slot], X1, 1))
                val = jnp.where(pe < GHOST, left, jnp.where(pe >= X1 + GHOST, right, mid))
                rows.append(keep(along[sy], jnp.where(tile_lane < GHOST * XE, val, 0.0)))
            zp1[slot, 0:R1, :] = rows[1]
            zp1[slot, R1:RE, :] = jnp.where(low, rows[0], rows[2])

    def wide_sent(number):
        for copy, goes, _ in wide_copies(number):
            maybe(goes, copy.wait_send)

    def gather_send(own, whole, which):
        def go(dev):
            pltpu.make_async_remote_copy(
                src_ref=own,
                dst_ref=whole.at[me],
                send_sem=gs_sem.at[which],
                recv_sem=gr_sem.at[which],
                device_id=dev,
                device_id_type=LOGICAL,
            ).start()

        others(go)
        whole[pl.ds(me, 1)] = own[...][None]

    def gather_wait(whole, which, recv):
        rest = whole.at[pl.ds(0, total - 1)]
        copy = pltpu.make_async_remote_copy(
            src_ref=rest,
            dst_ref=rest,
            send_sem=gs_sem.at[which],
            recv_sem=gr_sem.at[which],
            device_id=(ix, iy, 1 - iz),
            device_id_type=MESH,
        )
        if recv:
            copy.wait_recv()
        else:
            copy.wait_send()

    X0, R0, Z0 = mem.shape
    X2 = X1 // 2
    R2 = R1 // 2
    half = Z1 // 2

    widen8 = copy_matrix(lab.shape[2], Z0, 3)
    lab_planes = []
    for bx in range(lab.shape[0]):
        wide = jnp.dot(lab[bx].astype(F32), widen8, preferred_element_type=F32)
        lab_planes.append(
            jnp.concatenate(
                [jnp.broadcast_to(wide[by : by + 1], (8, Z0)) for by in range(lab.shape[1])], axis=0
            )
        )

    spread = copy_matrix(lab.shape[2], LANES, 0)

    def lab_lane(bx, by, at):
        line = jnp.dot(lab[bx].astype(F32), spread, preferred_element_type=F32)[by : by + 1]
        return jnp.broadcast_to(pltpu.roll(jnp.broadcast_to(line, (8, LANES)), at * lab.shape[2], 1), (8, LANES))

    def label_of(x):
        return lab_planes[x // 8]

    for x in range(X0):
        label = label_of(x)
        in0[x] = jnp.where(label == 1.0, 1.0, jnp.where(label == 2.0, 0.3, 0.0)) * fib[x]
        out0[x] = jnp.where(label == 0.0, 3.0, 1.0)
        uu[x] = mem[x] + ext[x]
    acc = jnp.zeros((8, LANES), F32)
    for bx in range(lab.shape[0]):
        for by in range(lab.shape[1]):
            at = bx * lab.shape[1] + by
            acc = jnp.where(lax.shift_right_logical(tile_lane, 5) == at, lab_lane(bx, by, at), acc)
    lab_own[...] = acc[0:1]
    halo0.put(INNER, in0)
    halo0.put(U, uu)
    pl.semaphore_wait(barrier, total - 1)
    send(0)
    gather_send(lab_own, lab_all, 2)
    halo0.put(OUTER, out0)
    halo0.put(V, ext)
    send(1)

    narrow = pair_matrix(Z0, Z1, 0)
    narrow_low = pair_matrix(Z1, Z1, 0)
    narrow_high = pair_matrix(Z1, Z1, half)
    double01 = copy_matrix(Z1, Z0, 1)
    double12 = copy_matrix(Z1, Z1, 1)

    def restrict0(plane, factor, base, order=None):
        for x in order or range(X1):
            tall[base + x * R1 : base + (x + 1) * R1, :] = halve_rows(tmp, x, plane(2 * x) + plane(2 * x + 1))
        whole = dot(tall[base : base + X1 * R1, :], narrow) * factor
        return [whole[x * R1 : (x + 1) * R1] for x in range(X1)]

    def restrict1(plane, factor, order=None):
        rows = [None] * X2
        for x in order or range(X2):
            rows[x] = halve_rows(tmp, x, plane(2 * x) + plane(2 * x + 1))
        low = jnp.concatenate(rows[: X2 // 2], axis=0)
        high = jnp.concatenate(rows[X2 // 2 :], axis=0)
        return (dot(low, narrow_low) + dot(high, narrow_high)) * factor

    for x in inner_first(0, X0):
        centre, near = halo0.neighbours(INNER, lambda x: in0[x], x, edge=True)
        u, near_u = halo0.neighbours(U, lambda x: uu[x], x)
        drive = jnp.zeros_like(u)
        for d in range(6):
            weight = jnp.minimum(centre, near[d])
            w0[d, x] = weight
            drive = drive + weight * (near_u[d] - u)
        m, r = mem[x], rec[x]
        tissue = jnp.where(label_of(x) != 0.0, 1.0, 0.0)
        ionic = ionic_gain * m * (m - ionic_onset) * (m - 1.0) + m * r
        mem_out[x] = m + TIME_STEP * (drive - tissue * ionic)
    publish(2, halo0, NEXT, mem_out)
    for x in range(X0):
        m, r = mem[x], rec[x]
        rec_out[x] = r + TIME_STEP * recovery_rate * (-r - ionic_gain * m * (m - ionic_onset - 1.0))

    for x, val in enumerate(restrict0(lambda x: in0[x], 0.125, 0)):
        ee[INNER1, GHOST + x, 0:R1, :] = val
    wide_publish(0)
    gc_own[...] = restrict1(lambda x: ee[INNER1, GHOST + x, 0:R1, :], 0.125)

    def scaled(grid, weights, centre, near, iz_edges):
        full = [weights[d] + 0.5 * (centre + near[d]) for d in range(6)]
        diag = ((full[0] + full[1]) + (full[2] + full[3])) + (full[4] + full[5])
        inv = 1.0 / diag
        full = [f * inv for f in full]
        low, high = iz_edges
        full[4] = jnp.where(low, 0.0, full[4])
        full[5] = jnp.where(high, 0.0, full[5])
        return full, diag, inv

    first0 = (g0.lane == 0) & (iz == 0)
    last0 = (g0.lane == Z0 - 1) & (iz == nz - 1)
    arrive(1)
    inv0 = vb
    for x in range(X0):
        centre, near = halo0.neighbours(OUTER, lambda x: out0[x], x, edge=True)
        full, diag, inv = scaled(g0, [w0[d, x] for d in range(6)], centre, near, (first0, last0))
        for d in range(6):
            c0[d, x] = full[d]
        d0[x] = diag
        b0[x] = inv

    def update(halo, slot, planes, c, b, x):
        val, near = halo.neighbours(slot, planes, x)
        a = b[x] + c[0, x] * near[0]
        e = c[1, x] * near[1] + c[2, x] * near[2]
        f = c[3, x] * near[3] + c[4, x] * near[4]
        return val, (a + c[5, x] * near[5]) + (e + f)

    def half_sweep(number, halo, slot, src, dst, c, b, colour):
        planes = halo.grid.planes
        for x in range(planes) if number is None else inner_first(number, planes):
            val, new = update(halo, slot, lambda x: src[x], c, b, x)
            dst[x] = jnp.where(halo.grid.colour(x, colour), new, val)

    for x in inner_first(2, X0):
        m, near = halo0.neighbours(NEXT, lambda x: mem_out[x], x)
        rhs = jnp.zeros_like(m)
        for d in range(6):
            rhs = rhs + w0[d, x] * (near[d] - m)
        b0[x] = rhs * b0[x]
        val, new = update(halo0, V, lambda x: ext[x], c0, b0, x)
        va[x] = jnp.where(g0.colour(x, 0), new, val)
    publish(3, halo0, RED, va)
    gather_send(gc_own, gc, 0)

    first1 = (g1.lane == 0) & (iz == 0)
    last1 = (g1.lane == Z1 - 1) & (iz == nz - 1)
    pack_row = lax.broadcasted_iota(jnp.int32, (RE, LANES), 0)
    pack_lane = lax.broadcasted_iota(jnp.int32, (RE, LANES), 1)
    pack_x = jnp.bitwise_and(pack_lane, XE - 1)
    depth_parity = lax.div(pack_lane, XE) + iz + pack_x + pack_row
    pack_own = [jnp.bitwise_and(depth_parity + colour, 1) == 0 for colour in range(2)]

    def row_inside(row):
        return (
            (row < R1)
            | ((row < R1 + GHOST) & (iy < ny - 1))
            | ((row >= R1 + GHOST) & (iy > 0))
        )

    inside_row = row_inside(g1.row)
    pack_inside = (
        row_inside(pack_row)
        & (pack_lane < GHOST * XE)
        & ((pack_x >= GHOST) | (ix > 0))
        & ((pack_x < X1 + GHOST) | (ix < nx - 1))
    )

    def inside1(p):
        side = plane_side(p)
        return inside_row if side is None else inside_row & side

    def near1(planes, pack, p, edge=False):
        val = planes(p)
        side = jnp.broadcast_to(pack(p), (RE, Z1))
        side_m, side_p = side, side
        if edge:
            side_m = jnp.where(iz == 0, 0.0, side)
            side_p = jnp.where(iz == 0, side, 0.0)
        return val, (
            planes(p - 1),
            planes(p + 1),
            pltpu.roll(val, 1, 0),
            pltpu.roll(val, RE - 1, 0),
            jnp.where(g1.lane == 0, side_m, pltpu.roll(val, 1, 1)),
            jnp.where(g1.lane == Z1 - 1, side_p, pltpu.roll(val, Z1 - 1, 1)),
        )

    def near_pack(planes, val, first, last):
        own = jnp.zeros((RE, LANES), F32)
        for p in range(first, last):
            own = jnp.where(pack_lane == p, pltpu.roll(planes(p), p + 1 - iz, 1), own)
        return (
            pltpu.roll(val, 1, 1),
            pltpu.roll(val, LANES - 1, 1),
            pltpu.roll(val, 1, 0),
            pltpu.roll(val, RE - 1, 0),
            jnp.where(pack_lane < XE, own, pltpu.roll(val, XE, 1)),
            pltpu.roll(val, LANES - XE, 1),
        )

    def scaled_wide(ci, ni, co, no, inside):
        full = [jnp.minimum(ci, ni[k]) + 0.5 * (co + no[k]) for k in range(6)]
        diag = ((full[0] + full[1]) + (full[2] + full[3])) + (full[4] + full[5])
        inv = jnp.where(inside, 1.0 / diag, 0.0)
        return [jnp.where(inside, f * inv, 0.0) for f in full], diag, inv

    gather_wait(lab_all, 2, True)
    blocks = [(sx, bx) for sx, bx in ((-1, 1), (0, 0), (0, 1), (1, 0))]
    lines = [(0, 0), (0, 1), (1, 0), (-1, 1)]
    span = lab.shape[2]
    for z in range(2):
        core = iz if z == 0 else 1 - iz
        for i, (sx, bx) in enumerate(blocks):
            for j, (sy, by) in enumerate(lines):
                px, py = jnp.clip(ix + sx, 0, nx - 1), jnp.clip(iy + sy, 0, ny - 1)
                at = (z * 4 + i) * 4 + j
                tall[at : at + 1, 0:LANES] = lab_all[(px * ny + py) * nz + core]
    near_labels = tall[0:32, 0:LANES]
    order = lax.bitwise_and(lax.broadcasted_iota(jnp.int32, (32, LANES), 0), 15)
    segment = jnp.zeros((32, LANES), jnp.int32)
    for i, (_, bx) in enumerate(blocks):
        for j, (_, by) in enumerate(lines):
            segment = jnp.where(order == i * 4 + j, bx * lab.shape[1] + by, segment)
    lined = near_labels
    for k in range(1, LANES // span):
        lined = jnp.where(segment == k, pltpu.roll(near_labels, LANES - k * span, 1), lined)
    stretched = jnp.dot(lined[0:16], copy_matrix(LANES, Z1, 2), preferred_element_type=F32)
    edge_labels = jnp.where(iz == 0, lined[16:32, 0:1], lined[16:32, span - 1 : span])
    edge_labels = jnp.broadcast_to(edge_labels, (16, LANES))
    group = lax.shift_right_logical(g1.row, 2)
    pack_group = lax.shift_right_logical(pack_row, 2)
    pack_block = lax.shift_right_logical(pack_x, 2)
    packed_labels = jnp.zeros((RE, LANES), F32)
    for i in range(4):
        block_labels = jnp.zeros((RE, Z1), F32)
        for j in range(4):
            at = i * 4 + j
            block_labels = jnp.where(
                group == j, jnp.broadcast_to(stretched[at : at + 1], (RE, Z1)), block_labels
            )
            packed_labels = jnp.where(
                (pack_group == j) & (pack_block == i),
                jnp.broadcast_to(edge_labels[at : at + 1], (RE, LANES)),
                packed_labels,
            )
        block_outer = jnp.where(block_labels == 0.0, 3.0, 1.0)
        for p in range(4 * i, 4 * i + 4):
            ee[OUTER1, p] = jnp.where(inside1(p), block_outer, 0.0)
    zp1[OUTER1] = jnp.where(pack_inside, jnp.where(packed_labels == 0.0, 3.0, 1.0), 0.0)
    wide_arrive(0)
    for p in range(1, XE - 1):
        ci, ni = near1(lambda p: ee[INNER1, p], lambda p: zp1[INNER1, :, p : p + 1], p, edge=True)
        co, no = near1(lambda p: ee[OUTER1, p], lambda p: zp1[OUTER1, :, p : p + 1], p, edge=True)
        full, diag, inv = scaled_wide(ci, ni, co, no, inside1(p))
        full[4] = jnp.where(first1, 0.0, full[4])
        full[5] = jnp.where(last1, 0.0, full[5])
        for d in range(6):
            c1[d, p] = full[d]
        if GHOST <= p < X1 + GHOST:
            d1[p - GHOST] = diag[0:R1]
            b1[p - GHOST] = inv[0:R1]
    ci, co = zp1[INNER1], zp1[OUTER1]
    full, _, _ = scaled_wide(
        ci,
        near_pack(lambda p: ee[INNER1, p], ci, 0, XE),
        co,
        near_pack(lambda p: ee[OUTER1, p], co, 0, XE),
        pack_inside,
    )
    for d in range(6):
        cz1[d] = full[d]

    def stencil(b, c, near):
        a = b + c(0) * near[0]
        e = c(1) * near[1] + c(2) * near[2]
        f = c(3) * near[3] + c(4) * near[4]
        return (a + c(5) * near[5]) + (e + f)

    def update1(src, pack, p):
        val, near = near1(lambda p: src[p], lambda p: pack[:, p : p + 1], p)
        return val, stencil(ee[RHS1, p], lambda d: c1[d, p], near)

    def half1(src, pack, dst, colour, planes):
        for p in planes:
            val, new = update1(src, pack, p)
            dst[p] = jnp.where(g1.colour(p, colour), new, val)

    def half_pack(src, pack, dst, colour, first, last):
        val = pack[...]
        near = near_pack(lambda p: src[p], val, first, last)
        new = stencil(zp1[RHS1], lambda d: cz1[d], near)
        dst[...] = jnp.where(pack_own[colour], new, val)

    half_sweep(3, halo0, RED, va, vb, c0, b0, 1)
    publish(4, halo0, BLACK, vb)

    XG, RG, ZG = in2.shape
    XH, RH = XG // 2, RG // 2
    g2 = Grid(XG, RG, ZG)
    g3 = Grid(XH, RH, ZG)
    def unpack(tile, dst):
        for px in range(nx):
            for py in range(ny // 2):
                lows, highs = [], []
                for part in range(2):
                    base = (px * ny + 2 * py + part) * nz
                    s0, s1 = tile(base), tile(base + 1)
                    lows.append(jnp.where(tile_lane < half, s0, pltpu.roll(s1, half, 1)))
                    highs.append(jnp.where(tile_lane < half, pltpu.roll(s0, half, 1), s1))
                for xhi, pair in enumerate((lows, highs)):
                    p = px * X2 + xhi * 2
                    dst[p, py * 8 : py * 8 + 8, :] = jnp.where(tile_row < R2, pair[0], pltpu.roll(pair[1], R2, 0))
                    dst[p + 1, py * 8 : py * 8 + 8, :] = jnp.where(
                        tile_row < R2, pltpu.roll(pair[0], R2, 0), pair[1]
                    )

    def whole_neighbours(grid, planes, x, last, mask):
        val = planes(x)
        zero = jnp.zeros_like(val)
        xm = planes(x - 1) if x > 0 else zero
        xp = planes(x + 1) if x < grid.planes - 1 else zero
        near = [
            xm,
            xp,
            pltpu.roll(val, 1, 0),
            pltpu.roll(val, grid.rows - 1, 0),
            pltpu.roll(val, 1, 1),
            pltpu.roll(val, grid.lanes - 1, 1),
        ]
        if mask:
            near[2] = jnp.where(grid.row == 0, 0.0, near[2])
            near[3] = jnp.where(grid.row == grid.rows - 1, 0.0, near[3])
            near[4] = jnp.where(grid.lane == 0, 0.0, near[4])
            near[5] = jnp.where(grid.lane >= last, 0.0, near[5])
        return val, near

    def whole_couplings(grid, inner, outer, last, c, d, b):
        for x in range(grid.planes):
            ci, ni = whole_neighbours(grid, lambda x: inner[x], x, last, True)
            co, no = whole_neighbours(grid, lambda x: outer[x], x, last, True)
            full = [jnp.minimum(ci, ni[k]) + 0.5 * (co + no[k]) for k in range(6)]
            diag = ((full[0] + full[1]) + (full[2] + full[3])) + (full[4] + full[5])
            if last < grid.lanes - 1:
                diag = jnp.where(grid.lane <= last, diag, 1.0)
            inv = 1.0 / diag
            edges = (
                None,
                None,
                grid.row == 0,
                grid.row == grid.rows - 1,
                grid.lane == 0,
                grid.lane >= last,
            )
            for k in range(6):
                f = full[k] * inv
                if edges[k] is not None:
                    f = jnp.where(edges[k], 0.0, f)
                if last < grid.lanes - 1:
                    f = jnp.where(grid.lane <= last, f, 0.0)
                c[k, x] = f
            if d is not None:
                d[x] = diag
            b[x] = inv

    def whole_update(grid, planes, c, b, x):
        val, near = whole_neighbours(grid, planes, x, None, False)
        a = b[x] + c[2, x] * near[2]
        e = c[3, x] * near[3] + c[4, x] * near[4]
        a = a + c[5, x] * near[5]
        if x > 0:
            a = a + c[0, x] * near[0]
        if x < grid.planes - 1:
            e = e + c[1, x] * near[1]
        return val, a + e

    def restrict2(plane, factor):
        pieces = [halve_rows(tmp, x, plane(2 * x) + plane(2 * x + 1)) for x in range(XH)]
        for x in range(XH):
            tall[x * RH : (x + 1) * RH, 0:ZG] = pieces[x]
        whole = dot(tall[0 : XH * RH, 0:ZG], narrow_low) * factor
        return [whole[x * RH : (x + 1) * RH] for x in range(XH)]

    gather_wait(gc, 0, True)
    unpack(lambda t: gc[t], in2)
    for t in range(total):
        tall[t : t + 1, 0:LANES] = lab_all[t]
    k = lax.broadcasted_iota(jnp.int32, (LANES, LANES), 0)
    j = lax.broadcasted_iota(jnp.int32, (LANES, LANES), 1)
    from_lane = lax.div(j, half) * (lab.shape[1] * span) + lax.div(lax.rem(j, half), half // span)
    every = [
        jnp.dot(
            tall[0:total, 0:LANES],
            jnp.where(k == from_lane + by * span, 1.0, 0.0).astype(F32),
            preferred_element_type=F32,
        )
        for by in range(2)
    ]
    first_rows = lax.rem(tile_row, R2) < R2 // 2

    def label_tile(t):
        pair = [jnp.broadcast_to(e[t : t + 1], (8, LANES)) for e in every]
        return jnp.where(jnp.where(first_rows, pair[0], pair[1]) == 0.0, 3.0, 1.0)

    unpack(label_tile, out2)
    whole_couplings(g2, in2, out2, ZG - 1, c2, d2, b2)
    for x, val in enumerate(restrict2(lambda x: in2[x], 0.125)):
        v3[x] = val
    for x, val in enumerate(restrict2(lambda x: out2[x], 0.125)):
        v2a[x, 0:RH] = val
    whole_couplings(g3, v3, v2a.at[:, 0:RH], ZG // 2 - 1, c3, None, b3)

    XP = XH // 2
    own = (g3.even, g3.odd)

    def pack(colour, near, far):
        return jnp.where(own[colour], near, far)

    for colour in range(2):
        for p in range(XP):
            a, z = 2 * p, 2 * p + 1
            k3[colour * 6, p] = pack(colour, c3[1, a], c3[0, z])
            k3[colour * 6 + 1, p] = pack(colour, c3[0, a], c3[1, z])
            for k in range(2, 6):
                k3[colour * 6 + k, p] = pack(colour, c3[k, a], c3[k, z])

    def residual0(x):
        val, new = update(halo0, BLACK, lambda x: vb[x], c0, b0, x)
        return d0[x] * (new - val)

    for x, val in enumerate(restrict0(residual0, 0.5, 0, inner_first(4, X1))):
        ee[RHS1, GHOST + x, 0:R1, :] = val * b1[x]
    wide_publish(1)
    wide_arrive(1)
    ring = GHOST - 1
    for p in range(ring - 1, XE - ring + 1):
        v1a[p] = jnp.where(g1.colour(p, 0), ee[RHS1, p], 0.0)
    z1a[...] = jnp.where(pack_own[0], zp1[RHS1], 0.0)
    half_pack(v1a, z1a, z1b, 1, ring, XE - ring)
    half1(v1a, z1a, v1b, 1, range(ring, XE - ring))

    def residual1(x):
        val, new = update1(v1b, z1b, GHOST + x)
        return d1[x] * (new - val)[0:R1]

    gr_own[...] = restrict1(residual1, 0.5)
    gather_send(gr_own, gr, 1)
    for p in (0, 1, XE - 2, XE - 1):
        v1a[p] = jnp.where(g1.colour(p, 0), ee[RHS1, p], 0.0)
    half_pack(v1a, z1a, z1b, 1, 0, XE)
    half1(v1a, z1a, v1b, 1, (1, 2, XE - 3, XE - 2))
    gather_wait(gr, 1, True)
    unpack(lambda t: gr[t], v2b)
    for x in range(XG):
        b2[x] = v2b[x] * b2[x]
        v2a[x] = jnp.where(g2.colour(x, 0), b2[x], 0.0)
    for x in range(XG):
        val, new = whole_update(g2, lambda x: v2a[x], c2, b2, x)
        v2b[x] = jnp.where(g2.colour(x, 1), new, val)

    def residual2(x):
        val, new = whole_update(g2, lambda x: v2b[x], c2, b2, x)
        return d2[x] * (new - val)

    for x, val in enumerate(restrict2(residual2, 0.5)):
        b3[x] = val * b3[x]

    for colour in range(2):
        for p in range(XP):
            h3[colour, p] = pack(colour, b3[2 * p], b3[2 * p + 1])
    none = jnp.zeros((RH, ZG), F32)

    def relaxed(colour, other):
        fresh = []
        for p in range(XP):
            val, at = other[p], colour * 6
            before = other[p - 1] if p > 0 else none
            after = other[p + 1] if p < XP - 1 else none
            i = h3[colour, p] + k3[at, p] * val
            j = k3[at + 1, p] * pack(colour, before, after) + k3[at + 2, p] * pltpu.roll(val, 1, 0)
            l = k3[at + 3, p] * pltpu.roll(val, RH - 1, 0) + k3[at + 4, p] * pltpu.roll(val, 1, 1)
            fresh.append((i + k3[at + 5, p] * pltpu.roll(val, ZG - 1, 1)) + (j + l))
        return fresh

    def coarse(step, state):
        red = relaxed(0, state[XP:])
        black = relaxed(1, red)
        return tuple(red + black)

    state = lax.fori_loop(0, COARSE_SWEEPS, coarse, (none,) * (2 * XP))
    solved = []
    for p in range(XP):
        solved.append(pack(0, state[p], state[XP + p]))
        solved.append(pack(1, state[p], state[XP + p]))
    for x in range(XH):
        tall[x * RH : (x + 1) * RH, 0:ZG] = solved[x]
    wide = dot(tall[0 : XH * RH, 0:ZG], double12)
    for x in range(XH):
        corr = double_rows(tmp, x, wide[x * RH : (x + 1) * RH])
        v2a[2 * x] = v2b[2 * x] + corr
        v2a[2 * x + 1] = v2b[2 * x + 1] + corr
    for colour, src, dst in ((0, v2a, v2b), (1, v2b, v2a)):
        for x in range(XG):
            val, new = whole_update(g2, lambda x: src[x], c2, b2, x)
            dst[x] = jnp.where(g2.colour(x, colour), new, val)

    row_shift = lax.rem(RG - iy * R2, RG)
    lane_shift = lax.rem(ZG - iz * half, ZG)
    edge2 = GHOST // 2
    rows2 = R2 + 2 * edge2
    planes2 = X2 + 2 * edge2
    for k in range(planes2):
        part = v2a[jnp.clip(ix * X2 + k - edge2, 0, XG - 1)]
        part = pltpu.roll(pltpu.roll(part, row_shift, 0), lane_shift, 1)
        tall[k * rows2 : (k + 1) * rows2, 0:ZG] = jnp.where(
            tile_row < R2 + edge2, part[0:rows2], part[RG - rows2 : RG]
        )
    source = lax.broadcasted_iota(jnp.int32, (ZG, LANES), 0)
    target = lax.broadcasted_iota(jnp.int32, (ZG, LANES), 1)
    target = lax.div(target, 2 * XE)
    pick = jnp.where(source == jnp.where(iz == 0, half + target, ZG - 1 - target), 1.0, 0.0).astype(F32)
    coarse_rows = tall[0 : planes2 * rows2, 0:ZG]
    wide = dot(coarse_rows, double12)
    sides = dot(coarse_rows, pick)
    acc = jnp.zeros((rows2, LANES), F32)
    tile_plane = lax.div(jnp.bitwise_and(tile_lane, XE - 1), 2)
    for k in range(planes2):
        acc = jnp.where(tile_plane == k, sides[k * rows2 : (k + 1) * rows2], acc)
    z1a[...] = z1b[...] + jnp.where(pack_inside, double_rows(tmp, 0, acc), 0.0)
    for k in range(planes2):
        corr = double_rows(tmp, k, wide[k * rows2 : (k + 1) * rows2])
        for p in (2 * k, 2 * k + 1):
            if 0 < p < XE - 1:
                v1a[p] = v1b[p] + jnp.where(inside1(p), corr, 0.0)
    half_pack(v1a, z1a, z1b, 0, 1, XE - 1)
    half1(v1a, z1a, v1b, 0, range(2, XE - 2))
    half_pack(v1b, z1b, z1a, 1, 2, XE - 2)
    half1(v1b, z1b, v1a, 1, range(3, XE - 3))

    def enlarge(count, read, write):
        for x in range(count):
            tall[x * R1 : (x + 1) * R1, 0:Z1] = read(x)
        wide = dot(tall[0 : count * R1, 0:Z1], double01)
        for x in range(count):
            write(x, double_rows(tmp, x, wide[x * R1 : (x + 1) * R1]))

    def inside(x, corr):
        va[2 * x] = vb[2 * x] + corr
        va[2 * x + 1] = vb[2 * x + 1] + corr

    enlarge(X1, lambda x: v1a[GHOST + x, 0:R1, :], inside)
    for x in range(X1):
        yrim[0, x : x + 1, :] = v1a[GHOST + x, RE - 1 : RE, :]
        yrim[1, x : x + 1, :] = v1a[GHOST + x, R1 : R1 + 1, :]

    def rim(k):
        if k < 2:
            return v1a[GHOST - 1 if k == 0 else X1 + GHOST, 0:R1, :]
        if k < 4:
            return yrim[k - 2]
        return pltpu.roll(z1a[0:R1, :], LANES - GHOST, 1)

    def outside(k, corr):
        if k < 2:
            xh0[k, FIXED] = xh0[k, BLACK] + corr
        elif k < 4:
            yh0[k - 2, FIXED] = yh0[k - 2, BLACK] + corr
        else:
            zh0[FIXED] = zh0[BLACK] + corr[:, 0:LANES]

    enlarge(5, rim, outside)
    half_sweep(None, halo0, FIXED, va, vb, c0, b0, 0)
    publish(5, halo0, LAST, vb)
    half_sweep(5, halo0, LAST, vb, ext_out, c0, b0, 1)

    for number in range(len(EXCHANGES)):
        sent(number)
    for number in range(len(WIDE)):
        wide_sent(number)
    gather_wait(gc, 0, False)
    gather_wait(gr, 1, False)
    gather_wait(lab_all, 2, False)


def finish(*refs):
    count = (len(refs) - 1) // 2
    sem = refs[-1]
    copies = [pltpu.make_async_copy(refs[i], refs[count + i], sem.at[i]) for i in range(count)]
    for copy in copies:
        copy.start()
    for copy in copies:
        copy.wait()


def solution(mesh):
    nx, ny, nz = (mesh.shape[a] for a in ("gx", "gy", "gz"))
    spec = P("gx", "gy", "gz")

    def on_device(membrane, recovery, extracellular, fiber_scale, labels):
        X, R, Z = membrane.shape
        X1, R1, Z1 = X // 2, R // 2, Z // 2
        XG, RG, ZG = nx * X // 4, ny * R // 4, nz * Z // 4
        assert nz == 2 and ny % 2 == 0 and ZG == LANES and Z1 == LANES
        assert R1 == 8 and X1 == 8 and X % 8 == 0
        total = nx * ny * nz
        assert labels.shape == (2, 2, LANES // 4)
        f0 = 9
        field = (X, R, Z)
        lvl1 = (X1, R1, Z1)
        whole = (XG, RG, ZG)
        third = (XG // 2, RG // 2, ZG)

        def v(*shape):
            return pltpu.VMEM(shape, F32)

        def faces(f, x, r, z):
            return [v(2, f, r, z), v(2, f, x, z), v(f, r, LANES)] * 2

        anywhere = pl.BlockSpec(memory_space=pl.ANY)
        scratch = [v(*field)] * 4 + [pltpu.VMEM(labels.shape, jnp.int32), pltpu.SemaphoreType.DMA((5,))]
        scratch += faces(f0, *field)
        scratch += [v(*field), v(*field), v(*field), v(6, *field), v(6, *field), v(*field), v(*field)]
        scratch += [v(*field), v(*field)]
        scratch += [
            v(2 * max(X1, XG // 2), max(R, RG), LANES),
            v(max(X1 * R1, (XG // 2) * (RG // 2), 2 * X1 * R1, total), Z),
        ]
        XE, RE = X1 + 2 * GHOST, R1 + 2 * GHOST
        assert GHOST * XE <= LANES and 2 * GHOST == R1 and GHOST <= X1
        wide, pack = (XE, RE, Z1), (RE, LANES)
        scratch += [v(3, *wide), v(2, 3, X1 // 2, R1, Z1), v(2, 3, XE // 2, R1, Z1), v(3, R1, LANES)]
        scratch += [v(9, 3, R1, LANES), v(3, *pack), v(6, *wide), v(6, *pack), v(*lvl1), v(*lvl1)]
        scratch += [v(*wide), v(*wide), v(*pack), v(*pack), v(2, X1, Z1)]
        scratch += [v(1, LANES), v(total, 1, LANES), v(8, LANES), v(total, 8, LANES), v(8, LANES), v(total, 8, LANES)]
        scratch += [v(*whole), v(*whole), v(6, *whole), v(*whole), v(*whole), v(*whole), v(*whole)]
        scratch += [v(6, *third), v(*third), v(*third)]
        packed = (XG // 4, RG // 2, ZG)
        scratch += [v(12, *packed), v(2, *packed)]
        sems = SIDES * len(EXCHANGES)
        scratch += [pltpu.SemaphoreType.DMA((sems,))] * 2
        scratch += [pltpu.SemaphoreType.DMA((WIDE_SIDES * len(WIDE),))] * 2
        scratch += [pltpu.SemaphoreType.DMA((3,))] * 2
        vmem = pl.BlockSpec(memory_space=pltpu.VMEM)
        room = 54400 << 10
        shape = jax.ShapeDtypeStruct(field, F32)
        results = pl.pallas_call(
            functools.partial(kernel, (nx, ny, nz)),
            out_shape=[shape] * 3,
            in_specs=[anywhere] * 5,
            out_specs=[vmem] * 3,
            scratch_shapes=scratch,
            compiler_params=pltpu.CompilerParams(
                collective_id=0, has_side_effects=True, vmem_limit_bytes=room
            ),
        )(membrane, recovery, extracellular, fiber_scale, labels)
        return tuple(
            pl.pallas_call(
                finish,
                out_shape=[shape] * 3,
                in_specs=[vmem] * 3,
                out_specs=[anywhere] * 3,
                scratch_shapes=[pltpu.SemaphoreType.DMA((3,))],
                compiler_params=pltpu.CompilerParams(vmem_limit_bytes=4 << 20),
            )(*results)
        )

    return jax.shard_map(
        on_device,
        mesh=mesh,
        in_specs=(spec,) * 5,
        out_specs=(spec,) * 3,
        check_vma=False,
    )
```

```python
import functools

import jax
import jax.numpy as jnp
from jax import lax
from jax.experimental import pallas as pl
from jax.experimental.pallas import tpu as pltpu
from jax.sharding import PartitionSpec as P

COARSE_SWEEPS = 8
TIME_STEP = 0.05
ionic_gain = 8.0
ionic_onset = 0.15
recovery_rate = 0.01
MESH = pl.DeviceIdType.MESH
LOGICAL = pl.DeviceIdType.LOGICAL
LANES = 128
F32 = jnp.float32

INNER, U, OUTER, V, NEXT, RED, BLACK, MIXED, READY, FIXED, LAST = range(11)
INNER1, OUTER1, RHS1 = range(3)
GHOST = 4
EXCHANGES = (
    (INNER, 2),
    (OUTER, 2),
    (NEXT, 1),
    (RED, 1),
    (BLACK, 1),
    (MIXED, 2),
)
SIDES = 5
WIDE = ((INNER1, 1), (RHS1, 1))
STEPS = (-1, 0, 1)
WIDE_SIDES = 17


def dot(a, b):
    return jnp.dot(a, b, precision=lax.Precision.HIGHEST, preferred_element_type=F32)


def pair_matrix(rows, cols, offset):
    j = lax.broadcasted_iota(jnp.int32, (rows, cols), 0)
    k = lax.broadcasted_iota(jnp.int32, (rows, cols), 1)
    return jnp.where(lax.shift_right_logical(j, 1) + offset == k, 1.0, 0.0).astype(F32)


def copy_matrix(rows, cols, shift):
    k = lax.broadcasted_iota(jnp.int32, (rows, cols), 0)
    j = lax.broadcasted_iota(jnp.int32, (rows, cols), 1)
    return jnp.where(lax.shift_right_logical(j, shift) == k, 1.0, 0.0).astype(F32)


class Grid:
    def __init__(self, planes, rows, lanes):
        self.planes, self.rows, self.lanes = planes, rows, lanes
        self.row = lax.broadcasted_iota(jnp.int32, (rows, lanes), 0)
        self.lane = lax.broadcasted_iota(jnp.int32, (rows, lanes), 1)
        self.even = jnp.bitwise_and(self.row + self.lane, 1) == 0
        self.odd = jnp.bitwise_and(self.row + self.lane, 1) == 1

    def colour(self, x, colour):
        return self.even if (x + colour) % 2 == 0 else self.odd


class Halo:
    def __init__(self, grid, refs, iz):
        self.grid, self.iz = grid, iz
        self.xs, self.ys, self.zs, self.xh, self.yh, self.zh = refs
        self.flane = lax.broadcasted_iota(jnp.int32, (grid.rows, LANES), 1)

    def faces(self, slot, planes):
        g = self.grid
        acc = jnp.zeros((g.rows, LANES), F32)
        for x, val in planes:
            self.ys[0, slot, x : x + 1, :] = val[0:1]
            self.ys[1, slot, x : x + 1, :] = val[g.rows - 1 :]
            if g.lanes > LANES:
                end = jnp.where(self.iz == 0, val[:, g.lanes - LANES :], val[:, :LANES])
            else:
                end = val
            acc = jnp.where(self.flane == x, pltpu.roll(end, x + 1 - self.iz, 1), acc)
            yield
        self.zs[slot] = acc

    def put_ends(self, slot, ref):
        self.xs[0, slot] = ref[0]
        self.xs[1, slot] = ref[self.grid.planes - 1]

    def put_rest(self, slot, ref):
        for _ in self.faces(slot, [(x, ref[x]) for x in range(self.grid.planes)]):
            pass

    def put(self, slot, ref):
        self.put_ends(slot, ref)
        self.put_rest(slot, ref)

    def neighbours(self, slot, planes, x, edge=False):
        g = self.grid
        val = planes(x)
        xm = planes(x - 1) if x > 0 else self.xh[0, slot]
        xp = planes(x + 1) if x < g.planes - 1 else self.xh[1, slot]
        shape = (g.rows, g.lanes)
        low = jnp.broadcast_to(self.yh[0, slot, x : x + 1, :], shape)
        high = jnp.broadcast_to(self.yh[1, slot, x : x + 1, :], shape)
        ym = jnp.where(g.row == 0, low, pltpu.roll(val, 1, 0))
        yp = jnp.where(g.row == g.rows - 1, high, pltpu.roll(val, g.rows - 1, 0))
        side = jnp.broadcast_to(self.zh[slot, :, x : x + 1], shape)
        side_m, side_p = side, side
        if edge:
            side_m = jnp.where(self.iz == 0, 0.0, side)
            side_p = jnp.where(self.iz == 0, side, 0.0)
        zm = jnp.where(g.lane == 0, side_m, pltpu.roll(val, 1, 1))
        zp = jnp.where(g.lane == g.lanes - 1, side_p, pltpu.roll(val, g.lanes - 1, 1))
        return val, (xm, xp, ym, yp, zm, zp)


def halve_rows(tmp, slot, val):
    rows, lanes = val.shape
    parts = []
    for k in range(lanes // LANES):
        at = 2 * slot + k
        tmp[at, 0:rows, :] = val[:, k * LANES : (k + 1) * LANES]
        parts.append(tmp[at, pl.ds(0, rows // 2, 2), :] + tmp[at, pl.ds(1, rows // 2, 2), :])
    return parts[0] if len(parts) == 1 else jnp.concatenate(parts, axis=1)


def double_rows(tmp, slot, val):
    rows, lanes = val.shape
    parts = []
    for k in range(lanes // LANES):
        at = 2 * slot + k
        piece = val[:, k * LANES : (k + 1) * LANES]
        tmp[at, pl.ds(0, rows, 2), :] = piece
        tmp[at, pl.ds(1, rows, 2), :] = piece
        parts.append(tmp[at, 0 : 2 * rows, :])
    return parts[0] if len(parts) == 1 else jnp.concatenate(parts, axis=1)


def kernel(counts, *refs):
    sources, (mem_out, rec_out, ext_out) = refs[:5], refs[5:8]
    refs = refs[8:]
    mem, rec, ext, fib, lab, in_sem = refs[:6]
    refs = (None,) + refs
    (xs0, ys0, zs0, xh0, yh0, zh0) = refs[7:13]
    (in0, out0, uu, w0, c0, d0, b0, va, vb, tmp, tall) = refs[13:24]
    (ee, ys1, yr1, zs1, zr1, zp1, c1, cz1, d1, b1, v1a, v1b, z1a, z1b, yrim, mixed, tall2) = refs[24:41]
    (lab_own, lab_all, gc_own, gc, gr_own, gr, in2, out2, c2, d2, b2, v2a, v2b) = refs[41:54]
    (c3, b3, v3, k3, h3, send_sem, recv_sem, wide_send, wide_recv, gs_sem, gr_sem) = refs[54:]
    nx, ny, nz = counts
    ix, iy, iz = lax.axis_index("gx"), lax.axis_index("gy"), lax.axis_index("gz")
    me = (ix * ny + iy) * nz + iz
    total = nx * ny * nz

    loads = [
        pltpu.make_async_copy(src, dst, in_sem.at[i])
        for i, (src, dst) in enumerate(zip(sources, (mem, rec, ext, fib, lab)))
    ]
    for i in (4, 3, 0, 2, 1):
        loads[i].start()

    barrier = pltpu.get_barrier_semaphore()

    def others(body):
        for i in range(1, total):
            dev = me + i
            body(jnp.where(dev >= total, dev - total, dev))

    others(lambda dev: pl.semaphore_signal(barrier, inc=1, device_id=dev, device_id_type=LOGICAL))

    def clear(missing, ref, side):
        def fill():
            ref[side] = jnp.zeros(ref.at[side].shape, F32)

        pl.when(missing)(fill)

    X1, R1, Z1 = mem.shape[0] // 2, mem.shape[1] // 2, mem.shape[2] // 2
    XE, RE = X1 + 2 * GHOST, R1 + 2 * GHOST
    clear(ix == 0, xh0, 0)
    clear(ix == nx - 1, xh0, 1)
    clear(iy == 0, yh0, 0)
    clear(iy == ny - 1, yh0, 1)
    for slot in range(3):
        for p in range(GHOST):
            clear(ix == 0, ee, (slot, p))
            clear(ix == nx - 1, ee, (slot, XE - 1 - p))
    for load in loads:
        load.wait()

    g0 = Grid(*mem.shape)
    g1 = Grid(XE, RE, Z1)
    halo0 = Halo(g0, (xs0, ys0, zs0, xh0, yh0, zh0), iz)

    def copies(number):
        first, slots = EXCHANGES[number]
        h = halo0
        part = pl.ds(first, slots)
        plan = (
            (h.xs.at[0, part], h.xh.at[1, part], (ix - 1, iy, iz), ix > 0, ix < nx - 1),
            (h.xs.at[1, part], h.xh.at[0, part], (ix + 1, iy, iz), ix < nx - 1, ix > 0),
            (h.ys.at[0, part], h.yh.at[1, part], (ix, iy - 1, iz), iy > 0, iy < ny - 1),
            (h.ys.at[1, part], h.yh.at[0, part], (ix, iy + 1, iz), iy < ny - 1, iy > 0),
            (h.zs.at[part], h.zh.at[part], (ix, iy, 1 - iz), None, None),
        )
        for side, (src, dst, dev, goes, comes) in enumerate(plan):
            copy = pltpu.make_async_remote_copy(
                src_ref=src,
                dst_ref=dst,
                send_sem=send_sem.at[number * SIDES + side],
                recv_sem=recv_sem.at[number * SIDES + side],
                device_id=dev,
                device_id_type=MESH,
            )
            yield copy, goes, comes

    ends, rest = slice(0, 2), slice(2, SIDES)

    def send(number, sides=slice(0, SIDES)):
        for copy, goes, _ in list(copies(number))[sides]:
            if goes is None:
                copy.start()
            else:
                pl.when(goes)(copy.start)

    def arrive(number, sides=slice(0, SIDES)):
        for copy, _, comes in list(copies(number))[sides]:
            if comes is None:
                copy.wait_recv()
            else:
                pl.when(comes)(copy.wait_recv)

    def inner_first(number, count):
        arrive(number, rest)
        yield from range(1, count - 1)
        arrive(number, ends)
        yield 0
        yield count - 1

    def publish(number, halo, slot, ref):
        halo.put_ends(slot, ref)
        send(number, ends)
        halo.put_rest(slot, ref)
        send(number, rest)

    def sent(number):
        for copy, goes, _ in copies(number):
            if goes is None:
                copy.wait_send()
            else:
                pl.when(goes)(copy.wait_send)

    here = {-1: ix > 0, 0: None, 1: ix < nx - 1}
    along = {-1: iy > 0, 0: None, 1: iy < ny - 1}

    def both(a, b):
        if a is None or b is None:
            return b if a is None else a
        return jnp.logical_and(a, b)

    def wide_copies(number):
        first, count = WIDE[number]
        part = pl.ds(first, count)
        pairs, edge = X1 // 2, GHOST // 2
        plan = []
        for sx in (-1, 1):
            src = ee.at[part, pl.ds(GHOST if sx < 0 else X1, GHOST), pl.ds(0, R1)]
            dst = ee.at[part, pl.ds(X1 + GHOST if sx < 0 else 0, GHOST), pl.ds(0, R1)]
            plan.append((src, dst, sx, 0, iz))
        for sx in STEPS:
            for sy in (-1, 1):
                mine, theirs = (0, 1) if sy < 0 else (1, 0)
                at = {-1: (0, edge, pairs + edge), 0: (0, pairs, edge), 1: (pairs - edge, edge, 0)}[sx]
                src = ys1.at[mine, part, pl.ds(at[0], at[1])]
                dst = yr1.at[theirs, part, pl.ds(at[2], at[1])]
                plan.append((src, dst, sx, sy, iz))
        for sx in STEPS:
            for sy in STEPS:
                plan.append((zs1.at[part], zr1.at[(1 - sx) * 3 + 1 - sy, part], sx, sy, 1 - iz))
        for side, (src, dst, sx, sy, z) in enumerate(plan):
            copy = pltpu.make_async_remote_copy(
                src_ref=src,
                dst_ref=dst,
                send_sem=wide_send.at[number * WIDE_SIDES + side],
                recv_sem=wide_recv.at[number * WIDE_SIDES + side],
                device_id=(ix + sx, iy + sy, z),
                device_id_type=MESH,
            )
            yield copy, both(here[sx], along[sy]), both(here[-sx], along[-sy])

    def maybe(condition, action):
        if condition is None:
            action()
        else:
            pl.when(condition)(action)

    tile_row = lax.broadcasted_iota(jnp.int32, (8, LANES), 0)
    tile_lane = lax.broadcasted_iota(jnp.int32, (8, LANES), 1)

    def wide_publish(number):
        first, count = WIDE[number]
        for slot in range(first, first + count):
            acc = jnp.zeros((R1, LANES), F32)
            for x in range(X1):
                val = ee[slot, GHOST + x, 0:R1, :]
                for depth in range(GHOST):
                    at = depth * XE + GHOST + x
                    shift = jnp.where(iz == 0, at + 1 + depth, at - depth)
                    acc = jnp.where(tile_lane == at, pltpu.roll(val, shift, 1), acc)
            zs1[slot] = acc
            for k in range(X1 // 2):
                even, odd = ee[slot, GHOST + 2 * k, 0:R1, :], ee[slot, GHOST + 2 * k + 1, 0:R1, :]
                ys1[0, slot, k] = jnp.where(tile_row < GHOST, even, pltpu.roll(odd, GHOST, 0))
                ys1[1, slot, k] = jnp.where(tile_row < GHOST, pltpu.roll(odd, GHOST, 0), even)
        for copy, goes, _ in wide_copies(number):
            maybe(goes, copy.start)

    def keep(condition, val):
        return val if condition is None else jnp.where(condition, val, 0.0)

    def plane_side(p):
        return here[-1 if p < GHOST else (1 if p >= X1 + GHOST else 0)]

    def wide_arrive(number):
        first, count = WIDE[number]
        for copy, _, comes in wide_copies(number):
            maybe(comes, copy.wait_recv)
        low = tile_row >= GHOST
        pe = jnp.bitwise_and(tile_lane, XE - 1)
        for slot in range(first, first + count):
            for p in range(XE):
                after, before = yr1[1, slot, p // 2], yr1[0, slot, p // 2]
                if p % 2:
                    after, before = pltpu.roll(after, GHOST, 0), pltpu.roll(before, GHOST, 0)
                side = plane_side(p)
                after = keep(both(side, along[1]), after)
                before = keep(both(side, along[-1]), before)
                ee[slot, p, R1:RE, :] = jnp.where(low, before, after)
            rows = []
            for sy in STEPS:
                mid = zr1[3 + sy + 1, slot]
                left = keep(here[-1], pltpu.roll(zr1[sy + 1, slot], LANES - X1, 1))
                right = keep(here[1], pltpu.roll(zr1[6 + sy + 1, slot], X1, 1))
                val = jnp.where(pe < GHOST, left, jnp.where(pe >= X1 + GHOST, right, mid))
                rows.append(keep(along[sy], jnp.where(tile_lane < GHOST * XE, val, 0.0)))
            zp1[slot, 0:R1, :] = rows[1]
            zp1[slot, R1:RE, :] = jnp.where(low, rows[0], rows[2])

    def wide_sent(number):
        for copy, goes, _ in wide_copies(number):
            maybe(goes, copy.wait_send)

    def gather_send(own, whole, which):
        def go(dev):
            pltpu.make_async_remote_copy(
                src_ref=own,
                dst_ref=whole.at[me],
                send_sem=gs_sem.at[which],
                recv_sem=gr_sem.at[which],
                device_id=dev,
                device_id_type=LOGICAL,
            ).start()

        others(go)
        whole[pl.ds(me, 1)] = own[...][None]

    def gather_wait(whole, which, recv):
        rest = whole.at[pl.ds(0, total - 1)]
        copy = pltpu.make_async_remote_copy(
            src_ref=rest,
            dst_ref=rest,
            send_sem=gs_sem.at[which],
            recv_sem=gr_sem.at[which],
            device_id=(ix, iy, 1 - iz),
            device_id_type=MESH,
        )
        if recv:
            copy.wait_recv()
        else:
            copy.wait_send()

    X0, R0, Z0 = mem.shape
    X2 = X1 // 2
    R2 = R1 // 2
    half = Z1 // 2

    widen8 = copy_matrix(lab.shape[2], Z0, 3)
    lab_planes = []
    for bx in range(lab.shape[0]):
        wide = jnp.dot(lab[bx].astype(F32), widen8, preferred_element_type=F32)
        lab_planes.append(
            jnp.concatenate(
                [jnp.broadcast_to(wide[by : by + 1], (8, Z0)) for by in range(lab.shape[1])], axis=0
            )
        )

    spread = copy_matrix(lab.shape[2], LANES, 0)

    def lab_lane(bx, by, at):
        line = jnp.dot(lab[bx].astype(F32), spread, preferred_element_type=F32)[by : by + 1]
        return jnp.broadcast_to(pltpu.roll(jnp.broadcast_to(line, (8, LANES)), at * lab.shape[2], 1), (8, LANES))

    def label_of(x):
        return lab_planes[x // 8]

    for x in range(X0):
        label = label_of(x)
        in0[x] = jnp.where(label == 1.0, 1.0, jnp.where(label == 2.0, 0.3, 0.0)) * fib[x]
        out0[x] = jnp.where(label == 0.0, 3.0, 1.0)
        uu[x] = mem[x] + ext[x]
    acc = jnp.zeros((8, LANES), F32)
    for bx in range(lab.shape[0]):
        for by in range(lab.shape[1]):
            at = bx * lab.shape[1] + by
            acc = jnp.where(lax.shift_right_logical(tile_lane, 5) == at, lab_lane(bx, by, at), acc)
    lab_own[...] = acc[0:1]
    halo0.put(INNER, in0)
    halo0.put(U, uu)
    pl.semaphore_wait(barrier, total - 1)
    send(0)
    gather_send(lab_own, lab_all, 2)
    halo0.put(OUTER, out0)
    halo0.put(V, ext)
    send(1)

    narrow = pair_matrix(Z0, Z1, 0)
    narrow_low = pair_matrix(Z1, Z1, 0)
    narrow_high = pair_matrix(Z1, Z1, half)
    double01 = copy_matrix(Z1, Z0, 1)
    double12 = copy_matrix(Z1, Z1, 1)

    def restrict0(plane, factor, base, order=None):
        for x in order or range(X1):
            tall[base + x * R1 : base + (x + 1) * R1, :] = halve_rows(tmp, x, plane(2 * x) + plane(2 * x + 1))
        whole = dot(tall[base : base + X1 * R1, :], narrow) * factor
        return [whole[x * R1 : (x + 1) * R1] for x in range(X1)]

    def restrict1(plane, factor, order=None):
        rows = [None] * X2
        for x in order or range(X2):
            rows[x] = halve_rows(tmp, x, plane(2 * x) + plane(2 * x + 1))
        low = jnp.concatenate(rows[: X2 // 2], axis=0)
        high = jnp.concatenate(rows[X2 // 2 :], axis=0)
        return (dot(low, narrow_low) + dot(high, narrow_high)) * factor

    for x in inner_first(0, X0):
        centre, near = halo0.neighbours(INNER, lambda x: in0[x], x, edge=True)
        u, near_u = halo0.neighbours(U, lambda x: uu[x], x)
        drive = jnp.zeros_like(u)
        for d in range(6):
            weight = jnp.minimum(centre, near[d])
            w0[d, x] = weight
            drive = drive + weight * (near_u[d] - u)
        m, r = mem[x], rec[x]
        tissue = jnp.where(label_of(x) != 0.0, 1.0, 0.0)
        ionic = ionic_gain * m * (m - ionic_onset) * (m - 1.0) + m * r
        mem_out[x] = m + TIME_STEP * (drive - tissue * ionic)
    publish(2, halo0, NEXT, mem_out)
    for x in range(X0):
        m, r = mem[x], rec[x]
        rec_out[x] = r + TIME_STEP * recovery_rate * (-r - ionic_gain * m * (m - ionic_onset - 1.0))

    for x, val in enumerate(restrict0(lambda x: in0[x], 0.125, 0)):
        ee[INNER1, GHOST + x, 0:R1, :] = val
    wide_publish(0)
    gc_own[...] = restrict1(lambda x: ee[INNER1, GHOST + x, 0:R1, :], 0.125)

    def scaled(grid, weights, centre, near, iz_edges):
        full = [weights[d] + 0.5 * (centre + near[d]) for d in range(6)]
        diag = ((full[0] + full[1]) + (full[2] + full[3])) + (full[4] + full[5])
        inv = 1.0 / diag
        full = [f * inv for f in full]
        low, high = iz_edges
        along_z = jnp.where(even_lane, full[4], full[5])
        full[4] = jnp.where(low, 0.0, full[4])
        full[5] = jnp.where(high, 0.0, full[5])
        return full, diag, inv, along_z

    even_lane = jnp.bitwise_and(g0.lane, 1) == 0
    even_row = jnp.bitwise_and(g0.row, 1) == 0
    first0 = (g0.lane == 0) & (iz == 0)
    last0 = (g0.lane == Z0 - 1) & (iz == nz - 1)
    arrive(1)
    inv0 = vb
    for x in range(X0):
        centre, near = halo0.neighbours(OUTER, lambda x: out0[x], x, edge=True)
        full, diag, inv, along_z = scaled(g0, [w0[d, x] for d in range(6)], centre, near, (first0, last0))
        for d in range(6):
            c0[d, x] = full[d]
        d0[x] = diag
        b0[x] = inv
        mixed[x] = pltpu.roll(along_z, 1, 1)

    def update(halo, slot, planes, c, b, x):
        val, near = halo.neighbours(slot, planes, x)
        a = b[x] + c[0, x] * near[0]
        e = c[1, x] * near[1] + c[2, x] * near[2]
        f = c[3, x] * near[3] + c[4, x] * near[4]
        return val, (a + c[5, x] * near[5]) + (e + f)

    def half_sweep(number, halo, slot, src, dst, c, b, colour):
        planes = halo.grid.planes
        for x in range(planes) if number is None else inner_first(number, planes):
            val, new = update(halo, slot, lambda x: src[x], c, b, x)
            dst[x] = jnp.where(halo.grid.colour(x, colour), new, val)

    for x in inner_first(2, X0):
        m, near = halo0.neighbours(NEXT, lambda x: mem_out[x], x)
        rhs = jnp.zeros_like(m)
        for d in range(6):
            rhs = rhs + w0[d, x] * (near[d] - m)
        b0[x] = rhs * b0[x]
        val, new = update(halo0, V, lambda x: ext[x], c0, b0, x)
        va[x] = jnp.where(g0.colour(x, 0), new, val)
    publish(3, halo0, RED, va)
    gather_send(gc_own, gc, 0)

    first1 = (g1.lane == 0) & (iz == 0)
    last1 = (g1.lane == Z1 - 1) & (iz == nz - 1)
    pack_row = lax.broadcasted_iota(jnp.int32, (RE, LANES), 0)
    pack_lane = lax.broadcasted_iota(jnp.int32, (RE, LANES), 1)
    pack_x = jnp.bitwise_and(pack_lane, XE - 1)
    depth_parity = lax.div(pack_lane, XE) + iz + pack_x + pack_row
    pack_own = [jnp.bitwise_and(depth_parity + colour, 1) == 0 for colour in range(2)]

    def row_inside(row):
        return (
            (row < R1)
            | ((row < R1 + GHOST) & (iy < ny - 1))
            | ((row >= R1 + GHOST) & (iy > 0))
        )

    inside_row = row_inside(g1.row)
    pack_inside = (
        row_inside(pack_row)
        & (pack_lane < GHOST * XE)
        & ((pack_x >= GHOST) | (ix > 0))
        & ((pack_x < X1 + GHOST) | (ix < nx - 1))
    )

    def inside1(p):
        side = plane_side(p)
        return inside_row if side is None else inside_row & side

    def near1(planes, pack, p, edge=False):
        val = planes(p)
        side = jnp.broadcast_to(pack(p), (RE, Z1))
        side_m, side_p = side, side
        if edge:
            side_m = jnp.where(iz == 0, 0.0, side)
            side_p = jnp.where(iz == 0, side, 0.0)
        return val, (
            planes(p - 1),
            planes(p + 1),
            pltpu.roll(val, 1, 0),
            pltpu.roll(val, RE - 1, 0),
            jnp.where(g1.lane == 0, side_m, pltpu.roll(val, 1, 1)),
            jnp.where(g1.lane == Z1 - 1, side_p, pltpu.roll(val, Z1 - 1, 1)),
        )

    def near_pack(planes, val, first, last):
        own = jnp.zeros((RE, LANES), F32)
        for p in range(first, last):
            own = jnp.where(pack_lane == p, pltpu.roll(planes(p), p + 1 - iz, 1), own)
        return (
            pltpu.roll(val, 1, 1),
            pltpu.roll(val, LANES - 1, 1),
            pltpu.roll(val, 1, 0),
            pltpu.roll(val, RE - 1, 0),
            jnp.where(pack_lane < XE, own, pltpu.roll(val, XE, 1)),
            pltpu.roll(val, LANES - XE, 1),
        )

    def scaled_wide(ci, ni, co, no, inside):
        full = [jnp.minimum(ci, ni[k]) + 0.5 * (co + no[k]) for k in range(6)]
        diag = ((full[0] + full[1]) + (full[2] + full[3])) + (full[4] + full[5])
        inv = jnp.where(inside, 1.0 / diag, 0.0)
        return [jnp.where(inside, f * inv, 0.0) for f in full], diag, inv

    gather_wait(lab_all, 2, True)
    blocks = [(sx, bx) for sx, bx in ((-1, 1), (0, 0), (0, 1), (1, 0))]
    lines = [(0, 0), (0, 1), (1, 0), (-1, 1)]
    span = lab.shape[2]
    for z in range(2):
        core = iz if z == 0 else 1 - iz
        for i, (sx, bx) in enumerate(blocks):
            for j, (sy, by) in enumerate(lines):
                px, py = jnp.clip(ix + sx, 0, nx - 1), jnp.clip(iy + sy, 0, ny - 1)
                at = (z * 4 + i) * 4 + j
                tall[at : at + 1, 0:LANES] = lab_all[(px * ny + py) * nz + core]
    near_labels = tall[0:32, 0:LANES]
    order = lax.bitwise_and(lax.broadcasted_iota(jnp.int32, (32, LANES), 0), 15)
    segment = jnp.zeros((32, LANES), jnp.int32)
    for i, (_, bx) in enumerate(blocks):
        for j, (_, by) in enumerate(lines):
            segment = jnp.where(order == i * 4 + j, bx * lab.shape[1] + by, segment)
    lined = near_labels
    for k in range(1, LANES // span):
        lined = jnp.where(segment == k, pltpu.roll(near_labels, LANES - k * span, 1), lined)
    stretched = jnp.dot(lined[0:16], copy_matrix(LANES, Z1, 2), preferred_element_type=F32)
    edge_labels = jnp.where(iz == 0, lined[16:32, 0:1], lined[16:32, span - 1 : span])
    edge_labels = jnp.broadcast_to(edge_labels, (16, LANES))
    group = lax.shift_right_logical(g1.row, 2)
    pack_group = lax.shift_right_logical(pack_row, 2)
    pack_block = lax.shift_right_logical(pack_x, 2)
    packed_labels = jnp.zeros((RE, LANES), F32)
    for i in range(4):
        block_labels = jnp.zeros((RE, Z1), F32)
        for j in range(4):
            at = i * 4 + j
            block_labels = jnp.where(
                group == j, jnp.broadcast_to(stretched[at : at + 1], (RE, Z1)), block_labels
            )
            packed_labels = jnp.where(
                (pack_group == j) & (pack_block == i),
                jnp.broadcast_to(edge_labels[at : at + 1], (RE, LANES)),
                packed_labels,
            )
        block_outer = jnp.where(block_labels == 0.0, 3.0, 1.0)
        for p in range(4 * i, 4 * i + 4):
            ee[OUTER1, p] = jnp.where(inside1(p), block_outer, 0.0)
    zp1[OUTER1] = jnp.where(pack_inside, jnp.where(packed_labels == 0.0, 3.0, 1.0), 0.0)
    wide_arrive(0)
    for p in range(1, XE - 1):
        ci, ni = near1(lambda p: ee[INNER1, p], lambda p: zp1[INNER1, :, p : p + 1], p, edge=True)
        co, no = near1(lambda p: ee[OUTER1, p], lambda p: zp1[OUTER1, :, p : p + 1], p, edge=True)
        full, diag, inv = scaled_wide(ci, ni, co, no, inside1(p))
        full[4] = jnp.where(first1, 0.0, full[4])
        full[5] = jnp.where(last1, 0.0, full[5])
        for d in range(6):
            c1[d, p] = full[d]
        if GHOST <= p < X1 + GHOST:
            d1[p - GHOST] = diag[0:R1]
            b1[p - GHOST] = inv[0:R1]
    ci, co = zp1[INNER1], zp1[OUTER1]
    full, _, _ = scaled_wide(
        ci,
        near_pack(lambda p: ee[INNER1, p], ci, 0, XE),
        co,
        near_pack(lambda p: ee[OUTER1, p], co, 0, XE),
        pack_inside,
    )
    for d in range(6):
        cz1[d] = full[d]

    def stencil(b, c, near):
        a = b + c(0) * near[0]
        e = c(1) * near[1] + c(2) * near[2]
        f = c(3) * near[3] + c(4) * near[4]
        return (a + c(5) * near[5]) + (e + f)

    def update1(src, pack, p):
        val, near = near1(lambda p: src[p], lambda p: pack[:, p : p + 1], p)
        return val, stencil(ee[RHS1, p], lambda d: c1[d, p], near)

    def half1(src, pack, dst, colour, planes):
        for p in planes:
            val, new = update1(src, pack, p)
            dst[p] = jnp.where(g1.colour(p, colour), new, val)

    def half_pack(src, pack, dst, colour, first, last):
        val = pack[...]
        near = near_pack(lambda p: src[p], val, first, last)
        new = stencil(zp1[RHS1], lambda d: cz1[d], near)
        dst[...] = jnp.where(pack_own[colour], new, val)

    half_sweep(3, halo0, RED, va, vb, c0, b0, 1)
    publish(4, halo0, BLACK, vb)

    XG, RG, ZG = in2.shape
    XH, RH = XG // 2, RG // 2
    g2 = Grid(XG, RG, ZG)
    g3 = Grid(XH, RH, ZG)
    def unpack(tile, dst):
        for px in range(nx):
            for py in range(ny // 2):
                lows, highs = [], []
                for part in range(2):
                    base = (px * ny + 2 * py + part) * nz
                    s0, s1 = tile(base), tile(base + 1)
                    lows.append(jnp.where(tile_lane < half, s0, pltpu.roll(s1, half, 1)))
                    highs.append(jnp.where(tile_lane < half, pltpu.roll(s0, half, 1), s1))
                for xhi, pair in enumerate((lows, highs)):
                    p = px * X2 + xhi * 2
                    dst[p, py * 8 : py * 8 + 8, :] = jnp.where(tile_row < R2, pair[0], pltpu.roll(pair[1], R2, 0))
                    dst[p + 1, py * 8 : py * 8 + 8, :] = jnp.where(
                        tile_row < R2, pltpu.roll(pair[0], R2, 0), pair[1]
                    )

    def whole_neighbours(grid, planes, x, last, mask):
        val = planes(x)
        zero = jnp.zeros_like(val)
        xm = planes(x - 1) if x > 0 else zero
        xp = planes(x + 1) if x < grid.planes - 1 else zero
        near = [
            xm,
            xp,
            pltpu.roll(val, 1, 0),
            pltpu.roll(val, grid.rows - 1, 0),
            pltpu.roll(val, 1, 1),
            pltpu.roll(val, grid.lanes - 1, 1),
        ]
        if mask:
            near[2] = jnp.where(grid.row == 0, 0.0, near[2])
            near[3] = jnp.where(grid.row == grid.rows - 1, 0.0, near[3])
            near[4] = jnp.where(grid.lane == 0, 0.0, near[4])
            near[5] = jnp.where(grid.lane >= last, 0.0, near[5])
        return val, near

    def whole_couplings(grid, inner, outer, last, c, d, b):
        for x in range(grid.planes):
            ci, ni = whole_neighbours(grid, lambda x: inner[x], x, last, True)
            co, no = whole_neighbours(grid, lambda x: outer[x], x, last, True)
            full = [jnp.minimum(ci, ni[k]) + 0.5 * (co + no[k]) for k in range(6)]
            diag = ((full[0] + full[1]) + (full[2] + full[3])) + (full[4] + full[5])
            if last < grid.lanes - 1:
                diag = jnp.where(grid.lane <= last, diag, 1.0)
            inv = 1.0 / diag
            edges = (
                None,
                None,
                grid.row == 0,
                grid.row == grid.rows - 1,
                grid.lane == 0,
                grid.lane >= last,
            )
            for k in range(6):
                f = full[k] * inv
                if edges[k] is not None:
                    f = jnp.where(edges[k], 0.0, f)
                if last < grid.lanes - 1:
                    f = jnp.where(grid.lane <= last, f, 0.0)
                c[k, x] = f
            if d is not None:
                d[x] = diag
            b[x] = inv

    def whole_update(grid, planes, c, b, x):
        val, near = whole_neighbours(grid, planes, x, None, False)
        a = b[x] + c[2, x] * near[2]
        e = c[3, x] * near[3] + c[4, x] * near[4]
        a = a + c[5, x] * near[5]
        if x > 0:
            a = a + c[0, x] * near[0]
        if x < grid.planes - 1:
            e = e + c[1, x] * near[1]
        return val, a + e

    def restrict2(plane, factor):
        pieces = [halve_rows(tmp, x, plane(2 * x) + plane(2 * x + 1)) for x in range(XH)]
        for x in range(XH):
            tall[x * RH : (x + 1) * RH, 0:ZG] = pieces[x]
        whole = dot(tall[0 : XH * RH, 0:ZG], narrow_low) * factor
        return [whole[x * RH : (x + 1) * RH] for x in range(XH)]

    def mix(x, a, b):
        return jnp.where(g0.colour(x, 0), a, pltpu.roll(b, 1, 1))

    across = jnp.zeros((R0, LANES), F32)
    face_lane = lax.broadcasted_iota(jnp.int32, (R0, LANES), 1)
    for x in range(X0):
        along_y = jnp.where(even_row, c0[2, x], c0[3, x])
        along_x = c0[x % 2, x]
        if x == 0 or x == X0 - 1:
            xs0[x // (X0 - 1), MIXED] = mix(x, c0[x % 2, x], along_y)
        val = mix(x, jnp.where(g0.row < R0 // 2, c0[2, x], c0[3, x]), along_x)
        ys0[0, MIXED, x : x + 1, :] = val[0:1]
        ys0[1, MIXED, x : x + 1, :] = val[R0 - 1 :]
        toward = jnp.where(iz == 0, c0[5, x, :, Z0 - LANES :], c0[4, x, :, 0:LANES])
        outs = [toward] + [
            jnp.where(iz == 0, f[:, Z0 - LANES :], f[:, 0:LANES]) for f in (along_x, along_y)
        ]
        for k, end in enumerate(outs):
            at = k * X0 + x
            across = jnp.where(face_lane == at, pltpu.roll(end, at + 1 - iz, 1), across)
    zs0[MIXED] = across
    def residual0(x):
        val, new = update(halo0, BLACK, lambda x: vb[x], c0, b0, x)
        mixed[x] = jnp.where(g0.colour(x, 0), new, mixed[x])
        return d0[x] * (new - val)

    for x, val in enumerate(restrict0(residual0, 0.5, 0, inner_first(4, X1))):
        ee[RHS1, GHOST + x, 0:R1, :] = val * b1[x]
    wide_publish(1)
    halo0.put(READY, mixed)
    send(5)
    gather_wait(gc, 0, True)
    unpack(lambda t: gc[t], in2)
    for t in range(total):
        tall[t : t + 1, 0:LANES] = lab_all[t]
    k = lax.broadcasted_iota(jnp.int32, (LANES, LANES), 0)
    j = lax.broadcasted_iota(jnp.int32, (LANES, LANES), 1)
    from_lane = lax.div(j, half) * (lab.shape[1] * span) + lax.div(lax.rem(j, half), half // span)
    every = [
        jnp.dot(
            tall[0:total, 0:LANES],
            jnp.where(k == from_lane + by * span, 1.0, 0.0).astype(F32),
            preferred_element_type=F32,
        )
        for by in range(2)
    ]
    first_rows = lax.rem(tile_row, R2) < R2 // 2

    def label_tile(t):
        pair = [jnp.broadcast_to(e[t : t + 1], (8, LANES)) for e in every]
        return jnp.where(jnp.where(first_rows, pair[0], pair[1]) == 0.0, 3.0, 1.0)

    unpack(label_tile, out2)
    whole_couplings(g2, in2, out2, ZG - 1, c2, d2, b2)
    for x, val in enumerate(restrict2(lambda x: in2[x], 0.125)):
        v3[x] = val
    for x, val in enumerate(restrict2(lambda x: out2[x], 0.125)):
        v2a[x, 0:RH] = val
    whole_couplings(g3, v3, v2a.at[:, 0:RH], ZG // 2 - 1, c3, None, b3)

    XP = XH // 2
    own = (g3.even, g3.odd)

    def pack(colour, near, far):
        return jnp.where(own[colour], near, far)

    for colour in range(2):
        for p in range(XP):
            a, z = 2 * p, 2 * p + 1
            k3[colour * 6, p] = pack(colour, c3[1, a], c3[0, z])
            k3[colour * 6 + 1, p] = pack(colour, c3[0, a], c3[1, z])
            for k in range(2, 6):
                k3[colour * 6 + k, p] = pack(colour, c3[k, a], c3[k, z])

    wide_arrive(1)
    ring = GHOST - 1
    for p in range(ring - 1, XE - ring + 1):
        v1a[p] = jnp.where(g1.colour(p, 0), ee[RHS1, p], 0.0)
    z1a[...] = jnp.where(pack_own[0], zp1[RHS1], 0.0)
    half_pack(v1a, z1a, z1b, 1, ring, XE - ring)
    half1(v1a, z1a, v1b, 1, range(ring, XE - ring))

    def residual1(x):
        val, new = update1(v1b, z1b, GHOST + x)
        return d1[x] * (new - val)[0:R1]

    gr_own[...] = restrict1(residual1, 0.5)
    gather_send(gr_own, gr, 1)
    for p in (0, 1, XE - 2, XE - 1):
        v1a[p] = jnp.where(g1.colour(p, 0), ee[RHS1, p], 0.0)
    half_pack(v1a, z1a, z1b, 1, 0, XE)
    half1(v1a, z1a, v1b, 1, (1, 2, XE - 3, XE - 2))
    gather_wait(gr, 1, True)
    unpack(lambda t: gr[t], v2b)
    for x in range(XG):
        b2[x] = v2b[x] * b2[x]
        v2a[x] = jnp.where(g2.colour(x, 0), b2[x], 0.0)
    for x in range(XG):
        val, new = whole_update(g2, lambda x: v2a[x], c2, b2, x)
        v2b[x] = jnp.where(g2.colour(x, 1), new, val)

    def residual2(x):
        val, new = whole_update(g2, lambda x: v2b[x], c2, b2, x)
        return d2[x] * (new - val)

    for x, val in enumerate(restrict2(residual2, 0.5)):
        b3[x] = val * b3[x]

    for colour in range(2):
        for p in range(XP):
            h3[colour, p] = pack(colour, b3[2 * p], b3[2 * p + 1])
    none = jnp.zeros((RH, ZG), F32)

    def relaxed(colour, other):
        fresh = []
        for p in range(XP):
            val, at = other[p], colour * 6
            before = other[p - 1] if p > 0 else none
            after = other[p + 1] if p < XP - 1 else none
            i = h3[colour, p] + k3[at, p] * val
            j = k3[at + 1, p] * pack(colour, before, after) + k3[at + 2, p] * pltpu.roll(val, 1, 0)
            l = k3[at + 3, p] * pltpu.roll(val, RH - 1, 0) + k3[at + 4, p] * pltpu.roll(val, 1, 1)
            fresh.append((i + k3[at + 5, p] * pltpu.roll(val, ZG - 1, 1)) + (j + l))
        return fresh

    def coarse(step, state):
        red = relaxed(0, state[XP:])
        black = relaxed(1, red)
        return tuple(red + black)

    state = lax.fori_loop(0, COARSE_SWEEPS, coarse, (none,) * (2 * XP))
    solved = []
    for p in range(XP):
        solved.append(pack(0, state[p], state[XP + p]))
        solved.append(pack(1, state[p], state[XP + p]))
    for x in range(XH):
        tall[x * RH : (x + 1) * RH, 0:ZG] = solved[x]
    wide = dot(tall[0 : XH * RH, 0:ZG], double12)
    for x in range(XH):
        corr = double_rows(tmp, x, wide[x * RH : (x + 1) * RH])
        v2a[2 * x] = v2b[2 * x] + corr
        v2a[2 * x + 1] = v2b[2 * x + 1] + corr
    for colour, src, dst in ((0, v2a, v2b), (1, v2b, v2a)):
        for x in range(XG):
            val, new = whole_update(g2, lambda x: src[x], c2, b2, x)
            dst[x] = jnp.where(g2.colour(x, colour), new, val)

    row_shift = lax.rem(RG - iy * R2, RG)
    lane_shift = lax.rem(ZG - iz * half, ZG)
    edge2 = GHOST // 2
    rows2 = R2 + 2 * edge2
    planes2 = X2 + 2 * edge2
    for k in range(planes2):
        part = v2a[jnp.clip(ix * X2 + k - edge2, 0, XG - 1)]
        part = pltpu.roll(pltpu.roll(part, row_shift, 0), lane_shift, 1)
        tall[k * rows2 : (k + 1) * rows2, 0:ZG] = jnp.where(
            tile_row < R2 + edge2, part[0:rows2], part[RG - rows2 : RG]
        )
    source = lax.broadcasted_iota(jnp.int32, (ZG, LANES), 0)
    target = lax.broadcasted_iota(jnp.int32, (ZG, LANES), 1)
    target = lax.div(target, 2 * XE)
    pick = jnp.where(source == jnp.where(iz == 0, half + target, ZG - 1 - target), 1.0, 0.0).astype(F32)
    coarse_rows = tall[0 : planes2 * rows2, 0:ZG]
    wide = dot(coarse_rows, double12)
    sides = dot(coarse_rows, pick)
    acc = jnp.zeros((rows2, LANES), F32)
    tile_plane = lax.div(jnp.bitwise_and(tile_lane, XE - 1), 2)
    for k in range(planes2):
        acc = jnp.where(tile_plane == k, sides[k * rows2 : (k + 1) * rows2], acc)
    z1a[...] = z1b[...] + jnp.where(pack_inside, double_rows(tmp, 0, acc), 0.0)
    for k in range(planes2):
        corr = double_rows(tmp, k, wide[k * rows2 : (k + 1) * rows2])
        for p in (2 * k, 2 * k + 1):
            if 0 < p < XE - 1:
                v1a[p] = v1b[p] + jnp.where(inside1(p), corr, 0.0)
    half_pack(v1a, z1a, z1b, 0, 1, XE - 1)
    half1(v1a, z1a, v1b, 0, range(2, XE - 2))
    half_pack(v1b, z1b, z1a, 1, 2, XE - 2)
    half1(v1b, z1b, v1a, 1, range(3, XE - 3))

    def enlarge(count, read, write):
        for x in range(count):
            tall[x * R1 : (x + 1) * R1, 0:Z1] = read(x)
        wide = dot(tall[0 : count * R1, 0:Z1], double01)
        for x in range(count):
            write(x, double_rows(tmp, x, wide[x * R1 : (x + 1) * R1]))

    def inside(x, corr):
        va[2 * x] = vb[2 * x] + corr
        va[2 * x + 1] = vb[2 * x + 1] + corr

    enlarge(X1, lambda x: v1a[GHOST + x, 0:R1, :], inside)
    arrive(5)
    diagonal = tile_lane == tile_row + GHOST
    stack, lined_stack = [], []
    own_pack = jnp.zeros((RE, LANES), F32)
    for p in range(GHOST, XE - GHOST):
        own_pack = jnp.where(pack_lane == p, pltpu.roll(v1a[p], p + 1 - iz, 1), own_pack)
    for k in range(2):
        p, own = (GHOST - 1, GHOST) if k == 0 else (X1 + GHOST, X1 + GHOST - 1)
        val, near = near1(lambda p: v1a[p], lambda p: z1a[:, p : p + 1], p, edge=True)
        stack += [val[0:R1]] + [(other - val)[0:R1] for other in (v1a[own], near[2], near[3])]
        lined_stack.append(((near[4] - val)[0:R1], (near[5] - val)[0:R1]))
    for k in range(2):
        row, own = (RE - 1, 0) if k == 0 else (R1, R1 - 1)
        for p in range(GHOST - 1, X1 + GHOST + 1):
            yrim[k, p : p + 1, :] = v1a[p, row : row + 1, :]
            if GHOST <= p < X1 + GHOST:
                yrim[2 + k, p : p + 1, :] = v1a[p, own : own + 1, :]
        val = yrim[k, GHOST : X1 + GHOST, :]
        others = [
            yrim[2 + k, GHOST : X1 + GHOST, :],
            yrim[k, GHOST - 1 : X1 + GHOST - 1, :],
            yrim[k, GHOST + 1 : X1 + GHOST + 1, :],
        ]
        stack += [val] + [other - val for other in others]
        line = jnp.where(diagonal, jnp.broadcast_to(z1a[row : row + 1, :], (8, LANES)), 0.0)
        column = jnp.broadcast_to(jnp.sum(line, axis=1, keepdims=True), (8, LANES))
        back = jnp.where(tile_lane == 0, jnp.where(iz == 0, 0.0, column), pltpu.roll(val, 1, 1))
        ahead = jnp.where(tile_lane == Z1 - 1, jnp.where(iz == 0, column, 0.0), pltpu.roll(val, Z1 - 1, 1))
        lined_stack.append((back - val, ahead - val))
    val = z1a[...]
    shifts = [pltpu.roll(val, 1, 0), pltpu.roll(val, RE - 1, 0), pltpu.roll(val, 1, 1), pltpu.roll(val, LANES - 1, 1)]
    face = [val, own_pack - val] + [other - val for other in shifts]
    face = [pltpu.roll(f[0:R1], LANES - GHOST, 1) for f in face]
    stack += face[:4]
    lined_stack.append((face[4], face[5]))
    for i, piece in enumerate(stack):
        tall[i * R1 : (i + 1) * R1, 0:Z1] = piece
    for i, (back, ahead) in enumerate(lined_stack):
        tall2[i * R1 : (i + 1) * R1, 0:Z1] = back
        tall2[i * R1 : (i + 1) * R1, Z1 : 2 * Z1] = ahead
    k = lax.broadcasted_iota(jnp.int32, (2 * Z1, Z0), 0)
    j = lax.broadcasted_iota(jnp.int32, (2 * Z1, Z0), 1)
    source = lax.shift_right_logical(j, 1) + Z1 * jnp.bitwise_and(j, 1)
    big = dot(tall[0 : len(stack) * R1, 0:Z1], double01)
    lined_big = dot(tall2[0 : len(lined_stack) * R1, :], jnp.where(k == source, 1.0, 0.0).astype(F32))

    def woven(slot, first, second):
        parts = []
        for k in range(Z0 // LANES):
            at = 2 * slot + k
            tmp[at, pl.ds(0, R1, 2), :] = first[:, k * LANES : (k + 1) * LANES]
            tmp[at, pl.ds(1, R1, 2), :] = second[:, k * LANES : (k + 1) * LANES]
            parts.append(tmp[at, 0:R0, :])
        return jnp.concatenate(parts, axis=1)

    def finished(k):
        piece = [big[(4 * k + i) * R1 : (4 * k + i + 1) * R1] for i in range(4)]
        lines = lined_big[k * R1 : (k + 1) * R1]
        at = 4 * (k % 2)
        return (
            woven(at, piece[0], piece[0]),
            woven(at + 1, piece[1], piece[1]),
            woven(at + 2, piece[2], piece[3]),
            woven(at + 3, lines, lines),
        )

    for k in range(4):
        ref, side = (xh0, k) if k < 2 else (yh0, k - 2)
        corr, toward, beside, lengthwise = finished(k)
        ref[side, FIXED] = ref[side, BLACK] + corr
        first, second = ref[side, MIXED], ref[side, READY]
        ref[side, LAST] = ((second + corr) + first * toward) + (
            pltpu.roll(first, Z0 - 1, 1) * beside + pltpu.roll(second, Z0 - 1, 1) * lengthwise
        )
    corr, toward, beside, sideways = [f[:, 0:LANES] for f in finished(4)]
    zh0[FIXED] = zh0[BLACK] + corr
    first = zh0[MIXED]
    zh0[LAST] = ((zh0[READY] + corr) + first * toward) + (
        pltpu.roll(first, LANES - X0, 1) * sideways + pltpu.roll(first, LANES - 2 * X0, 1) * beside
    )
    half_sweep(None, halo0, FIXED, va, vb, c0, b0, 0)
    half_sweep(None, halo0, LAST, vb, ext_out, c0, b0, 1)

    for number in range(len(EXCHANGES)):
        sent(number)
    for number in range(len(WIDE)):
        wide_sent(number)
    gather_wait(gc, 0, False)
    gather_wait(gr, 1, False)
    gather_wait(lab_all, 2, False)


def finish(*refs):
    count = (len(refs) - 1) // 2
    sem = refs[-1]
    copies = [pltpu.make_async_copy(refs[i], refs[count + i], sem.at[i]) for i in range(count)]
    for copy in copies:
        copy.start()
    for copy in copies:
        copy.wait()


def solution(mesh):
    nx, ny, nz = (mesh.shape[a] for a in ("gx", "gy", "gz"))
    spec = P("gx", "gy", "gz")

    def on_device(membrane, recovery, extracellular, fiber_scale, labels):
        X, R, Z = membrane.shape
        X1, R1, Z1 = X // 2, R // 2, Z // 2
        XG, RG, ZG = nx * X // 4, ny * R // 4, nz * Z // 4
        assert nz == 2 and ny % 2 == 0 and ZG == LANES and Z1 == LANES
        assert R1 == 8 and X1 == 8 and X % 8 == 0
        total = nx * ny * nz
        assert labels.shape == (2, 2, LANES // 4)
        f0 = 11
        field = (X, R, Z)
        lvl1 = (X1, R1, Z1)
        whole = (XG, RG, ZG)
        third = (XG // 2, RG // 2, ZG)

        def v(*shape):
            return pltpu.VMEM(shape, F32)

        def faces(f, x, r, z):
            return [v(2, f, r, z), v(2, f, x, z), v(f, r, LANES)] * 2

        anywhere = pl.BlockSpec(memory_space=pl.ANY)
        scratch = [v(*field)] * 4 + [pltpu.VMEM(labels.shape, jnp.int32), pltpu.SemaphoreType.DMA((5,))]
        scratch += faces(f0, *field)
        scratch += [v(*field), v(*field), v(*field), v(6, *field), v(6, *field), v(*field), v(*field)]
        scratch += [v(*field), v(*field)]
        scratch += [
            v(2 * max(X1, XG // 2), max(R, RG), LANES),
            v(max(X1 * R1, (XG // 2) * (RG // 2), 2 * X1 * R1, 20 * R1, total), Z),
        ]
        XE, RE = X1 + 2 * GHOST, R1 + 2 * GHOST
        assert GHOST * XE <= LANES and 2 * GHOST == R1 and GHOST <= X1
        wide, pack = (XE, RE, Z1), (RE, LANES)
        scratch += [v(3, *wide), v(2, 3, X1 // 2, R1, Z1), v(2, 3, XE // 2, R1, Z1), v(3, R1, LANES)]
        scratch += [v(9, 3, R1, LANES), v(3, *pack), v(6, *wide), v(6, *pack), v(*lvl1), v(*lvl1)]
        scratch += [v(*wide), v(*wide), v(*pack), v(*pack), v(4, XE, Z1)]
        scratch += [v(*field), v(8 * R1, Z)]
        scratch += [v(1, LANES), v(total, 1, LANES), v(8, LANES), v(total, 8, LANES), v(8, LANES), v(total, 8, LANES)]
        scratch += [v(*whole), v(*whole), v(6, *whole), v(*whole), v(*whole), v(*whole), v(*whole)]
        scratch += [v(6, *third), v(*third), v(*third)]
        packed = (XG // 4, RG // 2, ZG)
        scratch += [v(12, *packed), v(2, *packed)]
        sems = SIDES * len(EXCHANGES)
        scratch += [pltpu.SemaphoreType.DMA((sems,))] * 2
        scratch += [pltpu.SemaphoreType.DMA((WIDE_SIDES * len(WIDE),))] * 2
        scratch += [pltpu.SemaphoreType.DMA((3,))] * 2
        vmem = pl.BlockSpec(memory_space=pltpu.VMEM)
        room = 54400 << 10
        shape = jax.ShapeDtypeStruct(field, F32)
        results = pl.pallas_call(
            functools.partial(kernel, (nx, ny, nz)),
            out_shape=[shape] * 3,
            in_specs=[anywhere] * 5,
            out_specs=[vmem] * 3,
            scratch_shapes=scratch,
            compiler_params=pltpu.CompilerParams(
                collective_id=0, has_side_effects=True, vmem_limit_bytes=room
            ),
        )(membrane, recovery, extracellular, fiber_scale, labels)
        return tuple(
            pl.pallas_call(
                finish,
                out_shape=[shape] * 3,
                in_specs=[vmem] * 3,
                out_specs=[anywhere] * 3,
                scratch_shapes=[pltpu.SemaphoreType.DMA((3,))],
                compiler_params=pltpu.CompilerParams(vmem_limit_bytes=4 << 20),
            )(*results)
        )

    return jax.shard_map(
        on_device,
        mesh=mesh,
        in_specs=(spec,) * 5,
        out_specs=(spec,) * 3,
        check_vma=False,
    )
```

```python
import functools

import jax
import jax.numpy as jnp
from jax import lax
from jax.experimental import pallas as pl
from jax.experimental.pallas import tpu as pltpu
from jax.sharding import PartitionSpec as P

COARSE_SWEEPS = 8
TIME_STEP = 0.05
ionic_gain = 8.0
ionic_onset = 0.15
recovery_rate = 0.01
MESH = pl.DeviceIdType.MESH
LOGICAL = pl.DeviceIdType.LOGICAL
LANES = 128
F32 = jnp.float32

INNER, U, OUTER, V, NEXT, RED, BLACK, MIXED, READY, FIXED, LAST = range(11)
INNER1, OUTER1, RHS1 = range(3)
GHOST = 4
EXCHANGES = (
    (INNER, 2),
    (V, 1),
    (NEXT, 1),
    (RED, 1),
    (BLACK, 1),
    (MIXED, 2),
)
SIDES = 5
WIDE = ((INNER1, 1), (RHS1, 1))
STEPS = (-1, 0, 1)
WIDE_SIDES = 17


def dot(a, b):
    high = a.astype(jnp.bfloat16)
    rest = a - high.astype(F32)
    middle = rest.astype(jnp.bfloat16)
    low = (rest - middle.astype(F32)).astype(jnp.bfloat16)
    chosen = b.astype(jnp.bfloat16)
    rows = a.shape[0]
    both = jnp.dot(jnp.concatenate([low, middle, high], axis=0), chosen, preferred_element_type=F32)
    parts = [both[i * rows : (i + 1) * rows] for i in range(3)]
    return (parts[0] + parts[1]) + parts[2]


def pair_matrix(rows, cols, offset):
    j = lax.broadcasted_iota(jnp.int32, (rows, cols), 0)
    k = lax.broadcasted_iota(jnp.int32, (rows, cols), 1)
    return jnp.where(lax.shift_right_logical(j, 1) + offset == k, 1.0, 0.0).astype(F32)


def copy_matrix(rows, cols, shift):
    k = lax.broadcasted_iota(jnp.int32, (rows, cols), 0)
    j = lax.broadcasted_iota(jnp.int32, (rows, cols), 1)
    return jnp.where(lax.shift_right_logical(j, shift) == k, 1.0, 0.0).astype(F32)


class Grid:
    def __init__(self, planes, rows, lanes):
        self.planes, self.rows, self.lanes = planes, rows, lanes
        self.row = lax.broadcasted_iota(jnp.int32, (rows, lanes), 0)
        self.lane = lax.broadcasted_iota(jnp.int32, (rows, lanes), 1)
        self.even = jnp.bitwise_and(self.row + self.lane, 1) == 0
        self.odd = jnp.bitwise_and(self.row + self.lane, 1) == 1

    def colour(self, x, colour):
        return self.even if (x + colour) % 2 == 0 else self.odd


class Halo:
    def __init__(self, grid, refs, iz):
        self.grid, self.iz = grid, iz
        self.xs, self.ys, self.zs, self.xh, self.yh, self.zh = refs
        self.flane = lax.broadcasted_iota(jnp.int32, (grid.rows, LANES), 1)

    def faces(self, slot, planes):
        g = self.grid
        acc = jnp.zeros((g.rows, LANES), F32)
        for x, val in planes:
            self.ys[0, slot, x : x + 1, :] = val[0:1]
            self.ys[1, slot, x : x + 1, :] = val[g.rows - 1 :]
            if g.lanes > LANES:
                end = jnp.where(self.iz == 0, val[:, g.lanes - LANES :], val[:, :LANES])
            else:
                end = val
            acc = jnp.where(self.flane == x, pltpu.roll(end, x + 1 - self.iz, 1), acc)
            yield
        self.zs[slot] = acc

    def put_ends(self, slot, ref):
        self.xs[0, slot] = ref[0]
        self.xs[1, slot] = ref[self.grid.planes - 1]

    def put_rest(self, slot, ref):
        for _ in self.faces(slot, [(x, ref[x]) for x in range(self.grid.planes)]):
            pass

    def put(self, slot, ref):
        self.put_ends(slot, ref)
        self.put_rest(slot, ref)

    def neighbours(self, slot, planes, x, edge=False):
        g = self.grid
        val = planes(x)
        xm = planes(x - 1) if x > 0 else self.xh[0, slot]
        xp = planes(x + 1) if x < g.planes - 1 else self.xh[1, slot]
        shape = (g.rows, g.lanes)
        low = jnp.broadcast_to(self.yh[0, slot, x : x + 1, :], shape)
        high = jnp.broadcast_to(self.yh[1, slot, x : x + 1, :], shape)
        ym = jnp.where(g.row == 0, low, pltpu.roll(val, 1, 0))
        yp = jnp.where(g.row == g.rows - 1, high, pltpu.roll(val, g.rows - 1, 0))
        side = jnp.broadcast_to(self.zh[slot, :, x : x + 1], shape)
        side_m, side_p = side, side
        if edge:
            side_m = jnp.where(self.iz == 0, 0.0, side)
            side_p = jnp.where(self.iz == 0, side, 0.0)
        zm = jnp.where(g.lane == 0, side_m, pltpu.roll(val, 1, 1))
        zp = jnp.where(g.lane == g.lanes - 1, side_p, pltpu.roll(val, g.lanes - 1, 1))
        return val, (xm, xp, ym, yp, zm, zp)


def halve_rows(tmp, slot, val):
    rows, lanes = val.shape
    parts = []
    for k in range(lanes // LANES):
        at = 2 * slot + k
        tmp[at, 0:rows, :] = val[:, k * LANES : (k + 1) * LANES]
        parts.append(tmp[at, pl.ds(0, rows // 2, 2), :] + tmp[at, pl.ds(1, rows // 2, 2), :])
    return parts[0] if len(parts) == 1 else jnp.concatenate(parts, axis=1)


def double_rows(tmp, slot, val):
    rows, lanes = val.shape
    parts = []
    for k in range(lanes // LANES):
        at = 2 * slot + k
        piece = val[:, k * LANES : (k + 1) * LANES]
        tmp[at, pl.ds(0, rows, 2), :] = piece
        tmp[at, pl.ds(1, rows, 2), :] = piece
        parts.append(tmp[at, 0 : 2 * rows, :])
    return parts[0] if len(parts) == 1 else jnp.concatenate(parts, axis=1)


def kernel(counts, *refs):
    sources, (mem_out, rec_out, ext_out) = refs[:5], refs[5:8]
    refs = refs[8:]
    mem, rec, ext, fib, lab, in_sem = refs[:6]
    refs = (None,) + refs
    (xs0, ys0, zs0, xh0, yh0, zh0) = refs[7:13]
    (in0, out0, uu, w0, c0, d0, b0, va, vb, tmp, tall) = refs[13:24]
    (ee, ys1, yr1, zs1, zr1, zp1, c1, cz1, d1, b1, v1a, v1b, z1a, z1b, yrim, mixed, tall2) = refs[24:41]
    (gc_own, gc, gr_own, gr, in2, out2, c2, d2, b2, v2a, v2b) = refs[41:52]
    (c3, b3, v3, k3, h3, send_sem, recv_sem, wide_send, wide_recv, gs_sem, gr_sem) = refs[52:]
    nx, ny, nz = counts
    ix, iy, iz = lax.axis_index("gx"), lax.axis_index("gy"), lax.axis_index("gz")
    me = (ix * ny + iy) * nz + iz
    total = nx * ny * nz

    loads = [
        pltpu.make_async_copy(src, dst, in_sem.at[i])
        for i, (src, dst) in enumerate(zip(sources, (mem, rec, ext, fib, lab)))
    ]
    for i in (4, 3, 0, 2, 1):
        loads[i].start()

    barrier = pltpu.get_barrier_semaphore()

    def others(body):
        for i in sorted(range(1, total), key=lambda i: (abs(i // nz % ny * 2 - ny), i)):
            dev = me + i
            body(jnp.where(dev >= total, dev - total, dev))

    others(lambda dev: pl.semaphore_signal(barrier, inc=1, device_id=dev, device_id_type=LOGICAL))

    def clear(missing, ref, side):
        def fill():
            ref[side] = jnp.zeros(ref.at[side].shape, F32)

        pl.when(missing)(fill)

    X1, R1, Z1 = mem.shape[0] // 2, mem.shape[1] // 2, mem.shape[2] // 2
    XE, RE = X1 + 2 * GHOST, R1 + 2 * GHOST
    clear(ix == 0, xh0, 0)
    clear(ix == nx - 1, xh0, 1)
    clear(iy == 0, yh0, 0)
    clear(iy == ny - 1, yh0, 1)
    for slot in range(3):
        for p in range(GHOST):
            clear(ix == 0, ee, (slot, p))
            clear(ix == nx - 1, ee, (slot, XE - 1 - p))
    for load in loads:
        load.wait()

    g0 = Grid(*mem.shape)
    g1 = Grid(XE, RE, Z1)
    halo0 = Halo(g0, (xs0, ys0, zs0, xh0, yh0, zh0), iz)

    def copies(number):
        first, slots = EXCHANGES[number]
        h = halo0
        part = pl.ds(first, slots)
        plan = (
            (h.xs.at[0, part], h.xh.at[1, part], (ix - 1, iy, iz), ix > 0, ix < nx - 1),
            (h.xs.at[1, part], h.xh.at[0, part], (ix + 1, iy, iz), ix < nx - 1, ix > 0),
            (h.ys.at[0, part], h.yh.at[1, part], (ix, iy - 1, iz), iy > 0, iy < ny - 1),
            (h.ys.at[1, part], h.yh.at[0, part], (ix, iy + 1, iz), iy < ny - 1, iy > 0),
            (h.zs.at[part], h.zh.at[part], (ix, iy, 1 - iz), None, None),
        )
        for side, (src, dst, dev, goes, comes) in enumerate(plan):
            copy = pltpu.make_async_remote_copy(
                src_ref=src,
                dst_ref=dst,
                send_sem=send_sem.at[number * SIDES + side],
                recv_sem=recv_sem.at[number * SIDES + side],
                device_id=dev,
                device_id_type=MESH,
            )
            yield copy, goes, comes

    ends, rest = slice(0, 2), slice(2, SIDES)

    def send(number, sides=slice(0, SIDES)):
        for copy, goes, _ in list(copies(number))[sides]:
            if goes is None:
                copy.start()
            else:
                pl.when(goes)(copy.start)

    def arrive(number, sides=slice(0, SIDES)):
        for copy, _, comes in list(copies(number))[sides]:
            if comes is None:
                copy.wait_recv()
            else:
                pl.when(comes)(copy.wait_recv)

    def inner_first(number, count):
        arrive(number, rest)
        yield from range(1, count - 1)
        arrive(number, ends)
        yield 0
        yield count - 1

    def publish(number, halo, slot, ref):
        halo.put_ends(slot, ref)
        send(number, ends)
        halo.put_rest(slot, ref)
        send(number, rest)

    def sent(number):
        for copy, goes, _ in copies(number):
            if goes is None:
                copy.wait_send()
            else:
                pl.when(goes)(copy.wait_send)

    here = {-1: ix > 0, 0: None, 1: ix < nx - 1}
    along = {-1: iy > 0, 0: None, 1: iy < ny - 1}

    def both(a, b):
        if a is None or b is None:
            return b if a is None else a
        return jnp.logical_and(a, b)

    def wide_copies(number):
        first, count = WIDE[number]
        part = pl.ds(first, count)
        pairs, edge = X1 // 2, GHOST // 2
        plan = []
        for sx in (-1, 1):
            src = ee.at[part, pl.ds(GHOST if sx < 0 else X1, GHOST), pl.ds(0, R1)]
            dst = ee.at[part, pl.ds(X1 + GHOST if sx < 0 else 0, GHOST), pl.ds(0, R1)]
            plan.append((src, dst, sx, 0, iz))
        for sx in STEPS:
            for sy in (-1, 1):
                mine, theirs = (0, 1) if sy < 0 else (1, 0)
                at = {-1: (0, edge, pairs + edge), 0: (0, pairs, edge), 1: (pairs - edge, edge, 0)}[sx]
                src = ys1.at[mine, part, pl.ds(at[0], at[1])]
                dst = yr1.at[theirs, part, pl.ds(at[2], at[1])]
                plan.append((src, dst, sx, sy, iz))
        for sx in STEPS:
            for sy in STEPS:
                plan.append((zs1.at[part], zr1.at[(1 - sx) * 3 + 1 - sy, part], sx, sy, 1 - iz))
        for side, (src, dst, sx, sy, z) in enumerate(plan):
            copy = pltpu.make_async_remote_copy(
                src_ref=src,
                dst_ref=dst,
                send_sem=wide_send.at[number * WIDE_SIDES + side],
                recv_sem=wide_recv.at[number * WIDE_SIDES + side],
                device_id=(ix + sx, iy + sy, z),
                device_id_type=MESH,
            )
            yield copy, both(here[sx], along[sy]), both(here[-sx], along[-sy])

    def maybe(condition, action):
        if condition is None:
            action()
        else:
            pl.when(condition)(action)

    tile_row = lax.broadcasted_iota(jnp.int32, (8, LANES), 0)
    tile_lane = lax.broadcasted_iota(jnp.int32, (8, LANES), 1)

    def wide_publish(number):
        first, count = WIDE[number]
        for slot in range(first, first + count):
            acc = jnp.zeros((R1, LANES), F32)
            for x in range(X1):
                val = ee[slot, GHOST + x, 0:R1, :]
                for depth in range(GHOST):
                    at = depth * XE + GHOST + x
                    shift = jnp.where(iz == 0, at + 1 + depth, at - depth)
                    acc = jnp.where(tile_lane == at, pltpu.roll(val, shift, 1), acc)
            zs1[slot] = acc
            for k in range(X1 // 2):
                even, odd = ee[slot, GHOST + 2 * k, 0:R1, :], ee[slot, GHOST + 2 * k + 1, 0:R1, :]
                ys1[0, slot, k] = jnp.where(tile_row < GHOST, even, pltpu.roll(odd, GHOST, 0))
                ys1[1, slot, k] = jnp.where(tile_row < GHOST, pltpu.roll(odd, GHOST, 0), even)
        for copy, goes, _ in wide_copies(number):
            maybe(goes, copy.start)

    def keep(condition, val):
        return val if condition is None else jnp.where(condition, val, 0.0)

    def plane_side(p):
        return here[-1 if p < GHOST else (1 if p >= X1 + GHOST else 0)]

    def wide_arrive(number):
        first, count = WIDE[number]
        for copy, _, comes in wide_copies(number):
            maybe(comes, copy.wait_recv)
        low = tile_row >= GHOST
        pe = jnp.bitwise_and(tile_lane, XE - 1)
        for slot in range(first, first + count):
            for p in range(XE):
                after, before = yr1[1, slot, p // 2], yr1[0, slot, p // 2]
                if p % 2:
                    after, before = pltpu.roll(after, GHOST, 0), pltpu.roll(before, GHOST, 0)
                side = plane_side(p)
                after = keep(both(side, along[1]), after)
                before = keep(both(side, along[-1]), before)
                ee[slot, p, R1:RE, :] = jnp.where(low, before, after)
            rows = []
            for sy in STEPS:
                mid = zr1[3 + sy + 1, slot]
                left = keep(here[-1], pltpu.roll(zr1[sy + 1, slot], LANES - X1, 1))
                right = keep(here[1], pltpu.roll(zr1[6 + sy + 1, slot], X1, 1))
                val = jnp.where(pe < GHOST, left, jnp.where(pe >= X1 + GHOST, right, mid))
                rows.append(keep(along[sy], jnp.where(tile_lane < GHOST * XE, val, 0.0)))
            zp1[slot, 0:R1, :] = rows[1]
            zp1[slot, R1:RE, :] = jnp.where(low, rows[0], rows[2])

    def wide_sent(number):
        for copy, goes, _ in wide_copies(number):
            maybe(goes, copy.wait_send)

    def gather_send(own, whole, which):
        def go(dev):
            pltpu.make_async_remote_copy(
                src_ref=own,
                dst_ref=whole.at[me],
                send_sem=gs_sem.at[which],
                recv_sem=gr_sem.at[which],
                device_id=dev,
                device_id_type=LOGICAL,
            ).start()

        others(go)
        whole[pl.ds(me, 1)] = own[...][None]

    def gather_wait(whole, which, recv):
        rest = whole.at[pl.ds(0, total - 1)]
        copy = pltpu.make_async_remote_copy(
            src_ref=rest,
            dst_ref=rest,
            send_sem=gs_sem.at[which],
            recv_sem=gr_sem.at[which],
            device_id=(ix, iy, 1 - iz),
            device_id_type=MESH,
        )
        if recv:
            copy.wait_recv()
        else:
            copy.wait_send()

    X0, R0, Z0 = mem.shape
    X2 = X1 // 2
    R2 = R1 // 2
    half = Z1 // 2

    widen8 = copy_matrix(lab.shape[2], Z0, 3)
    lab_planes = []
    for bx in range(lab.shape[0]):
        wide = jnp.dot(lab[bx].astype(F32), widen8, preferred_element_type=F32)
        lab_planes.append(
            jnp.concatenate(
                [jnp.broadcast_to(wide[by : by + 1], (8, Z0)) for by in range(lab.shape[1])], axis=0
            )
        )

    def label_of(x):
        return lab_planes[x // 8]

    for x in range(X0):
        label = label_of(x)
        in0[x] = jnp.where(label == 1.0, 1.0, jnp.where(label == 2.0, 0.3, 0.0)) * fib[x]
        out0[x] = jnp.where(label == 0.0, 3.0, 1.0)
        uu[x] = mem[x] + ext[x]
    halo0.put(INNER, in0)
    halo0.put(U, uu)
    pl.semaphore_wait(barrier, total - 1)
    send(0)
    halo0.put(V, ext)
    send(1)

    narrow = pair_matrix(Z0, Z1, 0)
    narrow_low = pair_matrix(Z1, Z1, 0)
    narrow_high = pair_matrix(Z1, Z1, half)
    double01 = copy_matrix(Z1, Z0, 1)
    double12 = copy_matrix(Z1, Z1, 1)

    def restrict0(plane, factor, base, order=None):
        for x in order or range(X1):
            tall[base + x * R1 : base + (x + 1) * R1, :] = halve_rows(tmp, x, plane(2 * x) + plane(2 * x + 1))
        whole = dot(tall[base : base + X1 * R1, :], narrow) * factor
        return [whole[x * R1 : (x + 1) * R1] for x in range(X1)]

    def restrict1(plane, factor, order=None):
        rows = [None] * X2
        for x in order or range(X2):
            rows[x] = halve_rows(tmp, x, plane(2 * x) + plane(2 * x + 1))
        low = jnp.concatenate(rows[: X2 // 2], axis=0)
        high = jnp.concatenate(rows[X2 // 2 :], axis=0)
        return (dot(low, narrow_low) + dot(high, narrow_high)) * factor

    for x in inner_first(0, X0):
        centre, near = halo0.neighbours(INNER, lambda x: in0[x], x, edge=True)
        u, near_u = halo0.neighbours(U, lambda x: uu[x], x)
        drive = jnp.zeros_like(u)
        for d in range(6):
            weight = jnp.minimum(centre, near[d])
            w0[d, x] = weight
            drive = drive + weight * (near_u[d] - u)
        m, r = mem[x], rec[x]
        tissue = jnp.where(label_of(x) != 0.0, 1.0, 0.0)
        ionic = ionic_gain * m * (m - ionic_onset) * (m - 1.0) + m * r
        mem_out[x] = m + TIME_STEP * (drive - tissue * ionic)
    publish(2, halo0, NEXT, mem_out)
    for x in range(X0):
        m, r = mem[x], rec[x]
        rec_out[x] = r + TIME_STEP * recovery_rate * (-r - ionic_gain * m * (m - ionic_onset - 1.0))

    for x, val in enumerate(restrict0(lambda x: in0[x], 0.125, 0)):
        ee[INNER1, GHOST + x, 0:R1, :] = val
    wide_publish(0)
    gc_own[...] = restrict1(lambda x: ee[INNER1, GHOST + x, 0:R1, :], 0.125)

    def scaled(grid, weights, centre, near, iz_edges):
        full = [weights[d] + 0.5 * (centre + near[d]) for d in range(6)]
        diag = ((full[0] + full[1]) + (full[2] + full[3])) + (full[4] + full[5])
        inv = 1.0 / diag
        full = [f * inv for f in full]
        low, high = iz_edges
        along_z = jnp.where(even_lane, full[4], full[5])
        full[4] = jnp.where(low, 0.0, full[4])
        full[5] = jnp.where(high, 0.0, full[5])
        return full, diag, inv, along_z

    even_lane = jnp.bitwise_and(g0.lane, 1) == 0
    even_row = jnp.bitwise_and(g0.row, 1) == 0
    first0 = (g0.lane == 0) & (iz == 0)
    last0 = (g0.lane == Z0 - 1) & (iz == nz - 1)
    for side in range(2):
        for ref, has in ((xh0, here), (yh0, along)):
            val = jnp.where(ref[side, INNER] == 0.0, 3.0, 1.0)
            ref[side, OUTER] = jnp.where(has[2 * side - 1], val, 0.0)
    zh0[OUTER] = jnp.where(zh0[INNER] == 0.0, 3.0, 1.0)
    inv0 = vb
    for x in range(X0):
        centre, near = halo0.neighbours(OUTER, lambda x: out0[x], x, edge=True)
        full, diag, inv, along_z = scaled(g0, [w0[d, x] for d in range(6)], centre, near, (first0, last0))
        for d in range(6):
            c0[d, x] = full[d]
        d0[x] = diag
        b0[x] = inv
        mixed[x] = pltpu.roll(along_z, 1, 1)

    def update(halo, slot, planes, c, b, x):
        val, near = halo.neighbours(slot, planes, x)
        a = b[x] + c[0, x] * near[0]
        e = c[1, x] * near[1] + c[2, x] * near[2]
        f = c[3, x] * near[3] + c[4, x] * near[4]
        return val, (a + c[5, x] * near[5]) + (e + f)

    def half_sweep(number, halo, slot, src, dst, c, b, colour):
        planes = halo.grid.planes
        for x in range(planes) if number is None else inner_first(number, planes):
            val, new = update(halo, slot, lambda x: src[x], c, b, x)
            dst[x] = jnp.where(halo.grid.colour(x, colour), new, val)

    arrive(1)
    for x in inner_first(2, X0):
        m, near = halo0.neighbours(NEXT, lambda x: mem_out[x], x)
        rhs = jnp.zeros_like(m)
        for d in range(6):
            rhs = rhs + w0[d, x] * (near[d] - m)
        b0[x] = rhs * b0[x]
        val, new = update(halo0, V, lambda x: ext[x], c0, b0, x)
        va[x] = jnp.where(g0.colour(x, 0), new, val)
    publish(3, halo0, RED, va)
    gather_send(gc_own, gc, 0)

    first1 = (g1.lane == 0) & (iz == 0)
    last1 = (g1.lane == Z1 - 1) & (iz == nz - 1)
    pack_row = lax.broadcasted_iota(jnp.int32, (RE, LANES), 0)
    pack_lane = lax.broadcasted_iota(jnp.int32, (RE, LANES), 1)
    pack_x = jnp.bitwise_and(pack_lane, XE - 1)
    depth_parity = lax.div(pack_lane, XE) + iz + pack_x + pack_row
    pack_own = [jnp.bitwise_and(depth_parity + colour, 1) == 0 for colour in range(2)]

    def row_inside(row):
        return (
            (row < R1)
            | ((row < R1 + GHOST) & (iy < ny - 1))
            | ((row >= R1 + GHOST) & (iy > 0))
        )

    inside_row = row_inside(g1.row)
    pack_inside = (
        row_inside(pack_row)
        & (pack_lane < GHOST * XE)
        & ((pack_x >= GHOST) | (ix > 0))
        & ((pack_x < X1 + GHOST) | (ix < nx - 1))
    )

    def inside1(p):
        side = plane_side(p)
        return inside_row if side is None else inside_row & side

    def near1(planes, pack, p, edge=False):
        val = planes(p)
        side = jnp.broadcast_to(pack(p), (RE, Z1))
        side_m, side_p = side, side
        if edge:
            side_m = jnp.where(iz == 0, 0.0, side)
            side_p = jnp.where(iz == 0, side, 0.0)
        return val, (
            planes(p - 1),
            planes(p + 1),
            pltpu.roll(val, 1, 0),
            pltpu.roll(val, RE - 1, 0),
            jnp.where(g1.lane == 0, side_m, pltpu.roll(val, 1, 1)),
            jnp.where(g1.lane == Z1 - 1, side_p, pltpu.roll(val, Z1 - 1, 1)),
        )

    def near_pack(planes, val, first, last):
        own = jnp.zeros((RE, LANES), F32)
        for p in range(first, last):
            own = jnp.where(pack_lane == p, pltpu.roll(planes(p), p + 1 - iz, 1), own)
        return (
            pltpu.roll(val, 1, 1),
            pltpu.roll(val, LANES - 1, 1),
            pltpu.roll(val, 1, 0),
            pltpu.roll(val, RE - 1, 0),
            jnp.where(pack_lane < XE, own, pltpu.roll(val, XE, 1)),
            pltpu.roll(val, LANES - XE, 1),
        )

    def scaled_wide(ci, ni, co, no, inside):
        full = [jnp.minimum(ci, ni[k]) + 0.5 * (co + no[k]) for k in range(6)]
        diag = ((full[0] + full[1]) + (full[2] + full[3])) + (full[4] + full[5])
        inv = jnp.where(inside, 1.0 / diag, 0.0)
        return [jnp.where(inside, f * inv, 0.0) for f in full], diag, inv

    wide_arrive(0)

    def outer_of(inner):
        return jnp.where(inner == 0.0, 3.0, 1.0)

    for p in range(XE):
        ee[OUTER1, p] = jnp.where(inside1(p), outer_of(ee[INNER1, p]), 0.0)
    zp1[OUTER1] = jnp.where(pack_inside, outer_of(zp1[INNER1]), 0.0)
    for p in range(1, XE - 1):
        ci, ni = near1(lambda p: ee[INNER1, p], lambda p: zp1[INNER1, :, p : p + 1], p, edge=True)
        co, no = near1(lambda p: ee[OUTER1, p], lambda p: zp1[OUTER1, :, p : p + 1], p, edge=True)
        full, diag, inv = scaled_wide(ci, ni, co, no, inside1(p))
        full[4] = jnp.where(first1, 0.0, full[4])
        full[5] = jnp.where(last1, 0.0, full[5])
        for d in range(6):
            c1[d, p] = full[d]
        if GHOST <= p < X1 + GHOST:
            d1[p - GHOST] = diag[0:R1]
            b1[p - GHOST] = inv[0:R1]
    ci, co = zp1[INNER1], zp1[OUTER1]
    full, _, _ = scaled_wide(
        ci,
        near_pack(lambda p: ee[INNER1, p], ci, 0, XE),
        co,
        near_pack(lambda p: ee[OUTER1, p], co, 0, XE),
        pack_inside,
    )
    for d in range(6):
        cz1[d] = full[d]

    def stencil(b, c, near):
        a = b + c(0) * near[0]
        e = c(1) * near[1] + c(2) * near[2]
        f = c(3) * near[3] + c(4) * near[4]
        return (a + c(5) * near[5]) + (e + f)

    def update1(src, pack, p):
        val, near = near1(lambda p: src[p], lambda p: pack[:, p : p + 1], p)
        return val, stencil(ee[RHS1, p], lambda d: c1[d, p], near)

    def half1(src, pack, dst, colour, planes):
        for p in planes:
            val, new = update1(src, pack, p)
            dst[p] = jnp.where(g1.colour(p, colour), new, val)

    def half_pack(src, pack, dst, colour, first, last):
        val = pack[...]
        near = near_pack(lambda p: src[p], val, first, last)
        new = stencil(zp1[RHS1], lambda d: cz1[d], near)
        dst[...] = jnp.where(pack_own[colour], new, val)

    half_sweep(3, halo0, RED, va, vb, c0, b0, 1)
    publish(4, halo0, BLACK, vb)

    XG, RG, ZG = in2.shape
    XH, RH = XG // 2, RG // 2
    g2 = Grid(XG, RG, ZG)
    g3 = Grid(XH, RH, ZG)
    def unpack(tile, dst):
        for px in range(nx):
            for py in range(ny // 2):
                lows, highs = [], []
                for part in range(2):
                    base = (px * ny + 2 * py + part) * nz
                    s0, s1 = tile(base), tile(base + 1)
                    lows.append(jnp.where(tile_lane < half, s0, pltpu.roll(s1, half, 1)))
                    highs.append(jnp.where(tile_lane < half, pltpu.roll(s0, half, 1), s1))
                for xhi, pair in enumerate((lows, highs)):
                    p = px * X2 + xhi * 2
                    dst[p, py * 8 : py * 8 + 8, :] = jnp.where(tile_row < R2, pair[0], pltpu.roll(pair[1], R2, 0))
                    dst[p + 1, py * 8 : py * 8 + 8, :] = jnp.where(
                        tile_row < R2, pltpu.roll(pair[0], R2, 0), pair[1]
                    )

    def whole_neighbours(grid, planes, x, last, mask):
        val = planes(x)
        zero = jnp.zeros_like(val)
        xm = planes(x - 1) if x > 0 else zero
        xp = planes(x + 1) if x < grid.planes - 1 else zero
        near = [
            xm,
            xp,
            pltpu.roll(val, 1, 0),
            pltpu.roll(val, grid.rows - 1, 0),
            pltpu.roll(val, 1, 1),
            pltpu.roll(val, grid.lanes - 1, 1),
        ]
        if mask:
            near[2] = jnp.where(grid.row == 0, 0.0, near[2])
            near[3] = jnp.where(grid.row == grid.rows - 1, 0.0, near[3])
            near[4] = jnp.where(grid.lane == 0, 0.0, near[4])
            near[5] = jnp.where(grid.lane >= last, 0.0, near[5])
        return val, near

    def whole_couplings(grid, inner, outer, last, c, d, b):
        for x in range(grid.planes):
            ci, ni = whole_neighbours(grid, lambda x: inner[x], x, last, True)
            co, no = whole_neighbours(grid, lambda x: outer[x], x, last, True)
            full = [jnp.minimum(ci, ni[k]) + 0.5 * (co + no[k]) for k in range(6)]
            diag = ((full[0] + full[1]) + (full[2] + full[3])) + (full[4] + full[5])
            if last < grid.lanes - 1:
                diag = jnp.where(grid.lane <= last, diag, 1.0)
            inv = 1.0 / diag
            edges = (
                None,
                None,
                grid.row == 0,
                grid.row == grid.rows - 1,
                grid.lane == 0,
                grid.lane >= last,
            )
            for k in range(6):
                f = full[k] * inv
                if edges[k] is not None:
                    f = jnp.where(edges[k], 0.0, f)
                if last < grid.lanes - 1:
                    f = jnp.where(grid.lane <= last, f, 0.0)
                c[k, x] = f
            if d is not None:
                d[x] = diag
            b[x] = inv

    def whole_update(grid, planes, c, b, x):
        val, near = whole_neighbours(grid, planes, x, None, False)
        a = b[x] + c[2, x] * near[2]
        e = c[3, x] * near[3] + c[4, x] * near[4]
        a = a + c[5, x] * near[5]
        if x > 0:
            a = a + c[0, x] * near[0]
        if x < grid.planes - 1:
            e = e + c[1, x] * near[1]
        return val, a + e

    def restrict2(plane, factor):
        pieces = [halve_rows(tmp, x, plane(2 * x) + plane(2 * x + 1)) for x in range(XH)]
        for x in range(XH):
            tall[x * RH : (x + 1) * RH, 0:ZG] = pieces[x]
        whole = dot(tall[0 : XH * RH, 0:ZG], narrow_low) * factor
        return [whole[x * RH : (x + 1) * RH] for x in range(XH)]

    def mix(x, a, b):
        return jnp.where(g0.colour(x, 0), a, pltpu.roll(b, 1, 1))

    across = jnp.zeros((R0, LANES), F32)
    face_lane = lax.broadcasted_iota(jnp.int32, (R0, LANES), 1)
    for x in range(X0):
        along_y = jnp.where(even_row, c0[2, x], c0[3, x])
        along_x = c0[x % 2, x]
        if x == 0 or x == X0 - 1:
            xs0[x // (X0 - 1), MIXED] = mix(x, c0[x % 2, x], along_y)
        val = mix(x, jnp.where(g0.row < R0 // 2, c0[2, x], c0[3, x]), along_x)
        ys0[0, MIXED, x : x + 1, :] = val[0:1]
        ys0[1, MIXED, x : x + 1, :] = val[R0 - 1 :]
        toward = jnp.where(iz == 0, c0[5, x, :, Z0 - LANES :], c0[4, x, :, 0:LANES])
        outs = [toward] + [
            jnp.where(iz == 0, f[:, Z0 - LANES :], f[:, 0:LANES]) for f in (along_x, along_y)
        ]
        for k, end in enumerate(outs):
            at = k * X0 + x
            across = jnp.where(face_lane == at, pltpu.roll(end, at + 1 - iz, 1), across)
    zs0[MIXED] = across
    def residual0(x):
        val, new = update(halo0, BLACK, lambda x: vb[x], c0, b0, x)
        mixed[x] = jnp.where(g0.colour(x, 0), new, mixed[x])
        return d0[x] * (new - val)

    for x, val in enumerate(restrict0(residual0, 0.5, 0, inner_first(4, X1))):
        ee[RHS1, GHOST + x, 0:R1, :] = val * b1[x]
    wide_publish(1)
    halo0.put(READY, mixed)
    send(5)
    gather_wait(gc, 0, True)
    unpack(lambda t: gc[t], in2)
    for x in range(XG):
        out2[x] = outer_of(in2[x])
    whole_couplings(g2, in2, out2, ZG - 1, c2, d2, b2)
    for x, val in enumerate(restrict2(lambda x: in2[x], 0.125)):
        v3[x] = val
    for x, val in enumerate(restrict2(lambda x: out2[x], 0.125)):
        v2a[x, 0:RH] = val
    whole_couplings(g3, v3, v2a.at[:, 0:RH], ZG // 2 - 1, c3, None, b3)

    XP = XH // 2
    own = (g3.even, g3.odd)

    def pack(colour, near, far):
        return jnp.where(own[colour], near, far)

    for colour in range(2):
        for p in range(XP):
            a, z = 2 * p, 2 * p + 1
            k3[colour * 6, p] = pack(colour, c3[1, a], c3[0, z])
            k3[colour * 6 + 1, p] = pack(colour, c3[0, a], c3[1, z])
            for k in range(2, 6):
                k3[colour * 6 + k, p] = pack(colour, c3[k, a], c3[k, z])
            if colour == 0:
                for k in range(6):
                    k3[12 + k, p] = pltpu.roll(k3[k, p], 1, 1)
                    k3[18 + k, p] = pltpu.roll(k3[k, p], ZG - 1, 1)

    wide_arrive(1)
    ring = GHOST - 1
    for p in range(ring - 1, XE - ring + 1):
        v1a[p] = jnp.where(g1.colour(p, 0), ee[RHS1, p], 0.0)
    z1a[...] = jnp.where(pack_own[0], zp1[RHS1], 0.0)
    half_pack(v1a, z1a, z1b, 1, ring, XE - ring)
    half1(v1a, z1a, v1b, 1, range(ring, XE - ring))

    def residual1(x):
        val, new = update1(v1b, z1b, GHOST + x)
        return d1[x] * (new - val)[0:R1]

    gr_own[...] = restrict1(residual1, 0.5)
    gather_send(gr_own, gr, 1)
    for p in (0, 1, XE - 2, XE - 1):
        v1a[p] = jnp.where(g1.colour(p, 0), ee[RHS1, p], 0.0)
    half_pack(v1a, z1a, z1b, 1, 0, XE)
    half1(v1a, z1a, v1b, 1, (1, 2, XE - 3, XE - 2))
    gather_wait(gr, 1, True)
    arrive(5)
    unpack(lambda t: gr[t], v2b)
    for x in range(XG):
        b2[x] = v2b[x] * b2[x]
        v2a[x] = jnp.where(g2.colour(x, 0), b2[x], 0.0)
    for x in range(XG):
        val, new = whole_update(g2, lambda x: v2a[x], c2, b2, x)
        v2b[x] = jnp.where(g2.colour(x, 1), new, val)

    def residual2(x):
        val, new = whole_update(g2, lambda x: v2b[x], c2, b2, x)
        return d2[x] * (new - val)

    for x, val in enumerate(restrict2(residual2, 0.5)):
        b3[x] = val * b3[x]

    for colour in range(2):
        for p in range(XP):
            h3[colour, p] = pack(colour, b3[2 * p], b3[2 * p + 1])
    none = jnp.zeros((RH, ZG), F32)

    at_shift = {0: 0, 1: 12, -1: 18}
    first_h = {s: [pltpu.roll(h3[0, p], s % ZG, 1) if s else h3[0, p] for p in range(XP)] for s in STEPS}

    def relaxed(colour, shift, shifted):
        fresh = []
        for p in range(XP):
            val, at = shifted[shift][p], colour * 6 + at_shift[shift]
            before = shifted[shift][p - 1] if p > 0 else none
            after = shifted[shift][p + 1] if p < XP - 1 else none
            i = (h3[1, p] if colour else first_h[shift][p]) + k3[at, p] * val
            mask = own[(colour + shift) % 2]
            j = k3[at + 1, p] * jnp.where(mask, before, after) + k3[at + 2, p] * pltpu.roll(val, 1, 0)
            l = k3[at + 3, p] * pltpu.roll(val, RH - 1, 0) + k3[at + 4, p] * shifted[shift + 1][p]
            fresh.append((i + k3[at + 5, p] * shifted[shift - 1][p]) + (j + l))
        return fresh

    def coarse(step, state):
        shifted = {0: state[XP:]}
        for s in (-2, -1, 1, 2):
            shifted[s] = [pltpu.roll(v, s % ZG, 1) for v in shifted[0]]
        red = {s: relaxed(0, s, shifted) for s in STEPS}
        return tuple(red[0] + relaxed(1, 0, red))

    start = relaxed(1, 0, first_h)
    state = lax.fori_loop(1, COARSE_SWEEPS, coarse, tuple(first_h[0] + start))
    solved = []
    for p in range(XP):
        solved.append(pack(0, state[p], state[XP + p]))
        solved.append(pack(1, state[p], state[XP + p]))
    for x in range(XH):
        tall[x * RH : (x + 1) * RH, 0:ZG] = solved[x]
    wide = dot(tall[0 : XH * RH, 0:ZG], double12)
    for x in range(XH):
        corr = double_rows(tmp, x, wide[x * RH : (x + 1) * RH])
        v2a[2 * x] = v2b[2 * x] + corr
        v2a[2 * x + 1] = v2b[2 * x + 1] + corr
    for colour, src, dst in ((0, v2a, v2b), (1, v2b, v2a)):
        for x in range(XG):
            val, new = whole_update(g2, lambda x: src[x], c2, b2, x)
            dst[x] = jnp.where(g2.colour(x, colour), new, val)

    row_shift = lax.rem(RG - iy * R2, RG)
    lane_shift = lax.rem(ZG - iz * half, ZG)
    edge2 = GHOST // 2
    rows2 = R2 + 2 * edge2
    planes2 = X2 + 2 * edge2
    for k in range(planes2):
        part = v2a[jnp.clip(ix * X2 + k - edge2, 0, XG - 1)]
        part = pltpu.roll(pltpu.roll(part, row_shift, 0), lane_shift, 1)
        tall[k * rows2 : (k + 1) * rows2, 0:ZG] = jnp.where(
            tile_row < R2 + edge2, part[0:rows2], part[RG - rows2 : RG]
        )
    source = lax.broadcasted_iota(jnp.int32, (ZG, LANES), 0)
    target = lax.broadcasted_iota(jnp.int32, (ZG, LANES), 1)
    target = lax.div(target, 2 * XE)
    pick = jnp.where(source == jnp.where(iz == 0, half + target, ZG - 1 - target), 1.0, 0.0).astype(F32)
    coarse_rows = tall[0 : planes2 * rows2, 0:ZG]
    wide = dot(coarse_rows, double12)
    sides = dot(coarse_rows, pick)
    acc = jnp.zeros((rows2, LANES), F32)
    tile_plane = lax.div(jnp.bitwise_and(tile_lane, XE - 1), 2)
    for k in range(planes2):
        acc = jnp.where(tile_plane == k, sides[k * rows2 : (k + 1) * rows2], acc)
    z1a[...] = z1b[...] + jnp.where(pack_inside, double_rows(tmp, 0, acc), 0.0)
    for k in range(planes2):
        corr = double_rows(tmp, k, wide[k * rows2 : (k + 1) * rows2])
        for p in (2 * k, 2 * k + 1):
            if 0 < p < XE - 1:
                v1a[p] = v1b[p] + jnp.where(inside1(p), corr, 0.0)
    half_pack(v1a, z1a, z1b, 0, 1, XE - 1)
    half1(v1a, z1a, v1b, 0, range(2, XE - 2))
    half_pack(v1b, z1b, z1a, 1, 2, XE - 2)
    half1(v1b, z1b, v1a, 1, range(3, XE - 3))

    def enlarge(count, read, write):
        for x in range(count):
            tall[x * R1 : (x + 1) * R1, 0:Z1] = read(x)
        wide = dot(tall[0 : count * R1, 0:Z1], double01)
        for x in range(count):
            write(x, double_rows(tmp, x, wide[x * R1 : (x + 1) * R1]))

    def inside(x, corr):
        va[2 * x] = vb[2 * x] + corr
        va[2 * x + 1] = vb[2 * x + 1] + corr

    enlarge(X1, lambda x: v1a[GHOST + x, 0:R1, :], inside)
    diagonal = tile_lane == tile_row + GHOST
    stack, lined_stack = [], []
    own_pack = jnp.zeros((RE, LANES), F32)
    for p in range(GHOST, XE - GHOST):
        own_pack = jnp.where(pack_lane == p, pltpu.roll(v1a[p], p + 1 - iz, 1), own_pack)
    for k in range(2):
        p, own = (GHOST - 1, GHOST) if k == 0 else (X1 + GHOST, X1 + GHOST - 1)
        val, near = near1(lambda p: v1a[p], lambda p: z1a[:, p : p + 1], p, edge=True)
        stack += [val[0:R1]] + [(other - val)[0:R1] for other in (v1a[own], near[2], near[3])]
        lined_stack.append(((near[4] - val)[0:R1], (near[5] - val)[0:R1]))
    for k in range(2):
        row, own = (RE - 1, 0) if k == 0 else (R1, R1 - 1)
        for p in range(GHOST - 1, X1 + GHOST + 1):
            yrim[k, p : p + 1, :] = v1a[p, row : row + 1, :]
            if GHOST <= p < X1 + GHOST:
                yrim[2 + k, p : p + 1, :] = v1a[p, own : own + 1, :]
        val = yrim[k, GHOST : X1 + GHOST, :]
        others = [
            yrim[2 + k, GHOST : X1 + GHOST, :],
            yrim[k, GHOST - 1 : X1 + GHOST - 1, :],
            yrim[k, GHOST + 1 : X1 + GHOST + 1, :],
        ]
        stack += [val] + [other - val for other in others]
        line = jnp.where(diagonal, jnp.broadcast_to(z1a[row : row + 1, :], (8, LANES)), 0.0)
        column = jnp.broadcast_to(jnp.sum(line, axis=1, keepdims=True), (8, LANES))
        back = jnp.where(tile_lane == 0, jnp.where(iz == 0, 0.0, column), pltpu.roll(val, 1, 1))
        ahead = jnp.where(tile_lane == Z1 - 1, jnp.where(iz == 0, column, 0.0), pltpu.roll(val, Z1 - 1, 1))
        lined_stack.append((back - val, ahead - val))
    val = z1a[...]
    shifts = [pltpu.roll(val, 1, 0), pltpu.roll(val, RE - 1, 0), pltpu.roll(val, 1, 1), pltpu.roll(val, LANES - 1, 1)]
    face = [val, own_pack - val] + [other - val for other in shifts]
    face = [pltpu.roll(f[0:R1], LANES - GHOST, 1) for f in face]
    stack += face[:4]
    lined_stack.append((face[4], face[5]))
    for i, piece in enumerate(stack):
        tall[i * R1 : (i + 1) * R1, 0:Z1] = piece
    for i, (back, ahead) in enumerate(lined_stack):
        tall2[i * R1 : (i + 1) * R1, 0:Z1] = back
        tall2[i * R1 : (i + 1) * R1, Z1 : 2 * Z1] = ahead
    k = lax.broadcasted_iota(jnp.int32, (2 * Z1, Z0), 0)
    j = lax.broadcasted_iota(jnp.int32, (2 * Z1, Z0), 1)
    source = lax.shift_right_logical(j, 1) + Z1 * jnp.bitwise_and(j, 1)
    big = dot(tall[0 : len(stack) * R1, 0:Z1], double01)
    lined_big = dot(tall2[0 : len(lined_stack) * R1, :], jnp.where(k == source, 1.0, 0.0).astype(F32))

    def woven(slot, first, second):
        parts = []
        for k in range(Z0 // LANES):
            at = 2 * slot + k
            tmp[at, pl.ds(0, R1, 2), :] = first[:, k * LANES : (k + 1) * LANES]
            tmp[at, pl.ds(1, R1, 2), :] = second[:, k * LANES : (k + 1) * LANES]
            parts.append(tmp[at, 0:R0, :])
        return jnp.concatenate(parts, axis=1)

    def finished(k):
        piece = [big[(4 * k + i) * R1 : (4 * k + i + 1) * R1] for i in range(4)]
        lines = lined_big[k * R1 : (k + 1) * R1]
        at = 4 * (k % 2)
        return (
            woven(at, piece[0], piece[0]),
            woven(at + 1, piece[1], piece[1]),
            woven(at + 2, piece[2], piece[3]),
            woven(at + 3, lines, lines),
        )

    for k in range(4):
        ref, side = (xh0, k) if k < 2 else (yh0, k - 2)
        corr, toward, beside, lengthwise = finished(k)
        ref[side, FIXED] = ref[side, BLACK] + corr
        first, second = ref[side, MIXED], ref[side, READY]
        ref[side, LAST] = ((second + corr) + first * toward) + (
            pltpu.roll(first, Z0 - 1, 1) * beside + pltpu.roll(second, Z0 - 1, 1) * lengthwise
        )
    corr, toward, beside, sideways = [f[:, 0:LANES] for f in finished(4)]
    zh0[FIXED] = zh0[BLACK] + corr
    first = zh0[MIXED]
    zh0[LAST] = ((zh0[READY] + corr) + first * toward) + (
        pltpu.roll(first, LANES - X0, 1) * sideways + pltpu.roll(first, LANES - 2 * X0, 1) * beside
    )
    half_sweep(None, halo0, FIXED, va, vb, c0, b0, 0)
    half_sweep(None, halo0, LAST, vb, ext_out, c0, b0, 1)

    for number in range(len(EXCHANGES)):
        sent(number)
    for number in range(len(WIDE)):
        wide_sent(number)
    gather_wait(gc, 0, False)
    gather_wait(gr, 1, False)


def finish(*refs):
    count = (len(refs) - 1) // 2
    sem = refs[-1]
    copies = [pltpu.make_async_copy(refs[i], refs[count + i], sem.at[i]) for i in range(count)]
    for copy in copies:
        copy.start()
    for copy in copies:
        copy.wait()


def solution(mesh):
    nx, ny, nz = (mesh.shape[a] for a in ("gx", "gy", "gz"))
    spec = P("gx", "gy", "gz")

    def on_device(membrane, recovery, extracellular, fiber_scale, labels):
        X, R, Z = membrane.shape
        X1, R1, Z1 = X // 2, R // 2, Z // 2
        XG, RG, ZG = nx * X // 4, ny * R // 4, nz * Z // 4
        assert nz == 2 and ny % 2 == 0 and ZG == LANES and Z1 == LANES
        assert R1 == 8 and X1 == 8 and X % 8 == 0
        total = nx * ny * nz
        assert labels.shape == (2, 2, LANES // 4)
        f0 = 11
        field = (X, R, Z)
        lvl1 = (X1, R1, Z1)
        whole = (XG, RG, ZG)
        third = (XG // 2, RG // 2, ZG)

        def v(*shape):
            return pltpu.VMEM(shape, F32)

        def faces(f, x, r, z):
            return [v(2, f, r, z), v(2, f, x, z), v(f, r, LANES)] * 2

        anywhere = pl.BlockSpec(memory_space=pl.ANY)
        scratch = [v(*field)] * 4 + [pltpu.VMEM(labels.shape, jnp.int32), pltpu.SemaphoreType.DMA((5,))]
        scratch += faces(f0, *field)
        scratch += [v(*field), v(*field), v(*field), v(6, *field), v(6, *field), v(*field), v(*field)]
        scratch += [v(*field), v(*field)]
        scratch += [
            v(2 * max(X1, XG // 2), max(R, RG), LANES),
            v(max(X1 * R1, (XG // 2) * (RG // 2), 2 * X1 * R1, 20 * R1, total), Z),
        ]
        XE, RE = X1 + 2 * GHOST, R1 + 2 * GHOST
        assert GHOST * XE <= LANES and 2 * GHOST == R1 and GHOST <= X1
        wide, pack = (XE, RE, Z1), (RE, LANES)
        scratch += [v(3, *wide), v(2, 3, X1 // 2, R1, Z1), v(2, 3, XE // 2, R1, Z1), v(3, R1, LANES)]
        scratch += [v(9, 3, R1, LANES), v(3, *pack), v(6, *wide), v(6, *pack), v(*lvl1), v(*lvl1)]
        scratch += [v(*wide), v(*wide), v(*pack), v(*pack), v(4, XE, Z1)]
        scratch += [v(*field), v(8 * R1, Z)]
        scratch += [v(8, LANES), v(total, 8, LANES), v(8, LANES), v(total, 8, LANES)]
        scratch += [v(*whole), v(*whole), v(6, *whole), v(*whole), v(*whole), v(*whole), v(*whole)]
        scratch += [v(6, *third), v(*third), v(*third)]
        packed = (XG // 4, RG // 2, ZG)
        scratch += [v(24, *packed), v(2, *packed)]
        sems = SIDES * len(EXCHANGES)
        scratch += [pltpu.SemaphoreType.DMA((sems,))] * 2
        scratch += [pltpu.SemaphoreType.DMA((WIDE_SIDES * len(WIDE),))] * 2
        scratch += [pltpu.SemaphoreType.DMA((2,))] * 2
        vmem = pl.BlockSpec(memory_space=pltpu.VMEM)
        room = 54400 << 10
        shape = jax.ShapeDtypeStruct(field, F32)
        results = pl.pallas_call(
            functools.partial(kernel, (nx, ny, nz)),
            out_shape=[shape] * 3,
            in_specs=[anywhere] * 5,
            out_specs=[vmem] * 3,
            scratch_shapes=scratch,
            compiler_params=pltpu.CompilerParams(
                collective_id=0, has_side_effects=True, vmem_limit_bytes=room
            ),
        )(membrane, recovery, extracellular, fiber_scale, labels)
        return tuple(
            pl.pallas_call(
                finish,
                out_shape=[shape] * 3,
                in_specs=[vmem] * 3,
                out_specs=[anywhere] * 3,
                scratch_shapes=[pltpu.SemaphoreType.DMA((3,))],
                compiler_params=pltpu.CompilerParams(vmem_limit_bytes=4 << 20),
            )(*results)
        )

    return jax.shard_map(
        on_device,
        mesh=mesh,
        in_specs=(spec,) * 5,
        out_specs=(spec,) * 3,
        check_vma=False,
    )
```

```python
import functools

import jax
import jax.numpy as jnp
from jax import lax
from jax.experimental import pallas as pl
from jax.experimental.pallas import tpu as pltpu
from jax.sharding import PartitionSpec as P

COARSE_SWEEPS = 8
TIME_STEP = 0.05
ionic_gain = 8.0
ionic_onset = 0.15
recovery_rate = 0.01
MESH = pl.DeviceIdType.MESH
LOGICAL = pl.DeviceIdType.LOGICAL
LANES = 128
F32 = jnp.float32

INNER, U, OUTER, V, NEXT, RED, BLACK, MIXED, READY, FIXED, LAST = range(11)
INNER1, OUTER1, RHS1 = range(3)
GHOST = 4
EXCHANGES = (
    (INNER, 2),
    (V, 1),
    (NEXT, 1),
    (RED, 1),
    (BLACK, 1),
    (MIXED, 2),
)
SIDES = 5
WIDE = ((INNER1, 1), (RHS1, 1))
STEPS = (-1, 0, 1)
WIDE_SIDES = 17


def dot(a, b):
    high = a.astype(jnp.bfloat16)
    rest = a - high.astype(F32)
    middle = rest.astype(jnp.bfloat16)
    low = (rest - middle.astype(F32)).astype(jnp.bfloat16)
    chosen = b.astype(jnp.bfloat16)
    rows = a.shape[0]
    both = jnp.dot(jnp.concatenate([low, middle, high], axis=0), chosen, preferred_element_type=F32)
    parts = [both[i * rows : (i + 1) * rows] for i in range(3)]
    return (parts[0] + parts[1]) + parts[2]


def pair_matrix(rows, cols, offset):
    j = lax.broadcasted_iota(jnp.int32, (rows, cols), 0)
    k = lax.broadcasted_iota(jnp.int32, (rows, cols), 1)
    return jnp.where(lax.shift_right_logical(j, 1) + offset == k, 1.0, 0.0).astype(F32)


def copy_matrix(rows, cols, shift):
    k = lax.broadcasted_iota(jnp.int32, (rows, cols), 0)
    j = lax.broadcasted_iota(jnp.int32, (rows, cols), 1)
    return jnp.where(lax.shift_right_logical(j, shift) == k, 1.0, 0.0).astype(F32)


class Grid:
    def __init__(self, planes, rows, lanes):
        self.planes, self.rows, self.lanes = planes, rows, lanes
        self.row = lax.broadcasted_iota(jnp.int32, (rows, lanes), 0)
        self.lane = lax.broadcasted_iota(jnp.int32, (rows, lanes), 1)
        self.even = jnp.bitwise_and(self.row + self.lane, 1) == 0
        self.odd = jnp.bitwise_and(self.row + self.lane, 1) == 1

    def colour(self, x, colour):
        return self.even if (x + colour) % 2 == 0 else self.odd


class Halo:
    def __init__(self, grid, refs, iz):
        self.grid, self.iz = grid, iz
        self.xs, self.ys, self.zs, self.xh, self.yh, self.zh = refs
        self.flane = lax.broadcasted_iota(jnp.int32, (grid.rows, LANES), 1)

    def faces(self, slot, planes):
        g = self.grid
        acc = jnp.zeros((g.rows, LANES), F32)
        for x, val in planes:
            self.ys[0, slot, x : x + 1, :] = val[0:1]
            self.ys[1, slot, x : x + 1, :] = val[g.rows - 1 :]
            if g.lanes > LANES:
                end = jnp.where(self.iz == 0, val[:, g.lanes - LANES :], val[:, :LANES])
            else:
                end = val
            acc = jnp.where(self.flane == x, pltpu.roll(end, x + 1 - self.iz, 1), acc)
            yield
        self.zs[slot] = acc

    def put_ends(self, slot, ref):
        self.xs[0, slot] = ref[0]
        self.xs[1, slot] = ref[self.grid.planes - 1]

    def put_rest(self, slot, ref):
        for _ in self.faces(slot, [(x, ref[x]) for x in range(self.grid.planes)]):
            pass

    def put(self, slot, ref):
        self.put_ends(slot, ref)
        self.put_rest(slot, ref)

    def neighbours(self, slot, planes, x, edge=False):
        g = self.grid
        val = planes(x)
        xm = planes(x - 1) if x > 0 else self.xh[0, slot]
        xp = planes(x + 1) if x < g.planes - 1 else self.xh[1, slot]
        shape = (g.rows, g.lanes)
        low = jnp.broadcast_to(self.yh[0, slot, x : x + 1, :], shape)
        high = jnp.broadcast_to(self.yh[1, slot, x : x + 1, :], shape)
        ym = jnp.where(g.row == 0, low, pltpu.roll(val, 1, 0))
        yp = jnp.where(g.row == g.rows - 1, high, pltpu.roll(val, g.rows - 1, 0))
        side = jnp.broadcast_to(self.zh[slot, :, x : x + 1], shape)
        side_m, side_p = side, side
        if edge:
            side_m = jnp.where(self.iz == 0, 0.0, side)
            side_p = jnp.where(self.iz == 0, side, 0.0)
        zm = jnp.where(g.lane == 0, side_m, pltpu.roll(val, 1, 1))
        zp = jnp.where(g.lane == g.lanes - 1, side_p, pltpu.roll(val, g.lanes - 1, 1))
        return val, (xm, xp, ym, yp, zm, zp)


def halve_rows(tmp, slot, val):
    rows, lanes = val.shape
    parts = []
    for k in range(lanes // LANES):
        at = 2 * slot + k
        tmp[at, 0:rows, :] = val[:, k * LANES : (k + 1) * LANES]
        parts.append(tmp[at, pl.ds(0, rows // 2, 2), :] + tmp[at, pl.ds(1, rows // 2, 2), :])
    return parts[0] if len(parts) == 1 else jnp.concatenate(parts, axis=1)


def double_rows(tmp, slot, val):
    rows, lanes = val.shape
    parts = []
    for k in range(lanes // LANES):
        at = 2 * slot + k
        piece = val[:, k * LANES : (k + 1) * LANES]
        tmp[at, pl.ds(0, rows, 2), :] = piece
        tmp[at, pl.ds(1, rows, 2), :] = piece
        parts.append(tmp[at, 0 : 2 * rows, :])
    return parts[0] if len(parts) == 1 else jnp.concatenate(parts, axis=1)


def kernel(counts, *refs):
    sources, (mem_out, rec_out, ext_out) = refs[:5], refs[5:8]
    refs = refs[8:]
    mem, rec, ext, fib, lab, in_sem = refs[:6]
    refs = (None,) + refs
    (xs0, ys0, zs0, xh0, yh0, zh0) = refs[7:13]
    (in0, out0, uu, w0, c0, d0, b0, va, vb, tmp, tall) = refs[13:24]
    (ee, ys1, yr1, zs1, zr1, zp1, c1, cz1, d1, b1, v1a, v1b, z1a, z1b, yrim, mixed, tall2) = refs[24:41]
    (gc_own, gc, gr_own, gr, in2, out2, c2, d2, b2, v2a, v2b) = refs[41:52]
    (c3, b3, v3, k3, h3, send_sem, recv_sem, wide_send, wide_recv, gs_sem, gr_sem) = refs[52:]
    nx, ny, nz = counts
    ix, iy, iz = lax.axis_index("gx"), lax.axis_index("gy"), lax.axis_index("gz")
    me = (ix * ny + iy) * nz + iz
    total = nx * ny * nz

    loads = [
        pltpu.make_async_copy(src, dst, in_sem.at[i])
        for i, (src, dst) in enumerate(zip(sources, (mem, rec, ext, fib, lab)))
    ]
    for i in (4, 3, 0, 2, 1):
        loads[i].start()

    barrier = pltpu.get_barrier_semaphore()

    def others(body):
        for i in sorted(range(1, total), key=lambda i: (abs(i // nz % ny * 2 - ny), i)):
            dev = me + i
            body(jnp.where(dev >= total, dev - total, dev))

    close = nx <= 4 and ny <= 4
    if close:
        greeted = -1
        for dx in (-1, 0, 1):
            for dy in (-1, 0, 1):
                present = (ix + dx >= 0) & (ix + dx < nx) & (iy + dy >= 0) & (iy + dy < ny)
                greeted = greeted + jnp.where(present, nz, 0)
                for z in (iz, 1 - iz):
                    if dx == 0 and dy == 0 and z is iz:
                        continue

                    def hail(where=(ix + dx, iy + dy, z)):
                        pl.semaphore_signal(barrier, inc=1, device_id=where, device_id_type=MESH)

                    pl.when(present)(hail)
    else:
        greeted = total - 1
        others(lambda dev: pl.semaphore_signal(barrier, inc=1, device_id=dev, device_id_type=LOGICAL))

    def clear(missing, ref, side):
        def fill():
            ref[side] = jnp.zeros(ref.at[side].shape, F32)

        pl.when(missing)(fill)

    X1, R1, Z1 = mem.shape[0] // 2, mem.shape[1] // 2, mem.shape[2] // 2
    XE, RE = X1 + 2 * GHOST, R1 + 2 * GHOST
    clear(ix == 0, xh0, 0)
    clear(ix == nx - 1, xh0, 1)
    clear(iy == 0, yh0, 0)
    clear(iy == ny - 1, yh0, 1)
    for slot in range(3):
        for p in range(GHOST):
            clear(ix == 0, ee, (slot, p))
            clear(ix == nx - 1, ee, (slot, XE - 1 - p))
    for load in loads:
        load.wait()

    g0 = Grid(*mem.shape)
    g1 = Grid(XE, RE, Z1)
    halo0 = Halo(g0, (xs0, ys0, zs0, xh0, yh0, zh0), iz)

    def copies(number):
        first, slots = EXCHANGES[number]
        h = halo0
        part = pl.ds(first, slots)
        plan = (
            (h.xs.at[0, part], h.xh.at[1, part], (ix - 1, iy, iz), ix > 0, ix < nx - 1),
            (h.xs.at[1, part], h.xh.at[0, part], (ix + 1, iy, iz), ix < nx - 1, ix > 0),
            (h.ys.at[0, part], h.yh.at[1, part], (ix, iy - 1, iz), iy > 0, iy < ny - 1),
            (h.ys.at[1, part], h.yh.at[0, part], (ix, iy + 1, iz), iy < ny - 1, iy > 0),
            (h.zs.at[part], h.zh.at[part], (ix, iy, 1 - iz), None, None),
        )
        for side, (src, dst, dev, goes, comes) in enumerate(plan):
            copy = pltpu.make_async_remote_copy(
                src_ref=src,
                dst_ref=dst,
                send_sem=send_sem.at[number * SIDES + side],
                recv_sem=recv_sem.at[number * SIDES + side],
                device_id=dev,
                device_id_type=MESH,
            )
            yield copy, goes, comes

    ends, rest = slice(0, 2), slice(2, SIDES)

    def send(number, sides=slice(0, SIDES)):
        for copy, goes, _ in list(copies(number))[sides]:
            if goes is None:
                copy.start()
            else:
                pl.when(goes)(copy.start)

    def arrive(number, sides=slice(0, SIDES)):
        for copy, _, comes in list(copies(number))[sides]:
            if comes is None:
                copy.wait_recv()
            else:
                pl.when(comes)(copy.wait_recv)

    def inner_first(number, count):
        arrive(number, rest)
        yield from range(1, count - 1)
        arrive(number, ends)
        yield 0
        yield count - 1

    def publish(number, halo, slot, ref):
        halo.put_ends(slot, ref)
        send(number, ends)
        halo.put_rest(slot, ref)
        send(number, rest)

    def sent(number):
        for copy, goes, _ in copies(number):
            if goes is None:
                copy.wait_send()
            else:
                pl.when(goes)(copy.wait_send)

    here = {-1: ix > 0, 0: None, 1: ix < nx - 1}
    along = {-1: iy > 0, 0: None, 1: iy < ny - 1}

    def both(a, b):
        if a is None or b is None:
            return b if a is None else a
        return jnp.logical_and(a, b)

    def wide_copies(number):
        first, count = WIDE[number]
        part = pl.ds(first, count)
        pairs, edge = X1 // 2, GHOST // 2
        plan = []
        for sx in (-1, 1):
            src = ee.at[part, pl.ds(GHOST if sx < 0 else X1, GHOST), pl.ds(0, R1)]
            dst = ee.at[part, pl.ds(X1 + GHOST if sx < 0 else 0, GHOST), pl.ds(0, R1)]
            plan.append((src, dst, sx, 0, iz))
        for sx in STEPS:
            for sy in (-1, 1):
                mine, theirs = (0, 1) if sy < 0 else (1, 0)
                at = {-1: (0, edge, pairs + edge), 0: (0, pairs, edge), 1: (pairs - edge, edge, 0)}[sx]
                src = ys1.at[mine, part, pl.ds(at[0], at[1])]
                dst = yr1.at[theirs, part, pl.ds(at[2], at[1])]
                plan.append((src, dst, sx, sy, iz))
        for sx in STEPS:
            for sy in STEPS:
                plan.append((zs1.at[part], zr1.at[(1 - sx) * 3 + 1 - sy, part], sx, sy, 1 - iz))
        for side, (src, dst, sx, sy, z) in enumerate(plan):
            copy = pltpu.make_async_remote_copy(
                src_ref=src,
                dst_ref=dst,
                send_sem=wide_send.at[number * WIDE_SIDES + side],
                recv_sem=wide_recv.at[number * WIDE_SIDES + side],
                device_id=(ix + sx, iy + sy, z),
                device_id_type=MESH,
            )
            yield copy, both(here[sx], along[sy]), both(here[-sx], along[-sy])

    def maybe(condition, action):
        if condition is None:
            action()
        else:
            pl.when(condition)(action)

    tile_row = lax.broadcasted_iota(jnp.int32, (8, LANES), 0)
    tile_lane = lax.broadcasted_iota(jnp.int32, (8, LANES), 1)

    def wide_publish(number):
        first, count = WIDE[number]
        plan = list(wide_copies(number))

        def start(group):
            for copy, goes, _ in group:
                maybe(goes, copy.start)

        start(plan[:2])
        for slot in range(first, first + count):
            for k in range(X1 // 2):
                even, odd = ee[slot, GHOST + 2 * k, 0:R1, :], ee[slot, GHOST + 2 * k + 1, 0:R1, :]
                ys1[0, slot, k] = jnp.where(tile_row < GHOST, even, pltpu.roll(odd, GHOST, 0))
                ys1[1, slot, k] = jnp.where(tile_row < GHOST, pltpu.roll(odd, GHOST, 0), even)
        start(plan[2:8])
        for slot in range(first, first + count):
            acc = jnp.zeros((R1, LANES), F32)
            for x in range(X1):
                val = ee[slot, GHOST + x, 0:R1, :]
                for depth in range(GHOST):
                    at = depth * XE + GHOST + x
                    shift = jnp.where(iz == 0, at + 1 + depth, at - depth)
                    acc = jnp.where(tile_lane == at, pltpu.roll(val, shift, 1), acc)
            zs1[slot] = acc
        start(plan[8:])

    def keep(condition, val):
        return val if condition is None else jnp.where(condition, val, 0.0)

    def plane_side(p):
        return here[-1 if p < GHOST else (1 if p >= X1 + GHOST else 0)]

    def wide_arrive(number):
        first, count = WIDE[number]
        for copy, _, comes in wide_copies(number):
            maybe(comes, copy.wait_recv)
        low = tile_row >= GHOST
        pe = jnp.bitwise_and(tile_lane, XE - 1)
        for slot in range(first, first + count):
            for p in range(XE):
                after, before = yr1[1, slot, p // 2], yr1[0, slot, p // 2]
                if p % 2:
                    after, before = pltpu.roll(after, GHOST, 0), pltpu.roll(before, GHOST, 0)
                side = plane_side(p)
                after = keep(both(side, along[1]), after)
                before = keep(both(side, along[-1]), before)
                ee[slot, p, R1:RE, :] = jnp.where(low, before, after)
            rows = []
            for sy in STEPS:
                mid = zr1[3 + sy + 1, slot]
                left = keep(here[-1], pltpu.roll(zr1[sy + 1, slot], LANES - X1, 1))
                right = keep(here[1], pltpu.roll(zr1[6 + sy + 1, slot], X1, 1))
                val = jnp.where(pe < GHOST, left, jnp.where(pe >= X1 + GHOST, right, mid))
                rows.append(keep(along[sy], jnp.where(tile_lane < GHOST * XE, val, 0.0)))
            zp1[slot, 0:R1, :] = rows[1]
            zp1[slot, R1:RE, :] = jnp.where(low, rows[0], rows[2])

    def wide_sent(number):
        for copy, goes, _ in wide_copies(number):
            maybe(goes, copy.wait_send)

    def gather_send(own, whole, which):
        def go(dev):
            pltpu.make_async_remote_copy(
                src_ref=own,
                dst_ref=whole.at[me],
                send_sem=gs_sem.at[which],
                recv_sem=gr_sem.at[which],
                device_id=dev,
                device_id_type=LOGICAL,
            ).start()

        others(go)
        whole[pl.ds(me, 1)] = own[...][None]

    def gather_wait(whole, which, recv):
        rest = whole.at[pl.ds(0, total - 1)]
        copy = pltpu.make_async_remote_copy(
            src_ref=rest,
            dst_ref=rest,
            send_sem=gs_sem.at[which],
            recv_sem=gr_sem.at[which],
            device_id=(ix, iy, 1 - iz),
            device_id_type=MESH,
        )
        if recv:
            copy.wait_recv()
        else:
            copy.wait_send()

    X0, R0, Z0 = mem.shape
    X2 = X1 // 2
    R2 = R1 // 2
    half = Z1 // 2

    widen8 = copy_matrix(lab.shape[2], Z0, 3)
    lab_planes = []
    for bx in range(lab.shape[0]):
        wide = jnp.dot(lab[bx].astype(F32), widen8, preferred_element_type=F32)
        lab_planes.append(
            jnp.concatenate(
                [jnp.broadcast_to(wide[by : by + 1], (8, Z0)) for by in range(lab.shape[1])], axis=0
            )
        )

    def label_of(x):
        return lab_planes[x // 8]

    for x in range(X0):
        label = label_of(x)
        in0[x] = jnp.where(label == 1.0, 1.0, jnp.where(label == 2.0, 0.3, 0.0)) * fib[x]
        out0[x] = jnp.where(label == 0.0, 3.0, 1.0)
        uu[x] = mem[x] + ext[x]
    halo0.put_ends(INNER, in0)
    halo0.put_ends(U, uu)
    pl.semaphore_wait(barrier, greeted)
    send(0, ends)
    halo0.put_rest(INNER, in0)
    halo0.put_rest(U, uu)
    send(0, rest)
    halo0.put(V, ext)
    send(1)

    narrow = pair_matrix(Z0, Z1, 0)
    narrow_low = pair_matrix(Z1, Z1, 0)
    narrow_high = pair_matrix(Z1, Z1, half)
    double01 = copy_matrix(Z1, Z0, 1)
    double12 = copy_matrix(Z1, Z1, 1)

    def restrict0(plane, factor, base, order=None):
        for x in order or range(X1):
            tall[base + x * R1 : base + (x + 1) * R1, :] = halve_rows(tmp, x, plane(2 * x) + plane(2 * x + 1))
        whole = dot(tall[base : base + X1 * R1, :], narrow) * factor
        return [whole[x * R1 : (x + 1) * R1] for x in range(X1)]

    def restrict1(plane, factor, order=None):
        rows = [None] * X2
        for x in order or range(X2):
            rows[x] = halve_rows(tmp, x, plane(2 * x) + plane(2 * x + 1))
        low = jnp.concatenate(rows[: X2 // 2], axis=0)
        high = jnp.concatenate(rows[X2 // 2 :], axis=0)
        return (dot(low, narrow_low) + dot(high, narrow_high)) * factor

    for x in inner_first(0, X0):
        centre, near = halo0.neighbours(INNER, lambda x: in0[x], x, edge=True)
        u, near_u = halo0.neighbours(U, lambda x: uu[x], x)
        drive = jnp.zeros_like(u)
        for d in range(6):
            weight = jnp.minimum(centre, near[d])
            w0[d, x] = weight
            drive = drive + weight * (near_u[d] - u)
        m, r = mem[x], rec[x]
        tissue = jnp.where(label_of(x) != 0.0, 1.0, 0.0)
        ionic = ionic_gain * m * (m - ionic_onset) * (m - 1.0) + m * r
        mem_out[x] = m + TIME_STEP * (drive - tissue * ionic)
    publish(2, halo0, NEXT, mem_out)
    for x in range(X0):
        m, r = mem[x], rec[x]
        rec_out[x] = r + TIME_STEP * recovery_rate * (-r - ionic_gain * m * (m - ionic_onset - 1.0))

    for x, val in enumerate(restrict0(lambda x: in0[x], 0.125, 0)):
        ee[INNER1, GHOST + x, 0:R1, :] = val
    wide_publish(0)
    gc_own[...] = restrict1(lambda x: ee[INNER1, GHOST + x, 0:R1, :], 0.125)

    def scaled(grid, weights, centre, near, iz_edges):
        full = [weights[d] + 0.5 * (centre + near[d]) for d in range(6)]
        diag = ((full[0] + full[1]) + (full[2] + full[3])) + (full[4] + full[5])
        inv = 1.0 / diag
        full = [f * inv for f in full]
        low, high = iz_edges
        along_z = jnp.where(even_lane, full[4], full[5])
        full[4] = jnp.where(low, 0.0, full[4])
        full[5] = jnp.where(high, 0.0, full[5])
        return full, diag, inv, along_z

    even_lane = jnp.bitwise_and(g0.lane, 1) == 0
    even_row = jnp.bitwise_and(g0.row, 1) == 0
    first0 = (g0.lane == 0) & (iz == 0)
    last0 = (g0.lane == Z0 - 1) & (iz == nz - 1)
    for side in range(2):
        for ref, has in ((xh0, here), (yh0, along)):
            val = jnp.where(ref[side, INNER] == 0.0, 3.0, 1.0)
            ref[side, OUTER] = jnp.where(has[2 * side - 1], val, 0.0)
    zh0[OUTER] = jnp.where(zh0[INNER] == 0.0, 3.0, 1.0)
    inv0 = vb
    for x in range(X0):
        centre, near = halo0.neighbours(OUTER, lambda x: out0[x], x, edge=True)
        full, diag, inv, along_z = scaled(g0, [w0[d, x] for d in range(6)], centre, near, (first0, last0))
        for d in range(6):
            c0[d, x] = full[d]
        d0[x] = diag
        b0[x] = inv
        mixed[x] = pltpu.roll(along_z, 1, 1)

    def update(halo, slot, planes, c, b, x):
        val, near = halo.neighbours(slot, planes, x)
        a = b[x] + c[0, x] * near[0]
        e = c[1, x] * near[1] + c[2, x] * near[2]
        f = c[3, x] * near[3] + c[4, x] * near[4]
        return val, (a + c[5, x] * near[5]) + (e + f)

    def half_sweep(number, halo, slot, src, dst, c, b, colour):
        planes = halo.grid.planes
        for x in range(planes) if number is None else inner_first(number, planes):
            val, new = update(halo, slot, lambda x: src[x], c, b, x)
            dst[x] = jnp.where(halo.grid.colour(x, colour), new, val)

    arrive(1)
    for x in inner_first(2, X0):
        m, near = halo0.neighbours(NEXT, lambda x: mem_out[x], x)
        rhs = jnp.zeros_like(m)
        for d in range(6):
            rhs = rhs + w0[d, x] * (near[d] - m)
        b0[x] = rhs * b0[x]
        val, new = update(halo0, V, lambda x: ext[x], c0, b0, x)
        va[x] = jnp.where(g0.colour(x, 0), new, val)
    publish(3, halo0, RED, va)

    first1 = (g1.lane == 0) & (iz == 0)
    last1 = (g1.lane == Z1 - 1) & (iz == nz - 1)
    pack_row = lax.broadcasted_iota(jnp.int32, (RE, LANES), 0)
    pack_lane = lax.broadcasted_iota(jnp.int32, (RE, LANES), 1)
    pack_x = jnp.bitwise_and(pack_lane, XE - 1)
    depth_parity = lax.div(pack_lane, XE) + iz + pack_x + pack_row
    pack_own = [jnp.bitwise_and(depth_parity + colour, 1) == 0 for colour in range(2)]

    def row_inside(row):
        return (
            (row < R1)
            | ((row < R1 + GHOST) & (iy < ny - 1))
            | ((row >= R1 + GHOST) & (iy > 0))
        )

    inside_row = row_inside(g1.row)
    pack_inside = (
        row_inside(pack_row)
        & (pack_lane < GHOST * XE)
        & ((pack_x >= GHOST) | (ix > 0))
        & ((pack_x < X1 + GHOST) | (ix < nx - 1))
    )

    def inside1(p):
        side = plane_side(p)
        return inside_row if side is None else inside_row & side

    def near1(planes, pack, p, edge=False):
        val = planes(p)
        side = jnp.broadcast_to(pack(p), (RE, Z1))
        side_m, side_p = side, side
        if edge:
            side_m = jnp.where(iz == 0, 0.0, side)
            side_p = jnp.where(iz == 0, side, 0.0)
        return val, (
            planes(p - 1),
            planes(p + 1),
            pltpu.roll(val, 1, 0),
            pltpu.roll(val, RE - 1, 0),
            jnp.where(g1.lane == 0, side_m, pltpu.roll(val, 1, 1)),
            jnp.where(g1.lane == Z1 - 1, side_p, pltpu.roll(val, Z1 - 1, 1)),
        )

    def near_pack(planes, val, first, last):
        own = jnp.zeros((RE, LANES), F32)
        for p in range(first, last):
            own = jnp.where(pack_lane == p, pltpu.roll(planes(p), p + 1 - iz, 1), own)
        return (
            pltpu.roll(val, 1, 1),
            pltpu.roll(val, LANES - 1, 1),
            pltpu.roll(val, 1, 0),
            pltpu.roll(val, RE - 1, 0),
            jnp.where(pack_lane < XE, own, pltpu.roll(val, XE, 1)),
            pltpu.roll(val, LANES - XE, 1),
        )

    def scaled_wide(ci, ni, co, no, inside):
        full = [jnp.minimum(ci, ni[k]) + 0.5 * (co + no[k]) for k in range(6)]
        diag = ((full[0] + full[1]) + (full[2] + full[3])) + (full[4] + full[5])
        inv = jnp.where(inside, 1.0 / diag, 0.0)
        return [jnp.where(inside, f * inv, 0.0) for f in full], diag, inv

    wide_arrive(0)

    def outer_of(inner):
        return jnp.where(inner == 0.0, 3.0, 1.0)

    for p in range(XE):
        ee[OUTER1, p] = jnp.where(inside1(p), outer_of(ee[INNER1, p]), 0.0)
    zp1[OUTER1] = jnp.where(pack_inside, outer_of(zp1[INNER1]), 0.0)
    for p in range(1, XE - 1):
        ci, ni = near1(lambda p: ee[INNER1, p], lambda p: zp1[INNER1, :, p : p + 1], p, edge=True)
        co, no = near1(lambda p: ee[OUTER1, p], lambda p: zp1[OUTER1, :, p : p + 1], p, edge=True)
        full, diag, inv = scaled_wide(ci, ni, co, no, inside1(p))
        full[4] = jnp.where(first1, 0.0, full[4])
        full[5] = jnp.where(last1, 0.0, full[5])
        for d in range(6):
            c1[d, p] = full[d]
        if GHOST <= p < X1 + GHOST:
            d1[p - GHOST] = diag[0:R1]
            b1[p - GHOST] = inv[0:R1]
    ci, co = zp1[INNER1], zp1[OUTER1]
    full, _, _ = scaled_wide(
        ci,
        near_pack(lambda p: ee[INNER1, p], ci, 0, XE),
        co,
        near_pack(lambda p: ee[OUTER1, p], co, 0, XE),
        pack_inside,
    )
    for d in range(6):
        cz1[d] = full[d]

    def stencil(b, c, near):
        a = b + c(0) * near[0]
        e = c(1) * near[1] + c(2) * near[2]
        f = c(3) * near[3] + c(4) * near[4]
        return (a + c(5) * near[5]) + (e + f)

    def update1(src, pack, p):
        val, near = near1(lambda p: src[p], lambda p: pack[:, p : p + 1], p)
        return val, stencil(ee[RHS1, p], lambda d: c1[d, p], near)

    def half1(src, pack, dst, colour, planes):
        for p in planes:
            val, new = update1(src, pack, p)
            dst[p] = jnp.where(g1.colour(p, colour), new, val)

    def half_pack(src, pack, dst, colour, first, last):
        val = pack[...]
        near = near_pack(lambda p: src[p], val, first, last)
        new = stencil(zp1[RHS1], lambda d: cz1[d], near)
        dst[...] = jnp.where(pack_own[colour], new, val)

    half_sweep(3, halo0, RED, va, vb, c0, b0, 1)
    publish(4, halo0, BLACK, vb)

    XG, RG, ZG = in2.shape
    XH, RH = XG // 2, RG // 2
    g2 = Grid(XG, RG, ZG)
    g3 = Grid(XH, RH, ZG)
    def unpack(tile, dst):
        for px in range(nx):
            for py in range(ny // 2):
                lows, highs = [], []
                for part in range(2):
                    base = (px * ny + 2 * py + part) * nz
                    s0, s1 = tile(base), tile(base + 1)
                    lows.append(jnp.where(tile_lane < half, s0, pltpu.roll(s1, half, 1)))
                    highs.append(jnp.where(tile_lane < half, pltpu.roll(s0, half, 1), s1))
                for xhi, pair in enumerate((lows, highs)):
                    p = px * X2 + xhi * 2
                    dst[p, py * 8 : py * 8 + 8, :] = jnp.where(tile_row < R2, pair[0], pltpu.roll(pair[1], R2, 0))
                    dst[p + 1, py * 8 : py * 8 + 8, :] = jnp.where(
                        tile_row < R2, pltpu.roll(pair[0], R2, 0), pair[1]
                    )

    def whole_neighbours(grid, planes, x, last, mask):
        val = planes(x)
        zero = jnp.zeros_like(val)
        xm = planes(x - 1) if x > 0 else zero
        xp = planes(x + 1) if x < grid.planes - 1 else zero
        near = [
            xm,
            xp,
            pltpu.roll(val, 1, 0),
            pltpu.roll(val, grid.rows - 1, 0),
            pltpu.roll(val, 1, 1),
            pltpu.roll(val, grid.lanes - 1, 1),
        ]
        if mask:
            near[2] = jnp.where(grid.row == 0, 0.0, near[2])
            near[3] = jnp.where(grid.row == grid.rows - 1, 0.0, near[3])
            near[4] = jnp.where(grid.lane == 0, 0.0, near[4])
            near[5] = jnp.where(grid.lane >= last, 0.0, near[5])
        return val, near

    def whole_couplings(grid, inner, outer, last, c, d, b):
        for x in range(grid.planes):
            ci, ni = whole_neighbours(grid, lambda x: inner[x], x, last, True)
            co, no = whole_neighbours(grid, lambda x: outer[x], x, last, True)
            full = [jnp.minimum(ci, ni[k]) + 0.5 * (co + no[k]) for k in range(6)]
            diag = ((full[0] + full[1]) + (full[2] + full[3])) + (full[4] + full[5])
            if last < grid.lanes - 1:
                diag = jnp.where(grid.lane <= last, diag, 1.0)
            inv = 1.0 / diag
            edges = (
                None,
                None,
                grid.row == 0,
                grid.row == grid.rows - 1,
                grid.lane == 0,
                grid.lane >= last,
            )
            for k in range(6):
                f = full[k] * inv
                if edges[k] is not None:
                    f = jnp.where(edges[k], 0.0, f)
                if last < grid.lanes - 1:
                    f = jnp.where(grid.lane <= last, f, 0.0)
                c[k, x] = f
            if d is not None:
                d[x] = diag
            b[x] = inv

    def whole_update(grid, planes, c, b, x):
        val, near = whole_neighbours(grid, planes, x, None, False)
        a = b[x] + c[2, x] * near[2]
        e = c[3, x] * near[3] + c[4, x] * near[4]
        a = a + c[5, x] * near[5]
        if x > 0:
            a = a + c[0, x] * near[0]
        if x < grid.planes - 1:
            e = e + c[1, x] * near[1]
        return val, a + e

    def restrict2(plane, factor):
        pieces = [halve_rows(tmp, x, plane(2 * x) + plane(2 * x + 1)) for x in range(XH)]
        for x in range(XH):
            tall[x * RH : (x + 1) * RH, 0:ZG] = pieces[x]
        whole = dot(tall[0 : XH * RH, 0:ZG], narrow_low) * factor
        return [whole[x * RH : (x + 1) * RH] for x in range(XH)]

    def mix(x, a, b):
        return jnp.where(g0.colour(x, 0), a, pltpu.roll(b, 1, 1))

    across = jnp.zeros((R0, LANES), F32)
    face_lane = lax.broadcasted_iota(jnp.int32, (R0, LANES), 1)
    for x in range(X0):
        along_y = jnp.where(even_row, c0[2, x], c0[3, x])
        along_x = c0[x % 2, x]
        if x == 0 or x == X0 - 1:
            xs0[x // (X0 - 1), MIXED] = mix(x, c0[x % 2, x], along_y)
        val = mix(x, jnp.where(g0.row < R0 // 2, c0[2, x], c0[3, x]), along_x)
        ys0[0, MIXED, x : x + 1, :] = val[0:1]
        ys0[1, MIXED, x : x + 1, :] = val[R0 - 1 :]
        toward = jnp.where(iz == 0, c0[5, x, :, Z0 - LANES :], c0[4, x, :, 0:LANES])
        outs = [toward] + [
            jnp.where(iz == 0, f[:, Z0 - LANES :], f[:, 0:LANES]) for f in (along_x, along_y)
        ]
        for k, end in enumerate(outs):
            at = k * X0 + x
            across = jnp.where(face_lane == at, pltpu.roll(end, at + 1 - iz, 1), across)
    zs0[MIXED] = across
    def residual0(x):
        val, new = update(halo0, BLACK, lambda x: vb[x], c0, b0, x)
        mixed[x] = jnp.where(g0.colour(x, 0), new, mixed[x])
        return d0[x] * (new - val)

    for x, val in enumerate(restrict0(residual0, 0.5, 0, inner_first(4, X1))):
        ee[RHS1, GHOST + x, 0:R1, :] = val * b1[x]
    wide_publish(1)
    halo0.put(READY, mixed)
    send(5)
    gather_send(gc_own, gc, 0)
    wide_arrive(1)
    ring = GHOST - 1
    for p in range(ring - 1, XE - ring + 1):
        v1a[p] = jnp.where(g1.colour(p, 0), ee[RHS1, p], 0.0)
    z1a[...] = jnp.where(pack_own[0], zp1[RHS1], 0.0)
    half_pack(v1a, z1a, z1b, 1, ring, XE - ring)
    half1(v1a, z1a, v1b, 1, range(ring, XE - ring))

    def residual1(x):
        val, new = update1(v1b, z1b, GHOST + x)
        return d1[x] * (new - val)[0:R1]

    gr_own[...] = restrict1(residual1, 0.5)
    gather_send(gr_own, gr, 1)
    for p in (0, 1, XE - 2, XE - 1):
        v1a[p] = jnp.where(g1.colour(p, 0), ee[RHS1, p], 0.0)
    half_pack(v1a, z1a, z1b, 1, 0, XE)
    half1(v1a, z1a, v1b, 1, (1, 2, XE - 3, XE - 2))
    gather_wait(gc, 0, True)
    unpack(lambda t: gc[t], in2)
    for x in range(XG):
        out2[x] = outer_of(in2[x])
    whole_couplings(g2, in2, out2, ZG - 1, c2, d2, b2)
    for x, val in enumerate(restrict2(lambda x: in2[x], 0.125)):
        v3[x] = val
    for x, val in enumerate(restrict2(lambda x: out2[x], 0.125)):
        v2a[x, 0:RH] = val
    whole_couplings(g3, v3, v2a.at[:, 0:RH], ZG // 2 - 1, c3, None, b3)

    XP = XH // 2
    own = (g3.even, g3.odd)

    def pack(colour, near, far):
        return jnp.where(own[colour], near, far)

    for colour in range(2):
        for p in range(XP):
            a, z = 2 * p, 2 * p + 1
            k3[colour * 6, p] = pack(colour, c3[1, a], c3[0, z])
            k3[colour * 6 + 1, p] = pack(colour, c3[0, a], c3[1, z])
            for k in range(2, 6):
                k3[colour * 6 + k, p] = pack(colour, c3[k, a], c3[k, z])
            if colour == 0:
                for k in range(6):
                    k3[12 + k, p] = pltpu.roll(k3[k, p], 1, 1)
                    k3[18 + k, p] = pltpu.roll(k3[k, p], ZG - 1, 1)

    gather_wait(gr, 1, True)
    arrive(5)
    unpack(lambda t: gr[t], v2b)
    for x in range(XG):
        b2[x] = v2b[x] * b2[x]
        v2a[x] = jnp.where(g2.colour(x, 0), b2[x], 0.0)
    for x in range(XG):
        val, new = whole_update(g2, lambda x: v2a[x], c2, b2, x)
        v2b[x] = jnp.where(g2.colour(x, 1), new, val)

    def residual2(x):
        val, new = whole_update(g2, lambda x: v2b[x], c2, b2, x)
        return d2[x] * (new - val)

    for x, val in enumerate(restrict2(residual2, 0.5)):
        b3[x] = val * b3[x]

    for colour in range(2):
        for p in range(XP):
            h3[colour, p] = pack(colour, b3[2 * p], b3[2 * p + 1])
    none = jnp.zeros((RH, ZG), F32)

    at_shift = {0: 0, 1: 12, -1: 18}
    first_h = {s: [pltpu.roll(h3[0, p], s % ZG, 1) if s else h3[0, p] for p in range(XP)] for s in STEPS}

    def relaxed(colour, shift, shifted):
        fresh = []
        for p in range(XP):
            val, at = shifted[shift][p], colour * 6 + at_shift[shift]
            before = shifted[shift][p - 1] if p > 0 else none
            after = shifted[shift][p + 1] if p < XP - 1 else none
            i = (h3[1, p] if colour else first_h[shift][p]) + k3[at, p] * val
            mask = own[(colour + shift) % 2]
            j = k3[at + 1, p] * jnp.where(mask, before, after) + k3[at + 2, p] * pltpu.roll(val, 1, 0)
            l = k3[at + 3, p] * pltpu.roll(val, RH - 1, 0) + k3[at + 4, p] * shifted[shift + 1][p]
            fresh.append((i + k3[at + 5, p] * shifted[shift - 1][p]) + (j + l))
        return fresh

    def coarse(step, state):
        shifted = {0: state[XP:]}
        for s in (-2, -1, 1, 2):
            shifted[s] = [pltpu.roll(v, s % ZG, 1) for v in shifted[0]]
        red = {s: relaxed(0, s, shifted) for s in STEPS}
        return tuple(red[0] + relaxed(1, 0, red))

    start = relaxed(1, 0, first_h)
    state = lax.fori_loop(1, COARSE_SWEEPS, coarse, tuple(first_h[0] + start))
    solved = []
    for p in range(XP):
        solved.append(pack(0, state[p], state[XP + p]))
        solved.append(pack(1, state[p], state[XP + p]))
    for x in range(XH):
        tall[x * RH : (x + 1) * RH, 0:ZG] = solved[x]
    wide = dot(tall[0 : XH * RH, 0:ZG], double12)
    for x in range(XH):
        corr = double_rows(tmp, x, wide[x * RH : (x + 1) * RH])
        v2a[2 * x] = v2b[2 * x] + corr
        v2a[2 * x + 1] = v2b[2 * x + 1] + corr
    for colour, src, dst in ((0, v2a, v2b), (1, v2b, v2a)):
        for x in range(XG):
            val, new = whole_update(g2, lambda x: src[x], c2, b2, x)
            dst[x] = jnp.where(g2.colour(x, colour), new, val)

    row_shift = lax.rem(RG - iy * R2, RG)
    lane_shift = lax.rem(ZG - iz * half, ZG)
    edge2 = GHOST // 2
    rows2 = R2 + 2 * edge2
    planes2 = X2 + 2 * edge2
    for k in range(planes2):
        part = v2a[jnp.clip(ix * X2 + k - edge2, 0, XG - 1)]
        part = pltpu.roll(pltpu.roll(part, row_shift, 0), lane_shift, 1)
        tall[k * rows2 : (k + 1) * rows2, 0:ZG] = jnp.where(
            tile_row < R2 + edge2, part[0:rows2], part[RG - rows2 : RG]
        )
    source = lax.broadcasted_iota(jnp.int32, (ZG, LANES), 0)
    target = lax.broadcasted_iota(jnp.int32, (ZG, LANES), 1)
    target = lax.div(target, 2 * XE)
    pick = jnp.where(source == jnp.where(iz == 0, half + target, ZG - 1 - target), 1.0, 0.0).astype(F32)
    coarse_rows = tall[0 : planes2 * rows2, 0:ZG]
    wide = dot(coarse_rows, double12)
    sides = dot(coarse_rows, pick)
    acc = jnp.zeros((rows2, LANES), F32)
    tile_plane = lax.div(jnp.bitwise_and(tile_lane, XE - 1), 2)
    for k in range(planes2):
        acc = jnp.where(tile_plane == k, sides[k * rows2 : (k + 1) * rows2], acc)
    z1a[...] = z1b[...] + jnp.where(pack_inside, double_rows(tmp, 0, acc), 0.0)
    for k in range(planes2):
        corr = double_rows(tmp, k, wide[k * rows2 : (k + 1) * rows2])
        for p in (2 * k, 2 * k + 1):
            if 0 < p < XE - 1:
                v1a[p] = v1b[p] + jnp.where(inside1(p), corr, 0.0)
    half_pack(v1a, z1a, z1b, 0, 1, XE - 1)
    half1(v1a, z1a, v1b, 0, range(2, XE - 2))
    half_pack(v1b, z1b, z1a, 1, 2, XE - 2)
    half1(v1b, z1b, v1a, 1, range(3, XE - 3))

    def enlarge(count, read, write):
        for x in range(count):
            tall[x * R1 : (x + 1) * R1, 0:Z1] = read(x)
        wide = dot(tall[0 : count * R1, 0:Z1], double01)
        for x in range(count):
            write(x, double_rows(tmp, x, wide[x * R1 : (x + 1) * R1]))

    def inside(x, corr):
        va[2 * x] = vb[2 * x] + corr
        va[2 * x + 1] = vb[2 * x + 1] + corr

    enlarge(X1, lambda x: v1a[GHOST + x, 0:R1, :], inside)
    diagonal = tile_lane == tile_row + GHOST
    stack, lined_stack = [], []
    own_pack = jnp.zeros((RE, LANES), F32)
    for p in range(GHOST, XE - GHOST):
        own_pack = jnp.where(pack_lane == p, pltpu.roll(v1a[p], p + 1 - iz, 1), own_pack)
    for k in range(2):
        p, own = (GHOST - 1, GHOST) if k == 0 else (X1 + GHOST, X1 + GHOST - 1)
        val, near = near1(lambda p: v1a[p], lambda p: z1a[:, p : p + 1], p, edge=True)
        stack += [val[0:R1]] + [(other - val)[0:R1] for other in (v1a[own], near[2], near[3])]
        lined_stack.append(((near[4] - val)[0:R1], (near[5] - val)[0:R1]))
    for k in range(2):
        row, own = (RE - 1, 0) if k == 0 else (R1, R1 - 1)
        for p in range(GHOST - 1, X1 + GHOST + 1):
            yrim[k, p : p + 1, :] = v1a[p, row : row + 1, :]
            if GHOST <= p < X1 + GHOST:
                yrim[2 + k, p : p + 1, :] = v1a[p, own : own + 1, :]
        val = yrim[k, GHOST : X1 + GHOST, :]
        others = [
            yrim[2 + k, GHOST : X1 + GHOST, :],
            yrim[k, GHOST - 1 : X1 + GHOST - 1, :],
            yrim[k, GHOST + 1 : X1 + GHOST + 1, :],
        ]
        stack += [val] + [other - val for other in others]
        line = jnp.where(diagonal, jnp.broadcast_to(z1a[row : row + 1, :], (8, LANES)), 0.0)
        column = jnp.broadcast_to(jnp.sum(line, axis=1, keepdims=True), (8, LANES))
        back = jnp.where(tile_lane == 0, jnp.where(iz == 0, 0.0, column), pltpu.roll(val, 1, 1))
        ahead = jnp.where(tile_lane == Z1 - 1, jnp.where(iz == 0, column, 0.0), pltpu.roll(val, Z1 - 1, 1))
        lined_stack.append((back - val, ahead - val))
    val = z1a[...]
    shifts = [pltpu.roll(val, 1, 0), pltpu.roll(val, RE - 1, 0), pltpu.roll(val, 1, 1), pltpu.roll(val, LANES - 1, 1)]
    face = [val, own_pack - val] + [other - val for other in shifts]
    face = [pltpu.roll(f[0:R1], LANES - GHOST, 1) for f in face]
    stack += face[:4]
    lined_stack.append((face[4], face[5]))
    for i, piece in enumerate(stack):
        tall[i * R1 : (i + 1) * R1, 0:Z1] = piece
    for i, (back, ahead) in enumerate(lined_stack):
        tall2[i * R1 : (i + 1) * R1, 0:Z1] = back
        tall2[i * R1 : (i + 1) * R1, Z1 : 2 * Z1] = ahead
    k = lax.broadcasted_iota(jnp.int32, (2 * Z1, Z0), 0)
    j = lax.broadcasted_iota(jnp.int32, (2 * Z1, Z0), 1)
    source = lax.shift_right_logical(j, 1) + Z1 * jnp.bitwise_and(j, 1)
    big = dot(tall[0 : len(stack) * R1, 0:Z1], double01)
    lined_big = dot(tall2[0 : len(lined_stack) * R1, :], jnp.where(k == source, 1.0, 0.0).astype(F32))

    def woven(slot, first, second):
        parts = []
        for k in range(Z0 // LANES):
            at = 2 * slot + k
            tmp[at, pl.ds(0, R1, 2), :] = first[:, k * LANES : (k + 1) * LANES]
            tmp[at, pl.ds(1, R1, 2), :] = second[:, k * LANES : (k + 1) * LANES]
            parts.append(tmp[at, 0:R0, :])
        return jnp.concatenate(parts, axis=1)

    def finished(k):
        piece = [big[(4 * k + i) * R1 : (4 * k + i + 1) * R1] for i in range(4)]
        lines = lined_big[k * R1 : (k + 1) * R1]
        at = 4 * (k % 2)
        return (
            woven(at, piece[0], piece[0]),
            woven(at + 1, piece[1], piece[1]),
            woven(at + 2, piece[2], piece[3]),
            woven(at + 3, lines, lines),
        )

    for k in range(4):
        ref, side = (xh0, k) if k < 2 else (yh0, k - 2)
        corr, toward, beside, lengthwise = finished(k)
        ref[side, FIXED] = ref[side, BLACK] + corr
        first, second = ref[side, MIXED], ref[side, READY]
        ref[side, LAST] = ((second + corr) + first * toward) + (
            pltpu.roll(first, Z0 - 1, 1) * beside + pltpu.roll(second, Z0 - 1, 1) * lengthwise
        )
    corr, toward, beside, sideways = [f[:, 0:LANES] for f in finished(4)]
    zh0[FIXED] = zh0[BLACK] + corr
    first = zh0[MIXED]
    zh0[LAST] = ((zh0[READY] + corr) + first * toward) + (
        pltpu.roll(first, LANES - X0, 1) * sideways + pltpu.roll(first, LANES - 2 * X0, 1) * beside
    )
    half_sweep(None, halo0, FIXED, va, vb, c0, b0, 0)
    half_sweep(None, halo0, LAST, vb, ext_out, c0, b0, 1)

    for number in range(len(EXCHANGES)):
        sent(number)
    for number in range(len(WIDE)):
        wide_sent(number)
    gather_wait(gc, 0, False)
    gather_wait(gr, 1, False)


def finish(*refs):
    count = (len(refs) - 1) // 2
    sem = refs[-1]
    copies = [pltpu.make_async_copy(refs[i], refs[count + i], sem.at[i]) for i in range(count)]
    for copy in copies:
        copy.start()
    for copy in copies:
        copy.wait()


def solution(mesh):
    nx, ny, nz = (mesh.shape[a] for a in ("gx", "gy", "gz"))
    spec = P("gx", "gy", "gz")

    def on_device(membrane, recovery, extracellular, fiber_scale, labels):
        X, R, Z = membrane.shape
        X1, R1, Z1 = X // 2, R // 2, Z // 2
        XG, RG, ZG = nx * X // 4, ny * R // 4, nz * Z // 4
        assert nz == 2 and ny % 2 == 0 and ZG == LANES and Z1 == LANES
        assert R1 == 8 and X1 == 8 and X % 8 == 0
        total = nx * ny * nz
        assert labels.shape == (2, 2, LANES // 4)
        f0 = 11
        field = (X, R, Z)
        lvl1 = (X1, R1, Z1)
        whole = (XG, RG, ZG)
        third = (XG // 2, RG // 2, ZG)

        def v(*shape):
            return pltpu.VMEM(shape, F32)

        def faces(f, x, r, z):
            return [v(2, f, r, z), v(2, f, x, z), v(f, r, LANES)] * 2

        anywhere = pl.BlockSpec(memory_space=pl.ANY)
        scratch = [v(*field)] * 4 + [pltpu.VMEM(labels.shape, jnp.int32), pltpu.SemaphoreType.DMA((5,))]
        scratch += faces(f0, *field)
        scratch += [v(*field), v(*field), v(*field), v(6, *field), v(6, *field), v(*field), v(*field)]
        scratch += [v(*field), v(*field)]
        scratch += [
            v(2 * max(X1, XG // 2), max(R, RG), LANES),
            v(max(X1 * R1, (XG // 2) * (RG // 2), 2 * X1 * R1, 20 * R1, total), Z),
        ]
        XE, RE = X1 + 2 * GHOST, R1 + 2 * GHOST
        assert GHOST * XE <= LANES and 2 * GHOST == R1 and GHOST <= X1
        wide, pack = (XE, RE, Z1), (RE, LANES)
        scratch += [v(3, *wide), v(2, 3, X1 // 2, R1, Z1), v(2, 3, XE // 2, R1, Z1), v(3, R1, LANES)]
        scratch += [v(9, 3, R1, LANES), v(3, *pack), v(6, *wide), v(6, *pack), v(*lvl1), v(*lvl1)]
        scratch += [v(*wide), v(*wide), v(*pack), v(*pack), v(4, XE, Z1)]
        scratch += [v(*field), v(8 * R1, Z)]
        scratch += [v(8, LANES), v(total, 8, LANES), v(8, LANES), v(total, 8, LANES)]
        scratch += [v(*whole), v(*whole), v(6, *whole), v(*whole), v(*whole), v(*whole), v(*whole)]
        scratch += [v(6, *third), v(*third), v(*third)]
        packed = (XG // 4, RG // 2, ZG)
        scratch += [v(24, *packed), v(2, *packed)]
        sems = SIDES * len(EXCHANGES)
        scratch += [pltpu.SemaphoreType.DMA((sems,))] * 2
        scratch += [pltpu.SemaphoreType.DMA((WIDE_SIDES * len(WIDE),))] * 2
        scratch += [pltpu.SemaphoreType.DMA((2,))] * 2
        vmem = pl.BlockSpec(memory_space=pltpu.VMEM)
        room = 54400 << 10
        shape = jax.ShapeDtypeStruct(field, F32)
        results = pl.pallas_call(
            functools.partial(kernel, (nx, ny, nz)),
            out_shape=[shape] * 3,
            in_specs=[anywhere] * 5,
            out_specs=[vmem] * 3,
            scratch_shapes=scratch,
            compiler_params=pltpu.CompilerParams(
                collective_id=0, has_side_effects=True, vmem_limit_bytes=room
            ),
        )(membrane, recovery, extracellular, fiber_scale, labels)
        return tuple(
            pl.pallas_call(
                finish,
                out_shape=[shape] * 3,
                in_specs=[vmem] * 3,
                out_specs=[anywhere] * 3,
                scratch_shapes=[pltpu.SemaphoreType.DMA((3,))],
                compiler_params=pltpu.CompilerParams(vmem_limit_bytes=4 << 20),
            )(*results)
        )

    return jax.shard_map(
        on_device,
        mesh=mesh,
        in_specs=(spec,) * 5,
        out_specs=(spec,) * 3,
        check_vma=False,
    )
```

```python
import functools

import jax
import jax.numpy as jnp
from jax import lax
from jax.experimental import pallas as pl
from jax.experimental.pallas import tpu as pltpu
from jax.sharding import PartitionSpec as P

COARSE_SWEEPS = 8
TIME_STEP = 0.05
ionic_gain = 8.0
ionic_onset = 0.15
recovery_rate = 0.01
MESH = pl.DeviceIdType.MESH
LOGICAL = pl.DeviceIdType.LOGICAL
LANES = 128
F32 = jnp.float32

INNER, U, OUTER, V, NEXT, RED, BLACK, MIXED, READY, FIXED, LAST = range(11)
INNER1, OUTER1, RHS1 = range(3)
GHOST = 4
EXCHANGES = (
    (INNER, 2),
    (V, 1),
    (NEXT, 1),
    (RED, 1),
    (BLACK, 1),
    (MIXED, 2),
)
SIDES = 5
WIDE = ((INNER1, 1), (RHS1, 1))
STEPS = (-1, 0, 1)
WIDE_SIDES = 17


def dot(a, b):
    high = a.astype(jnp.bfloat16)
    rest = a - high.astype(F32)
    middle = rest.astype(jnp.bfloat16)
    low = (rest - middle.astype(F32)).astype(jnp.bfloat16)
    chosen = b.astype(jnp.bfloat16)
    rows = a.shape[0]
    both = jnp.dot(jnp.concatenate([low, middle, high], axis=0), chosen, preferred_element_type=F32)
    parts = [both[i * rows : (i + 1) * rows] for i in range(3)]
    return (parts[0] + parts[1]) + parts[2]


def pair_matrix(rows, cols, offset):
    j = lax.broadcasted_iota(jnp.int32, (rows, cols), 0)
    k = lax.broadcasted_iota(jnp.int32, (rows, cols), 1)
    return jnp.where(lax.shift_right_logical(j, 1) + offset == k, 1.0, 0.0).astype(F32)


def copy_matrix(rows, cols, shift):
    k = lax.broadcasted_iota(jnp.int32, (rows, cols), 0)
    j = lax.broadcasted_iota(jnp.int32, (rows, cols), 1)
    return jnp.where(lax.shift_right_logical(j, shift) == k, 1.0, 0.0).astype(F32)


class Grid:
    def __init__(self, planes, rows, lanes):
        self.planes, self.rows, self.lanes = planes, rows, lanes
        self.row = lax.broadcasted_iota(jnp.int32, (rows, lanes), 0)
        self.lane = lax.broadcasted_iota(jnp.int32, (rows, lanes), 1)
        self.even = jnp.bitwise_and(self.row + self.lane, 1) == 0
        self.odd = jnp.bitwise_and(self.row + self.lane, 1) == 1

    def colour(self, x, colour):
        return self.even if (x + colour) % 2 == 0 else self.odd


class Halo:
    def __init__(self, grid, refs, iz):
        self.grid, self.iz = grid, iz
        self.xs, self.ys, self.zs, self.xh, self.yh, self.zh = refs
        self.flane = lax.broadcasted_iota(jnp.int32, (grid.rows, LANES), 1)

    def faces(self, slot, planes):
        g = self.grid
        acc = jnp.zeros((g.rows, LANES), F32)
        for x, val in planes:
            self.ys[0, slot, x : x + 1, :] = val[0:1]
            self.ys[1, slot, x : x + 1, :] = val[g.rows - 1 :]
            if g.lanes > LANES:
                end = jnp.where(self.iz == 0, val[:, g.lanes - LANES :], val[:, :LANES])
            else:
                end = val
            acc = jnp.where(self.flane == x, pltpu.roll(end, x + 1 - self.iz, 1), acc)
            yield
        self.zs[slot] = acc

    def put_ends(self, slot, ref):
        self.xs[0, slot] = ref[0]
        self.xs[1, slot] = ref[self.grid.planes - 1]

    def put_rest(self, slot, ref):
        for _ in self.faces(slot, [(x, ref[x]) for x in range(self.grid.planes)]):
            pass

    def put(self, slot, ref):
        self.put_ends(slot, ref)
        self.put_rest(slot, ref)

    def neighbours(self, slot, planes, x, edge=False):
        g = self.grid
        val = planes(x)
        xm = planes(x - 1) if x > 0 else self.xh[0, slot]
        xp = planes(x + 1) if x < g.planes - 1 else self.xh[1, slot]
        shape = (g.rows, g.lanes)
        low = jnp.broadcast_to(self.yh[0, slot, x : x + 1, :], shape)
        high = jnp.broadcast_to(self.yh[1, slot, x : x + 1, :], shape)
        ym = jnp.where(g.row == 0, low, pltpu.roll(val, 1, 0))
        yp = jnp.where(g.row == g.rows - 1, high, pltpu.roll(val, g.rows - 1, 0))
        side = jnp.broadcast_to(self.zh[slot, :, x : x + 1], shape)
        side_m, side_p = side, side
        if edge:
            side_m = jnp.where(self.iz == 0, 0.0, side)
            side_p = jnp.where(self.iz == 0, side, 0.0)
        zm = jnp.where(g.lane == 0, side_m, pltpu.roll(val, 1, 1))
        zp = jnp.where(g.lane == g.lanes - 1, side_p, pltpu.roll(val, g.lanes - 1, 1))
        return val, (xm, xp, ym, yp, zm, zp)


def halve_rows(tmp, slot, val):
    rows, lanes = val.shape
    parts = []
    for k in range(lanes // LANES):
        at = 2 * slot + k
        tmp[at, 0:rows, :] = val[:, k * LANES : (k + 1) * LANES]
        parts.append(tmp[at, pl.ds(0, rows // 2, 2), :] + tmp[at, pl.ds(1, rows // 2, 2), :])
    return parts[0] if len(parts) == 1 else jnp.concatenate(parts, axis=1)


def double_rows(tmp, slot, val):
    rows, lanes = val.shape
    parts = []
    for k in range(lanes // LANES):
        at = 2 * slot + k
        piece = val[:, k * LANES : (k + 1) * LANES]
        tmp[at, pl.ds(0, rows, 2), :] = piece
        tmp[at, pl.ds(1, rows, 2), :] = piece
        parts.append(tmp[at, 0 : 2 * rows, :])
    return parts[0] if len(parts) == 1 else jnp.concatenate(parts, axis=1)


def kernel(counts, *refs):
    sources, (mem_out, rec_out, ext_out) = refs[:5], refs[5:8]
    refs = refs[8:]
    mem, rec, ext, fib, lab, in_sem = refs[:6]
    refs = (None,) + refs
    (xs0, ys0, zs0, xh0, yh0, zh0) = refs[7:13]
    (in0, out0, uu, w0, c0, d0, b0, va, vb, tmp, tall) = refs[13:24]
    (ee, ys1, yr1, zs1, zr1, zp1, c1, cz1, d1, b1, v1a, v1b, z1a, z1b, yrim, mixed, tall2) = refs[24:41]
    (gc_own, gc, gr_own, gr, in2, out2, c2, d2, b2, v2a, v2b) = refs[41:52]
    (c3, b3, v3, k3, h3, send_sem, recv_sem, wide_send, wide_recv, gs_sem, gr_sem) = refs[52:]
    nx, ny, nz = counts
    ix, iy, iz = lax.axis_index("gx"), lax.axis_index("gy"), lax.axis_index("gz")
    me = (ix * ny + iy) * nz + iz
    total = nx * ny * nz

    loads = [
        pltpu.make_async_copy(src, dst, in_sem.at[i])
        for i, (src, dst) in enumerate(zip(sources, (mem, rec, ext, fib, lab)))
    ]
    for i in (4, 3, 0, 2, 1):
        loads[i].start()

    barrier = pltpu.get_barrier_semaphore()

    def others(body):
        for i in sorted(range(1, total), key=lambda i: (abs(i // nz % ny * 2 - ny), i)):
            dev = me + i
            body(jnp.where(dev >= total, dev - total, dev))

    close = nx <= 4 and ny <= 4
    if close:
        greeted = -1
        for dx in (-1, 0, 1):
            for dy in (-1, 0, 1):
                present = (ix + dx >= 0) & (ix + dx < nx) & (iy + dy >= 0) & (iy + dy < ny)
                greeted = greeted + jnp.where(present, nz, 0)
                for z in (iz, 1 - iz):
                    if dx == 0 and dy == 0 and z is iz:
                        continue

                    def hail(where=(ix + dx, iy + dy, z)):
                        pl.semaphore_signal(barrier, inc=1, device_id=where, device_id_type=MESH)

                    pl.when(present)(hail)
    else:
        greeted = total - 1
        others(lambda dev: pl.semaphore_signal(barrier, inc=1, device_id=dev, device_id_type=LOGICAL))

    def clear(missing, ref, side):
        def fill():
            ref[side] = jnp.zeros(ref.at[side].shape, F32)

        pl.when(missing)(fill)

    X1, R1, Z1 = mem.shape[0] // 2, mem.shape[1] // 2, mem.shape[2] // 2
    XE, RE = X1 + 2 * GHOST, R1 + 2 * GHOST
    clear(ix == 0, xh0, 0)
    clear(ix == nx - 1, xh0, 1)
    clear(iy == 0, yh0, 0)
    clear(iy == ny - 1, yh0, 1)
    for slot in range(3):
        for p in range(GHOST):
            clear(ix == 0, ee, (slot, p))
            clear(ix == nx - 1, ee, (slot, XE - 1 - p))
    for load in loads:
        load.wait()

    g0 = Grid(*mem.shape)
    g1 = Grid(XE, RE, Z1)
    halo0 = Halo(g0, (xs0, ys0, zs0, xh0, yh0, zh0), iz)

    def copies(number):
        first, slots = EXCHANGES[number]
        h = halo0
        part = pl.ds(first, slots)
        plan = (
            (h.xs.at[0, part], h.xh.at[1, part], (ix - 1, iy, iz), ix > 0, ix < nx - 1),
            (h.xs.at[1, part], h.xh.at[0, part], (ix + 1, iy, iz), ix < nx - 1, ix > 0),
            (h.ys.at[0, part], h.yh.at[1, part], (ix, iy - 1, iz), iy > 0, iy < ny - 1),
            (h.ys.at[1, part], h.yh.at[0, part], (ix, iy + 1, iz), iy < ny - 1, iy > 0),
            (h.zs.at[part], h.zh.at[part], (ix, iy, 1 - iz), None, None),
        )
        for side, (src, dst, dev, goes, comes) in enumerate(plan):
            copy = pltpu.make_async_remote_copy(
                src_ref=src,
                dst_ref=dst,
                send_sem=send_sem.at[number * SIDES + side],
                recv_sem=recv_sem.at[number * SIDES + side],
                device_id=dev,
                device_id_type=MESH,
            )
            yield copy, goes, comes

    ends, rest = slice(0, 2), slice(2, SIDES)

    def send(number, sides=slice(0, SIDES)):
        for copy, goes, _ in list(copies(number))[sides]:
            if goes is None:
                copy.start()
            else:
                pl.when(goes)(copy.start)

    def arrive(number, sides=slice(0, SIDES)):
        for copy, _, comes in list(copies(number))[sides]:
            if comes is None:
                copy.wait_recv()
            else:
                pl.when(comes)(copy.wait_recv)

    def inner_first(number, count):
        arrive(number, rest)
        yield from range(1, count - 1)
        arrive(number, ends)
        yield 0
        yield count - 1

    def publish(number, halo, slot, ref):
        halo.put_ends(slot, ref)
        send(number, ends)
        halo.put_rest(slot, ref)
        send(number, rest)

    def sent(number):
        for copy, goes, _ in copies(number):
            if goes is None:
                copy.wait_send()
            else:
                pl.when(goes)(copy.wait_send)

    here = {-1: ix > 0, 0: None, 1: ix < nx - 1}
    along = {-1: iy > 0, 0: None, 1: iy < ny - 1}

    def both(a, b):
        if a is None or b is None:
            return b if a is None else a
        return jnp.logical_and(a, b)

    def wide_copies(number):
        first, count = WIDE[number]
        part = pl.ds(first, count)
        pairs, edge = X1 // 2, GHOST // 2
        plan = []
        for sx in (-1, 1):
            src = ee.at[part, pl.ds(GHOST if sx < 0 else X1, GHOST), pl.ds(0, R1)]
            dst = ee.at[part, pl.ds(X1 + GHOST if sx < 0 else 0, GHOST), pl.ds(0, R1)]
            plan.append((src, dst, sx, 0, iz))
        for sx in STEPS:
            for sy in (-1, 1):
                mine, theirs = (0, 1) if sy < 0 else (1, 0)
                at = {-1: (0, edge, pairs + edge), 0: (0, pairs, edge), 1: (pairs - edge, edge, 0)}[sx]
                src = ys1.at[mine, part, pl.ds(at[0], at[1])]
                dst = yr1.at[theirs, part, pl.ds(at[2], at[1])]
                plan.append((src, dst, sx, sy, iz))
        for sx in STEPS:
            for sy in STEPS:
                plan.append((zs1.at[part], zr1.at[(1 - sx) * 3 + 1 - sy, part], sx, sy, 1 - iz))
        for side, (src, dst, sx, sy, z) in enumerate(plan):
            copy = pltpu.make_async_remote_copy(
                src_ref=src,
                dst_ref=dst,
                send_sem=wide_send.at[number * WIDE_SIDES + side],
                recv_sem=wide_recv.at[number * WIDE_SIDES + side],
                device_id=(ix + sx, iy + sy, z),
                device_id_type=MESH,
            )
            yield copy, both(here[sx], along[sy]), both(here[-sx], along[-sy])

    def maybe(condition, action):
        if condition is None:
            action()
        else:
            pl.when(condition)(action)

    tile_row = lax.broadcasted_iota(jnp.int32, (8, LANES), 0)
    tile_lane = lax.broadcasted_iota(jnp.int32, (8, LANES), 1)

    def wide_publish(number):
        first, count = WIDE[number]
        plan = list(wide_copies(number))

        def start(group):
            for copy, goes, _ in group:
                maybe(goes, copy.start)

        start(plan[:2])
        for slot in range(first, first + count):
            for k in range(X1 // 2):
                even, odd = ee[slot, GHOST + 2 * k, 0:R1, :], ee[slot, GHOST + 2 * k + 1, 0:R1, :]
                ys1[0, slot, k] = jnp.where(tile_row < GHOST, even, pltpu.roll(odd, GHOST, 0))
                ys1[1, slot, k] = jnp.where(tile_row < GHOST, pltpu.roll(odd, GHOST, 0), even)
        start(plan[2:8])
        for slot in range(first, first + count):
            acc = jnp.zeros((R1, LANES), F32)
            for x in range(X1):
                val = ee[slot, GHOST + x, 0:R1, :]
                for depth in range(GHOST):
                    at = depth * XE + GHOST + x
                    shift = jnp.where(iz == 0, at + 1 + depth, at - depth)
                    acc = jnp.where(tile_lane == at, pltpu.roll(val, shift, 1), acc)
            zs1[slot] = acc
        start(plan[8:])

    def keep(condition, val):
        return val if condition is None else jnp.where(condition, val, 0.0)

    def plane_side(p):
        return here[-1 if p < GHOST else (1 if p >= X1 + GHOST else 0)]

    def wide_arrive(number):
        first, count = WIDE[number]
        for copy, _, comes in wide_copies(number):
            maybe(comes, copy.wait_recv)
        low = tile_row >= GHOST
        pe = jnp.bitwise_and(tile_lane, XE - 1)
        for slot in range(first, first + count):
            for p in range(XE):
                after, before = yr1[1, slot, p // 2], yr1[0, slot, p // 2]
                if p % 2:
                    after, before = pltpu.roll(after, GHOST, 0), pltpu.roll(before, GHOST, 0)
                side = plane_side(p)
                after = keep(both(side, along[1]), after)
                before = keep(both(side, along[-1]), before)
                ee[slot, p, R1:RE, :] = jnp.where(low, before, after)
            rows = []
            for sy in STEPS:
                mid = zr1[3 + sy + 1, slot]
                left = keep(here[-1], pltpu.roll(zr1[sy + 1, slot], LANES - X1, 1))
                right = keep(here[1], pltpu.roll(zr1[6 + sy + 1, slot], X1, 1))
                val = jnp.where(pe < GHOST, left, jnp.where(pe >= X1 + GHOST, right, mid))
                rows.append(keep(along[sy], jnp.where(tile_lane < GHOST * XE, val, 0.0)))
            zp1[slot, 0:R1, :] = rows[1]
            zp1[slot, R1:RE, :] = jnp.where(low, rows[0], rows[2])

    def wide_sent(number):
        for copy, goes, _ in wide_copies(number):
            maybe(goes, copy.wait_send)

    def gather_send(own, whole, which):
        def go(dev):
            pltpu.make_async_remote_copy(
                src_ref=own,
                dst_ref=whole.at[me],
                send_sem=gs_sem.at[which],
                recv_sem=gr_sem.at[which],
                device_id=dev,
                device_id_type=LOGICAL,
            ).start()

        others(go)
        whole[pl.ds(me, 1)] = own[...][None]

    def gather_wait(whole, which, recv):
        rest = whole.at[pl.ds(0, total - 1)]
        copy = pltpu.make_async_remote_copy(
            src_ref=rest,
            dst_ref=rest,
            send_sem=gs_sem.at[which],
            recv_sem=gr_sem.at[which],
            device_id=(ix, iy, 1 - iz),
            device_id_type=MESH,
        )
        if recv:
            copy.wait_recv()
        else:
            copy.wait_send()

    X0, R0, Z0 = mem.shape
    X2 = X1 // 2
    R2 = R1 // 2
    half = Z1 // 2

    widen8 = copy_matrix(lab.shape[2], Z0, 3)
    lab_planes = []
    for bx in range(lab.shape[0]):
        wide = jnp.dot(lab[bx].astype(F32), widen8, preferred_element_type=F32)
        lab_planes.append(
            jnp.concatenate(
                [jnp.broadcast_to(wide[by : by + 1], (8, Z0)) for by in range(lab.shape[1])], axis=0
            )
        )

    def label_of(x):
        return lab_planes[x // 8]

    for x in range(X0):
        label = label_of(x)
        in0[x] = jnp.where(label == 1.0, 1.0, jnp.where(label == 2.0, 0.3, 0.0)) * fib[x]
        out0[x] = jnp.where(label == 0.0, 3.0, 1.0)
        uu[x] = mem[x] + ext[x]
    halo0.put_ends(INNER, in0)
    halo0.put_ends(U, uu)
    pl.semaphore_wait(barrier, greeted)
    send(0, ends)
    halo0.put_rest(INNER, in0)
    halo0.put_rest(U, uu)
    send(0, rest)
    halo0.put(V, ext)
    send(1)

    narrow = pair_matrix(Z0, Z1, 0)
    narrow_low = pair_matrix(Z1, Z1, 0)
    narrow_high = pair_matrix(Z1, Z1, half)
    double01 = copy_matrix(Z1, Z0, 1)
    double12 = copy_matrix(Z1, Z1, 1)

    def restrict0(plane, factor, base, order=None):
        for x in order or range(X1):
            tall[base + x * R1 : base + (x + 1) * R1, :] = halve_rows(tmp, x, plane(2 * x) + plane(2 * x + 1))
        whole = dot(tall[base : base + X1 * R1, :], narrow) * factor
        return [whole[x * R1 : (x + 1) * R1] for x in range(X1)]

    def restrict1(plane, factor, order=None):
        rows = [None] * X2
        for x in order or range(X2):
            rows[x] = halve_rows(tmp, x, plane(2 * x) + plane(2 * x + 1))
        low = jnp.concatenate(rows[: X2 // 2], axis=0)
        high = jnp.concatenate(rows[X2 // 2 :], axis=0)
        return (dot(low, narrow_low) + dot(high, narrow_high)) * factor

    for x in inner_first(0, X0):
        centre, near = halo0.neighbours(INNER, lambda x: in0[x], x, edge=True)
        u, near_u = halo0.neighbours(U, lambda x: uu[x], x)
        drive = jnp.zeros_like(u)
        for d in range(6):
            weight = jnp.minimum(centre, near[d])
            w0[d, x] = weight
            drive = drive + weight * (near_u[d] - u)
        m, r = mem[x], rec[x]
        tissue = jnp.where(label_of(x) != 0.0, 1.0, 0.0)
        ionic = ionic_gain * m * (m - ionic_onset) * (m - 1.0) + m * r
        mem_out[x] = m + TIME_STEP * (drive - tissue * ionic)
    publish(2, halo0, NEXT, mem_out)
    for x in range(X0):
        m, r = mem[x], rec[x]
        rec_out[x] = r + TIME_STEP * recovery_rate * (-r - ionic_gain * m * (m - ionic_onset - 1.0))

    for x, val in enumerate(restrict0(lambda x: in0[x], 0.125, 0)):
        ee[INNER1, GHOST + x, 0:R1, :] = val
    wide_publish(0)
    gc_own[...] = restrict1(lambda x: ee[INNER1, GHOST + x, 0:R1, :], 0.125)

    def scaled(grid, weights, centre, near, iz_edges):
        full = [weights[d] + 0.5 * (centre + near[d]) for d in range(6)]
        diag = ((full[0] + full[1]) + (full[2] + full[3])) + (full[4] + full[5])
        inv = 1.0 / diag
        full = [f * inv for f in full]
        low, high = iz_edges
        along_z = jnp.where(even_lane, full[4], full[5])
        full[4] = jnp.where(low, 0.0, full[4])
        full[5] = jnp.where(high, 0.0, full[5])
        return full, diag, inv, along_z

    even_lane = jnp.bitwise_and(g0.lane, 1) == 0
    even_row = jnp.bitwise_and(g0.row, 1) == 0
    first0 = (g0.lane == 0) & (iz == 0)
    last0 = (g0.lane == Z0 - 1) & (iz == nz - 1)
    for side in range(2):
        for ref, has in ((xh0, here), (yh0, along)):
            val = jnp.where(ref[side, INNER] == 0.0, 3.0, 1.0)
            ref[side, OUTER] = jnp.where(has[2 * side - 1], val, 0.0)
    zh0[OUTER] = jnp.where(zh0[INNER] == 0.0, 3.0, 1.0)
    inv0 = vb
    for x in range(X0):
        centre, near = halo0.neighbours(OUTER, lambda x: out0[x], x, edge=True)
        full, diag, inv, along_z = scaled(g0, [w0[d, x] for d in range(6)], centre, near, (first0, last0))
        for d in range(6):
            c0[d, x] = full[d]
        d0[x] = diag
        b0[x] = inv
        mixed[x] = pltpu.roll(along_z, 1, 1)

    def update(halo, slot, planes, c, b, x):
        val, near = halo.neighbours(slot, planes, x)
        a = b[x] + c[0, x] * near[0]
        e = c[1, x] * near[1] + c[2, x] * near[2]
        f = c[3, x] * near[3] + c[4, x] * near[4]
        return val, (a + c[5, x] * near[5]) + (e + f)

    def half_sweep(number, halo, slot, src, dst, c, b, colour):
        planes = halo.grid.planes
        for x in range(planes) if number is None else inner_first(number, planes):
            val, new = update(halo, slot, lambda x: src[x], c, b, x)
            dst[x] = jnp.where(halo.grid.colour(x, colour), new, val)

    arrive(1)
    for x in inner_first(2, X0):
        m, near = halo0.neighbours(NEXT, lambda x: mem_out[x], x)
        rhs = jnp.zeros_like(m)
        for d in range(6):
            rhs = rhs + w0[d, x] * (near[d] - m)
        b0[x] = rhs * b0[x]
        val, new = update(halo0, V, lambda x: ext[x], c0, b0, x)
        va[x] = jnp.where(g0.colour(x, 0), new, val)
    publish(3, halo0, RED, va)

    first1 = (g1.lane == 0) & (iz == 0)
    last1 = (g1.lane == Z1 - 1) & (iz == nz - 1)
    pack_row = lax.broadcasted_iota(jnp.int32, (RE, LANES), 0)
    pack_lane = lax.broadcasted_iota(jnp.int32, (RE, LANES), 1)
    pack_x = jnp.bitwise_and(pack_lane, XE - 1)
    depth_parity = lax.div(pack_lane, XE) + iz + pack_x + pack_row
    pack_own = [jnp.bitwise_and(depth_parity + colour, 1) == 0 for colour in range(2)]

    def row_inside(row):
        return (
            (row < R1)
            | ((row < R1 + GHOST) & (iy < ny - 1))
            | ((row >= R1 + GHOST) & (iy > 0))
        )

    inside_row = row_inside(g1.row)
    pack_inside = (
        row_inside(pack_row)
        & (pack_lane < GHOST * XE)
        & ((pack_x >= GHOST) | (ix > 0))
        & ((pack_x < X1 + GHOST) | (ix < nx - 1))
    )

    def inside1(p):
        side = plane_side(p)
        return inside_row if side is None else inside_row & side

    def near1(planes, pack, p, edge=False):
        val = planes(p)
        side = jnp.broadcast_to(pack(p), (RE, Z1))
        side_m, side_p = side, side
        if edge:
            side_m = jnp.where(iz == 0, 0.0, side)
            side_p = jnp.where(iz == 0, side, 0.0)
        return val, (
            planes(p - 1),
            planes(p + 1),
            pltpu.roll(val, 1, 0),
            pltpu.roll(val, RE - 1, 0),
            jnp.where(g1.lane == 0, side_m, pltpu.roll(val, 1, 1)),
            jnp.where(g1.lane == Z1 - 1, side_p, pltpu.roll(val, Z1 - 1, 1)),
        )

    def near_pack(planes, val, first, last):
        own = jnp.zeros((RE, LANES), F32)
        for p in range(first, last):
            own = jnp.where(pack_lane == p, pltpu.roll(planes(p), p + 1 - iz, 1), own)
        return (
            pltpu.roll(val, 1, 1),
            pltpu.roll(val, LANES - 1, 1),
            pltpu.roll(val, 1, 0),
            pltpu.roll(val, RE - 1, 0),
            jnp.where(pack_lane < XE, own, pltpu.roll(val, XE, 1)),
            pltpu.roll(val, LANES - XE, 1),
        )

    def scaled_wide(ci, ni, co, no, inside):
        full = [jnp.minimum(ci, ni[k]) + 0.5 * (co + no[k]) for k in range(6)]
        diag = ((full[0] + full[1]) + (full[2] + full[3])) + (full[4] + full[5])
        inv = jnp.where(inside, 1.0 / diag, 0.0)
        return [jnp.where(inside, f * inv, 0.0) for f in full], diag, inv

    wide_arrive(0)

    def outer_of(inner):
        return jnp.where(inner == 0.0, 3.0, 1.0)

    for p in range(XE):
        ee[OUTER1, p] = jnp.where(inside1(p), outer_of(ee[INNER1, p]), 0.0)
    zp1[OUTER1] = jnp.where(pack_inside, outer_of(zp1[INNER1]), 0.0)
    for p in range(1, XE - 1):
        ci, ni = near1(lambda p: ee[INNER1, p], lambda p: zp1[INNER1, :, p : p + 1], p, edge=True)
        co, no = near1(lambda p: ee[OUTER1, p], lambda p: zp1[OUTER1, :, p : p + 1], p, edge=True)
        full, diag, inv = scaled_wide(ci, ni, co, no, inside1(p))
        full[4] = jnp.where(first1, 0.0, full[4])
        full[5] = jnp.where(last1, 0.0, full[5])
        for d in range(6):
            c1[d, p] = full[d]
        if GHOST <= p < X1 + GHOST:
            d1[p - GHOST] = diag[0:R1]
            b1[p - GHOST] = inv[0:R1]
    ci, co = zp1[INNER1], zp1[OUTER1]
    full, _, _ = scaled_wide(
        ci,
        near_pack(lambda p: ee[INNER1, p], ci, 0, XE),
        co,
        near_pack(lambda p: ee[OUTER1, p], co, 0, XE),
        pack_inside,
    )
    for d in range(6):
        cz1[d] = full[d]

    def stencil(b, c, near):
        a = b + c(0) * near[0]
        e = c(1) * near[1] + c(2) * near[2]
        f = c(3) * near[3] + c(4) * near[4]
        return (a + c(5) * near[5]) + (e + f)

    def update1(src, pack, p):
        val, near = near1(lambda p: src[p], lambda p: pack[:, p : p + 1], p)
        return val, stencil(ee[RHS1, p], lambda d: c1[d, p], near)

    def half1(src, pack, dst, colour, planes):
        for p in planes:
            val, new = update1(src, pack, p)
            dst[p] = jnp.where(g1.colour(p, colour), new, val)

    def half_pack(src, pack, dst, colour, first, last):
        val = pack[...]
        near = near_pack(lambda p: src[p], val, first, last)
        new = stencil(zp1[RHS1], lambda d: cz1[d], near)
        dst[...] = jnp.where(pack_own[colour], new, val)

    half_sweep(3, halo0, RED, va, vb, c0, b0, 1)
    publish(4, halo0, BLACK, vb)

    XG, RG, ZG = in2.shape
    XH, RH = XG // 2, RG // 2
    g2 = Grid(XG, RG, ZG)
    g3 = Grid(XH, RH, ZG)
    def unpack(tile, dst):
        for px in range(nx):
            for py in range(ny // 2):
                lows, highs = [], []
                for part in range(2):
                    base = (px * ny + 2 * py + part) * nz
                    s0, s1 = tile(base), tile(base + 1)
                    lows.append(jnp.where(tile_lane < half, s0, pltpu.roll(s1, half, 1)))
                    highs.append(jnp.where(tile_lane < half, pltpu.roll(s0, half, 1), s1))
                for xhi, pair in enumerate((lows, highs)):
                    p = px * X2 + xhi * 2
                    dst[p, py * 8 : py * 8 + 8, :] = jnp.where(tile_row < R2, pair[0], pltpu.roll(pair[1], R2, 0))
                    dst[p + 1, py * 8 : py * 8 + 8, :] = jnp.where(
                        tile_row < R2, pltpu.roll(pair[0], R2, 0), pair[1]
                    )

    def whole_neighbours(grid, planes, x, last, mask):
        val = planes(x)
        zero = jnp.zeros_like(val)
        xm = planes(x - 1) if x > 0 else zero
        xp = planes(x + 1) if x < grid.planes - 1 else zero
        near = [
            xm,
            xp,
            pltpu.roll(val, 1, 0),
            pltpu.roll(val, grid.rows - 1, 0),
            pltpu.roll(val, 1, 1),
            pltpu.roll(val, grid.lanes - 1, 1),
        ]
        if mask:
            near[2] = jnp.where(grid.row == 0, 0.0, near[2])
            near[3] = jnp.where(grid.row == grid.rows - 1, 0.0, near[3])
            near[4] = jnp.where(grid.lane == 0, 0.0, near[4])
            near[5] = jnp.where(grid.lane >= last, 0.0, near[5])
        return val, near

    def whole_couplings(grid, inner, outer, last, c, d, b):
        for x in range(grid.planes):
            ci, ni = whole_neighbours(grid, lambda x: inner[x], x, last, True)
            co, no = whole_neighbours(grid, lambda x: outer[x], x, last, True)
            full = [jnp.minimum(ci, ni[k]) + 0.5 * (co + no[k]) for k in range(6)]
            diag = ((full[0] + full[1]) + (full[2] + full[3])) + (full[4] + full[5])
            if last < grid.lanes - 1:
                diag = jnp.where(grid.lane <= last, diag, 1.0)
            inv = 1.0 / diag
            edges = (
                None,
                None,
                grid.row == 0,
                grid.row == grid.rows - 1,
                grid.lane == 0,
                grid.lane >= last,
            )
            for k in range(6):
                f = full[k] * inv
                if edges[k] is not None:
                    f = jnp.where(edges[k], 0.0, f)
                if last < grid.lanes - 1:
                    f = jnp.where(grid.lane <= last, f, 0.0)
                c[k, x] = f
            if d is not None:
                d[x] = diag
            b[x] = inv

    def whole_update(grid, planes, c, b, x):
        val, near = whole_neighbours(grid, planes, x, None, False)
        a = b[x] + c[2, x] * near[2]
        e = c[3, x] * near[3] + c[4, x] * near[4]
        a = a + c[5, x] * near[5]
        if x > 0:
            a = a + c[0, x] * near[0]
        if x < grid.planes - 1:
            e = e + c[1, x] * near[1]
        return val, a + e

    def restrict2(plane, factor):
        pieces = [halve_rows(tmp, x, plane(2 * x) + plane(2 * x + 1)) for x in range(XH)]
        for x in range(XH):
            tall[x * RH : (x + 1) * RH, 0:ZG] = pieces[x]
        whole = dot(tall[0 : XH * RH, 0:ZG], narrow_low) * factor
        return [whole[x * RH : (x + 1) * RH] for x in range(XH)]

    def mix(x, a, b):
        return jnp.where(g0.colour(x, 0), a, pltpu.roll(b, 1, 1))

    across = jnp.zeros((R0, LANES), F32)
    face_lane = lax.broadcasted_iota(jnp.int32, (R0, LANES), 1)
    for x in range(X0):
        along_y = jnp.where(even_row, c0[2, x], c0[3, x])
        along_x = c0[x % 2, x]
        if x == 0 or x == X0 - 1:
            xs0[x // (X0 - 1), MIXED] = mix(x, c0[x % 2, x], along_y)
        val = mix(x, jnp.where(g0.row < R0 // 2, c0[2, x], c0[3, x]), along_x)
        ys0[0, MIXED, x : x + 1, :] = val[0:1]
        ys0[1, MIXED, x : x + 1, :] = val[R0 - 1 :]
        toward = jnp.where(iz == 0, c0[5, x, :, Z0 - LANES :], c0[4, x, :, 0:LANES])
        outs = [toward] + [
            jnp.where(iz == 0, f[:, Z0 - LANES :], f[:, 0:LANES]) for f in (along_x, along_y)
        ]
        for k, end in enumerate(outs):
            at = k * X0 + x
            across = jnp.where(face_lane == at, pltpu.roll(end, at + 1 - iz, 1), across)
    zs0[MIXED] = across
    def residual0(x):
        val, new = update(halo0, BLACK, lambda x: vb[x], c0, b0, x)
        mixed[x] = jnp.where(g0.colour(x, 0), new, mixed[x])
        return d0[x] * (new - val)

    for x, val in enumerate(restrict0(residual0, 0.5, 0, inner_first(4, X1))):
        ee[RHS1, GHOST + x, 0:R1, :] = val * b1[x]
    wide_publish(1)
    halo0.put(READY, mixed)
    send(5)
    gather_send(gc_own, gc, 0)
    wide_arrive(1)
    ring = GHOST - 1
    for p in range(ring - 1, XE - ring + 1):
        v1a[p] = jnp.where(g1.colour(p, 0), ee[RHS1, p], 0.0)
    z1a[...] = jnp.where(pack_own[0], zp1[RHS1], 0.0)
    half_pack(v1a, z1a, z1b, 1, ring, XE - ring)
    half1(v1a, z1a, v1b, 1, range(ring, XE - ring))

    def residual1(x):
        val, new = update1(v1b, z1b, GHOST + x)
        return d1[x] * (new - val)[0:R1]

    gr_own[...] = restrict1(residual1, 0.5)
    gather_send(gr_own, gr, 1)
    for p in (0, 1, XE - 2, XE - 1):
        v1a[p] = jnp.where(g1.colour(p, 0), ee[RHS1, p], 0.0)
    half_pack(v1a, z1a, z1b, 1, 0, XE)
    half1(v1a, z1a, v1b, 1, (1, 2, XE - 3, XE - 2))
    gather_wait(gc, 0, True)
    unpack(lambda t: gc[t], in2)
    for x in range(XG):
        out2[x] = outer_of(in2[x])
    whole_couplings(g2, in2, out2, ZG - 1, c2, d2, b2)
    for x, val in enumerate(restrict2(lambda x: in2[x], 0.125)):
        v3[x] = val
    for x, val in enumerate(restrict2(lambda x: out2[x], 0.125)):
        v2a[x, 0:RH] = val
    whole_couplings(g3, v3, v2a.at[:, 0:RH], ZG // 2 - 1, c3, None, b3)

    XP = XH // 2
    own = (g3.even, g3.odd)

    def pack(colour, near, far):
        return jnp.where(own[colour], near, far)

    for colour in range(2):
        for p in range(XP):
            a, z = 2 * p, 2 * p + 1
            k3[colour * 6, p] = pack(colour, c3[1, a], c3[0, z])
            k3[colour * 6 + 1, p] = pack(colour, c3[0, a], c3[1, z])
            for k in range(2, 6):
                k3[colour * 6 + k, p] = pack(colour, c3[k, a], c3[k, z])
            if colour == 0:
                for k in range(6):
                    k3[12 + k, p] = pltpu.roll(k3[k, p], 1, 1)
                    k3[18 + k, p] = pltpu.roll(k3[k, p], ZG - 1, 1)

    gather_wait(gr, 1, True)
    arrive(5)
    unpack(lambda t: gr[t], v2b)
    for x in range(XG):
        b2[x] = v2b[x] * b2[x]
        v2a[x] = jnp.where(g2.colour(x, 0), b2[x], 0.0)
    for x in range(XG):
        val, new = whole_update(g2, lambda x: v2a[x], c2, b2, x)
        v2b[x] = jnp.where(g2.colour(x, 1), new, val)

    def residual2(x):
        val, new = whole_update(g2, lambda x: v2b[x], c2, b2, x)
        return d2[x] * (new - val)

    for x, val in enumerate(restrict2(residual2, 0.5)):
        b3[x] = val * b3[x]

    for colour in range(2):
        for p in range(XP):
            h3[colour, p] = pack(colour, b3[2 * p], b3[2 * p + 1])
    none = jnp.zeros((RH, ZG), F32)

    at_shift = {0: 0, 1: 12, -1: 18}
    first_h = {s: [pltpu.roll(h3[0, p], s % ZG, 1) if s else h3[0, p] for p in range(XP)] for s in STEPS}

    def relaxed(colour, shift, shifted):
        fresh = []
        for p in range(XP):
            val, at = shifted[shift][p], colour * 6 + at_shift[shift]
            before = shifted[shift][p - 1] if p > 0 else none
            after = shifted[shift][p + 1] if p < XP - 1 else none
            i = (h3[1, p] if colour else first_h[shift][p]) + k3[at, p] * val
            mask = own[(colour + shift) % 2]
            j = k3[at + 1, p] * jnp.where(mask, before, after) + k3[at + 2, p] * pltpu.roll(val, 1, 0)
            l = k3[at + 3, p] * pltpu.roll(val, RH - 1, 0) + k3[at + 4, p] * shifted[shift + 1][p]
            fresh.append((i + k3[at + 5, p] * shifted[shift - 1][p]) + (j + l))
        return fresh

    def coarse(step, state):
        shifted = {0: state[XP:]}
        for s in (-2, -1, 1, 2):
            shifted[s] = [pltpu.roll(v, s % ZG, 1) for v in shifted[0]]
        red = {s: relaxed(0, s, shifted) for s in STEPS}
        return tuple(red[0] + relaxed(1, 0, red))

    start = relaxed(1, 0, first_h)
    state = tuple(first_h[0] + start)
    for step in range(1, COARSE_SWEEPS):
        state = coarse(step, state)
    solved = []
    for p in range(XP):
        solved.append(pack(0, state[p], state[XP + p]))
        solved.append(pack(1, state[p], state[XP + p]))
    for x in range(XH):
        tall[x * RH : (x + 1) * RH, 0:ZG] = solved[x]
    wide = dot(tall[0 : XH * RH, 0:ZG], double12)
    for x in range(XH):
        corr = double_rows(tmp, x, wide[x * RH : (x + 1) * RH])
        v2a[2 * x] = v2b[2 * x] + corr
        v2a[2 * x + 1] = v2b[2 * x + 1] + corr
    for colour, src, dst in ((0, v2a, v2b), (1, v2b, v2a)):
        for x in range(XG):
            val, new = whole_update(g2, lambda x: src[x], c2, b2, x)
            dst[x] = jnp.where(g2.colour(x, colour), new, val)

    row_shift = lax.rem(RG - iy * R2, RG)
    lane_shift = lax.rem(ZG - iz * half, ZG)
    edge2 = GHOST // 2
    rows2 = R2 + 2 * edge2
    planes2 = X2 + 2 * edge2
    for k in range(planes2):
        part = v2a[jnp.clip(ix * X2 + k - edge2, 0, XG - 1)]
        part = pltpu.roll(pltpu.roll(part, row_shift, 0), lane_shift, 1)
        tall[k * rows2 : (k + 1) * rows2, 0:ZG] = jnp.where(
            tile_row < R2 + edge2, part[0:rows2], part[RG - rows2 : RG]
        )
    source = lax.broadcasted_iota(jnp.int32, (ZG, LANES), 0)
    target = lax.broadcasted_iota(jnp.int32, (ZG, LANES), 1)
    target = lax.div(target, 2 * XE)
    pick = jnp.where(source == jnp.where(iz == 0, half + target, ZG - 1 - target), 1.0, 0.0).astype(F32)
    coarse_rows = tall[0 : planes2 * rows2, 0:ZG]
    wide = dot(coarse_rows, double12)
    sides = dot(coarse_rows, pick)
    acc = jnp.zeros((rows2, LANES), F32)
    tile_plane = lax.div(jnp.bitwise_and(tile_lane, XE - 1), 2)
    for k in range(planes2):
        acc = jnp.where(tile_plane == k, sides[k * rows2 : (k + 1) * rows2], acc)
    z1a[...] = z1b[...] + jnp.where(pack_inside, double_rows(tmp, 0, acc), 0.0)
    for k in range(planes2):
        corr = double_rows(tmp, k, wide[k * rows2 : (k + 1) * rows2])
        for p in (2 * k, 2 * k + 1):
            if 0 < p < XE - 1:
                v1a[p] = v1b[p] + jnp.where(inside1(p), corr, 0.0)
    half_pack(v1a, z1a, z1b, 0, 1, XE - 1)
    half1(v1a, z1a, v1b, 0, range(2, XE - 2))
    half_pack(v1b, z1b, z1a, 1, 2, XE - 2)
    half1(v1b, z1b, v1a, 1, range(3, XE - 3))

    def enlarge(count, read, write):
        for x in range(count):
            tall[x * R1 : (x + 1) * R1, 0:Z1] = read(x)
        wide = dot(tall[0 : count * R1, 0:Z1], double01)
        for x in range(count):
            write(x, double_rows(tmp, x, wide[x * R1 : (x + 1) * R1]))

    def inside(x, corr):
        va[2 * x] = vb[2 * x] + corr
        va[2 * x + 1] = vb[2 * x + 1] + corr

    enlarge(X1, lambda x: v1a[GHOST + x, 0:R1, :], inside)
    diagonal = tile_lane == tile_row + GHOST
    stack, lined_stack = [], []
    own_pack = jnp.zeros((RE, LANES), F32)
    for p in range(GHOST, XE - GHOST):
        own_pack = jnp.where(pack_lane == p, pltpu.roll(v1a[p], p + 1 - iz, 1), own_pack)
    for k in range(2):
        p, own = (GHOST - 1, GHOST) if k == 0 else (X1 + GHOST, X1 + GHOST - 1)
        val, near = near1(lambda p: v1a[p], lambda p: z1a[:, p : p + 1], p, edge=True)
        stack += [val[0:R1]] + [(other - val)[0:R1] for other in (v1a[own], near[2], near[3])]
        lined_stack.append(((near[4] - val)[0:R1], (near[5] - val)[0:R1]))
    for k in range(2):
        row, own = (RE - 1, 0) if k == 0 else (R1, R1 - 1)
        for p in range(GHOST - 1, X1 + GHOST + 1):
            yrim[k, p : p + 1, :] = v1a[p, row : row + 1, :]
            if GHOST <= p < X1 + GHOST:
                yrim[2 + k, p : p + 1, :] = v1a[p, own : own + 1, :]
        val = yrim[k, GHOST : X1 + GHOST, :]
        others = [
            yrim[2 + k, GHOST : X1 + GHOST, :],
            yrim[k, GHOST - 1 : X1 + GHOST - 1, :],
            yrim[k, GHOST + 1 : X1 + GHOST + 1, :],
        ]
        stack += [val] + [other - val for other in others]
        line = jnp.where(diagonal, jnp.broadcast_to(z1a[row : row + 1, :], (8, LANES)), 0.0)
        column = jnp.broadcast_to(jnp.sum(line, axis=1, keepdims=True), (8, LANES))
        back = jnp.where(tile_lane == 0, jnp.where(iz == 0, 0.0, column), pltpu.roll(val, 1, 1))
        ahead = jnp.where(tile_lane == Z1 - 1, jnp.where(iz == 0, column, 0.0), pltpu.roll(val, Z1 - 1, 1))
        lined_stack.append((back - val, ahead - val))
    val = z1a[...]
    shifts = [pltpu.roll(val, 1, 0), pltpu.roll(val, RE - 1, 0), pltpu.roll(val, 1, 1), pltpu.roll(val, LANES - 1, 1)]
    face = [val, own_pack - val] + [other - val for other in shifts]
    face = [pltpu.roll(f[0:R1], LANES - GHOST, 1) for f in face]
    stack += face[:4]
    lined_stack.append((face[4], face[5]))
    for i, piece in enumerate(stack):
        tall[i * R1 : (i + 1) * R1, 0:Z1] = piece
    for i, (back, ahead) in enumerate(lined_stack):
        tall2[i * R1 : (i + 1) * R1, 0:Z1] = back
        tall2[i * R1 : (i + 1) * R1, Z1 : 2 * Z1] = ahead
    k = lax.broadcasted_iota(jnp.int32, (2 * Z1, Z0), 0)
    j = lax.broadcasted_iota(jnp.int32, (2 * Z1, Z0), 1)
    source = lax.shift_right_logical(j, 1) + Z1 * jnp.bitwise_and(j, 1)
    big = dot(tall[0 : len(stack) * R1, 0:Z1], double01)
    lined_big = dot(tall2[0 : len(lined_stack) * R1, :], jnp.where(k == source, 1.0, 0.0).astype(F32))

    def woven(slot, first, second):
        parts = []
        for k in range(Z0 // LANES):
            at = 2 * slot + k
            tmp[at, pl.ds(0, R1, 2), :] = first[:, k * LANES : (k + 1) * LANES]
            tmp[at, pl.ds(1, R1, 2), :] = second[:, k * LANES : (k + 1) * LANES]
            parts.append(tmp[at, 0:R0, :])
        return jnp.concatenate(parts, axis=1)

    def finished(k):
        piece = [big[(4 * k + i) * R1 : (4 * k + i + 1) * R1] for i in range(4)]
        lines = lined_big[k * R1 : (k + 1) * R1]
        at = 4 * (k % 2)
        return (
            woven(at, piece[0], piece[0]),
            woven(at + 1, piece[1], piece[1]),
            woven(at + 2, piece[2], piece[3]),
            woven(at + 3, lines, lines),
        )

    for k in range(4):
        ref, side = (xh0, k) if k < 2 else (yh0, k - 2)
        corr, toward, beside, lengthwise = finished(k)
        ref[side, FIXED] = ref[side, BLACK] + corr
        first, second = ref[side, MIXED], ref[side, READY]
        ref[side, LAST] = ((second + corr) + first * toward) + (
            pltpu.roll(first, Z0 - 1, 1) * beside + pltpu.roll(second, Z0 - 1, 1) * lengthwise
        )
    corr, toward, beside, sideways = [f[:, 0:LANES] for f in finished(4)]
    zh0[FIXED] = zh0[BLACK] + corr
    first = zh0[MIXED]
    zh0[LAST] = ((zh0[READY] + corr) + first * toward) + (
        pltpu.roll(first, LANES - X0, 1) * sideways + pltpu.roll(first, LANES - 2 * X0, 1) * beside
    )
    half_sweep(None, halo0, FIXED, va, vb, c0, b0, 0)
    half_sweep(None, halo0, LAST, vb, ext_out, c0, b0, 1)

    for number in range(len(EXCHANGES)):
        sent(number)
    for number in range(len(WIDE)):
        wide_sent(number)
    gather_wait(gc, 0, False)
    gather_wait(gr, 1, False)


def finish(*refs):
    count = (len(refs) - 1) // 2
    sem = refs[-1]
    copies = [pltpu.make_async_copy(refs[i], refs[count + i], sem.at[i]) for i in range(count)]
    for copy in copies:
        copy.start()
    for copy in copies:
        copy.wait()


def solution(mesh):
    nx, ny, nz = (mesh.shape[a] for a in ("gx", "gy", "gz"))
    spec = P("gx", "gy", "gz")

    def on_device(membrane, recovery, extracellular, fiber_scale, labels):
        X, R, Z = membrane.shape
        X1, R1, Z1 = X // 2, R // 2, Z // 2
        XG, RG, ZG = nx * X // 4, ny * R // 4, nz * Z // 4
        assert nz == 2 and ny % 2 == 0 and ZG == LANES and Z1 == LANES
        assert R1 == 8 and X1 == 8 and X % 8 == 0
        total = nx * ny * nz
        assert labels.shape == (2, 2, LANES // 4)
        f0 = 11
        field = (X, R, Z)
        lvl1 = (X1, R1, Z1)
        whole = (XG, RG, ZG)
        third = (XG // 2, RG // 2, ZG)

        def v(*shape):
            return pltpu.VMEM(shape, F32)

        def faces(f, x, r, z):
            return [v(2, f, r, z), v(2, f, x, z), v(f, r, LANES)] * 2

        anywhere = pl.BlockSpec(memory_space=pl.ANY)
        scratch = [v(*field)] * 4 + [pltpu.VMEM(labels.shape, jnp.int32), pltpu.SemaphoreType.DMA((5,))]
        scratch += faces(f0, *field)
        scratch += [v(*field), v(*field), v(*field), v(6, *field), v(6, *field), v(*field), v(*field)]
        scratch += [v(*field), v(*field)]
        scratch += [
            v(2 * max(X1, XG // 2), max(R, RG), LANES),
            v(max(X1 * R1, (XG // 2) * (RG // 2), 2 * X1 * R1, 20 * R1, total), Z),
        ]
        XE, RE = X1 + 2 * GHOST, R1 + 2 * GHOST
        assert GHOST * XE <= LANES and 2 * GHOST == R1 and GHOST <= X1
        wide, pack = (XE, RE, Z1), (RE, LANES)
        scratch += [v(3, *wide), v(2, 3, X1 // 2, R1, Z1), v(2, 3, XE // 2, R1, Z1), v(3, R1, LANES)]
        scratch += [v(9, 3, R1, LANES), v(3, *pack), v(6, *wide), v(6, *pack), v(*lvl1), v(*lvl1)]
        scratch += [v(*wide), v(*wide), v(*pack), v(*pack), v(4, XE, Z1)]
        scratch += [v(*field), v(8 * R1, Z)]
        scratch += [v(8, LANES), v(total, 8, LANES), v(8, LANES), v(total, 8, LANES)]
        scratch += [v(*whole), v(*whole), v(6, *whole), v(*whole), v(*whole), v(*whole), v(*whole)]
        scratch += [v(6, *third), v(*third), v(*third)]
        packed = (XG // 4, RG // 2, ZG)
        scratch += [v(24, *packed), v(2, *packed)]
        sems = SIDES * len(EXCHANGES)
        scratch += [pltpu.SemaphoreType.DMA((sems,))] * 2
        scratch += [pltpu.SemaphoreType.DMA((WIDE_SIDES * len(WIDE),))] * 2
        scratch += [pltpu.SemaphoreType.DMA((2,))] * 2
        vmem = pl.BlockSpec(memory_space=pltpu.VMEM)
        room = 54400 << 10
        shape = jax.ShapeDtypeStruct(field, F32)
        results = pl.pallas_call(
            functools.partial(kernel, (nx, ny, nz)),
            out_shape=[shape] * 3,
            in_specs=[anywhere] * 5,
            out_specs=[vmem] * 3,
            scratch_shapes=scratch,
            compiler_params=pltpu.CompilerParams(
                collective_id=0, has_side_effects=True, vmem_limit_bytes=room
            ),
        )(membrane, recovery, extracellular, fiber_scale, labels)
        return tuple(
            pl.pallas_call(
                finish,
                out_shape=[shape] * 3,
                in_specs=[vmem] * 3,
                out_specs=[anywhere] * 3,
                scratch_shapes=[pltpu.SemaphoreType.DMA((3,))],
                compiler_params=pltpu.CompilerParams(vmem_limit_bytes=4 << 20),
            )(*results)
        )

    return jax.shard_map(
        on_device,
        mesh=mesh,
        in_specs=(spec,) * 5,
        out_specs=(spec,) * 3,
        check_vma=False,
    )
```
